32 devices in a mesh: seq: 8 (over y, x, core), tensor: 4 (over z).
Axes of the slice: x: 2, y: 2, z: 4, core: 2. Of those that a mesh axis runs over, the one named last changes fastest.
Arguments:
- tokens_in: bfloat16 [9216, 2560], P(('seq', 'tensor')), may hold values from -6 to 6
- gain_pre: float32 [2560], replicated, may hold values from 0.5 to 1.5
- w_x: bfloat16 [2560, 10, 256], P(None, None, 'tensor'), may hold values from -0.125 to 0.125
- w_y: bfloat16 [2560, 10, 256], P(None, None, 'tensor'), may hold values from -0.125 to 0.125
- conv_w: float32 [4, 10, 256], P(None, None, 'tensor'), may hold values from -3 to 3
- gate_a: bfloat16 [10, 256, 256], P(None, None, 'tensor'), may hold values from -0.375 to 0.375
- gate_i: bfloat16 [10, 256, 256], P(None, None, 'tensor'), may hold values from -0.375 to 0.375
- decay_param: float32 [10, 256], P(None, 'tensor'), may hold values from -10 to -4
- w_out: bfloat16 [10, 256, 2560], P(None, 'tensor'), may hold values from -0.125 to 0.125
- gain_mlp: float32 [2560], replicated, may hold values from 0.5 to 1.5
- w_gate: bfloat16 [2560, 7680], P(None, 'tensor'), may hold values from -0.125 to 0.125
- w_up: bfloat16 [2560, 7680], P(None, 'tensor'), may hold values from -0.125 to 0.125
- w_down: bfloat16 [7680, 2560], P('tensor'), may hold values from -0.0625 to 0.0625
- cotangent: bfloat16 [9216, 2560], P(('seq', 'tensor')), may hold values from -6 to 6
Outputs:
- block_out: bfloat16 [9216, 2560], P(('seq', 'tensor'))
- input_grad: float32 [9216, 2560], P(('seq', 'tensor'))
- grad_gain_pre: float32 [2560], replicated
- grad_w_x: float32 [2560, 10, 256], P('seq', None, 'tensor')
- grad_w_y: float32 [2560, 10, 256], P('seq', None, 'tensor')
- grad_conv_w: float32 [4, 10, 256], P(None, None, ('tensor', 'seq'))
- grad_gate_a: float32 [10, 256, 256], P(None, 'seq', 'tensor')
- grad_gate_i: float32 [10, 256, 256], P(None, 'seq', 'tensor')
- grad_decay_param: float32 [10, 256], P(None, ('tensor', 'seq'))
- grad_w_out: float32 [10, 256, 2560], P(None, 'tensor', 'seq')
- grad_gain_mlp: float32 [2560], P('seq')
- grad_w_gate: float32 [2560, 7680], P('seq', 'tensor')
- grad_w_up: float32 [2560, 7680], P('seq', 'tensor')
- grad_w_down: float32 [7680, 2560], P('tensor', 'seq')
The draws below stay inside these ranges and needn't reach their ends.
All inputs are finite; a program needn't handle non-finite values.
Results may differ from the reference program's by a relative error of at most 0.02.
The reference program's roundings to bfloat16 on the way count: a program that leaves them out, or rounds other values in their place, can miss the bound.
Values may be sent and summed in bfloat16 or wider, within the bound.
A program may use at most 320 MiB of HBM per device.

```python
import math
import jax
import jax.numpy as jnp
from jax import lax

D = 2560
H = 10
BW = 256
FF = 7680
CONV = 4
SEQS = 3
LRU = 2560
TOKENS = 9216
LENGTH = 3072


def block_levels(rng, dims, split, least, largest):
    loudness = 1.0
    for axis_at, blocks in split:
        draws = jax.random.uniform(jax.random.fold_in(jax.random.fold_in(rng, 6), axis_at), (blocks,), jnp.float32, least / len(split), largest / len(split))
        loudness = loudness * jnp.repeat(jnp.exp(draws), dims[axis_at] // blocks).reshape((-1,) + (1,) * (len(dims) - 1 - axis_at))
    return loudness


def bell_draw(key, extent, deviation, limit, shards=(), kind=jnp.bfloat16):
    values = deviation * jax.random.normal(key, extent, jnp.float32)
    if shards:
        values = values * block_levels(key, extent, shards, -0.22, 0.18)
    return jnp.clip(values, -limit, limit).astype(kind)


def setup_inputs(seed: int = 0) -> dict:
    arg_keys = jax.random.split(jax.random.key(seed), 15)
    return {
        "tokens_in": bell_draw(arg_keys[0], (TOKENS, D), 1.0, 6.0, ((0, 32),)),
        "gain_pre": jnp.clip(1.0 + 0.1 * jax.random.normal(arg_keys[1], (D,), jnp.float32), 0.5, 1.5),
        "w_x": bell_draw(arg_keys[2], (D, H, BW), D ** -0.5, 0.125, ((2, 4),)),
        "w_y": bell_draw(arg_keys[3], (D, H, BW), D ** -0.5, 0.125, ((2, 4),)),
        "conv_w": bell_draw(arg_keys[4], (CONV, H, BW), CONV ** -0.5, 3.0, ((2, 4),), jnp.float32),
        "gate_a": bell_draw(arg_keys[5], (H, BW, BW), BW ** -0.5, 0.375, ((2, 4),)),
        "gate_i": bell_draw(arg_keys[6], (H, BW, BW), BW ** -0.5, 0.375, ((2, 4),)),
        "decay_param": jnp.clip(-10.0 + 6.0 * jax.random.uniform(arg_keys[7], (H, BW), jnp.float32) ** block_levels(arg_keys[7], (H, BW), ((1, 4),), -0.2, 0.2), -10.0, -4.0),
        "w_out": bell_draw(arg_keys[8], (H, BW, D), LRU ** -0.5, 0.125, ((1, 4),)),
        "gain_mlp": jnp.clip(1.0 + 0.1 * jax.random.normal(arg_keys[9], (D,), jnp.float32), 0.5, 1.5),
        "w_gate": bell_draw(arg_keys[10], (D, FF), D ** -0.5, 0.125, ((1, 4),)),
        "w_up": bell_draw(arg_keys[11], (D, FF), D ** -0.5, 0.125, ((1, 4),)),
        "w_down": bell_draw(arg_keys[12], (FF, D), FF ** -0.5, 0.0625, ((0, 4),)),
        "cotangent": bell_draw(arg_keys[13], (TOKENS, D), 1.0, 6.0, ((0, 32),)),
    }


@jax.custom_vjp
def low(v):
    return lax.optimization_barrier(v.astype(jnp.bfloat16)).astype(jnp.float32)

@jax.custom_vjp
def low_back(v):
    return v

def low_keep(v):
    return (low(v), None)

def low_pass(kept, grad):
    return (grad,)

def back_keep(v):
    return (v, None)

def back_low(kept, grad):
    return (low(grad),)
low.defvjp(low_keep, low_pass)
low_back.defvjp(back_keep, back_low)
epsilon = 1e-06
highest = lax.Precision.HIGHEST

def rms_scale(values, gain):
    return values * lax.rsqrt(lax.optimization_barrier(jnp.mean(values * values, axis=-1, keepdims=True)) + epsilon) * gain

def pair_combine(earlier, later):
    return (earlier[0] * later[0], later[0] * earlier[1] + later[1])

def block_states(running, pieces):
    decays, drives = pieces
    products, partial_states = lax.associative_scan(pair_combine, (decays, drives), axis=0)
    states = partial_states + products * running
    return (states[-1], states)

def recurrence(decays, drives):
    seq_rows = decays.shape[0]
    block_rows = math.gcd(seq_rows, 256)
    shaped = (seq_rows // block_rows, block_rows) + decays.shape[1:]
    initial = jnp.zeros(decays.shape[1:], jnp.float32)
    final_state, states = lax.scan(jax.checkpoint(block_states), initial, (decays.reshape(shaped), drives.reshape(shaped)))
    return states.reshape(decays.shape)

def forward(seq_in, gain_pre, w_x, w_y, conv_w, gate_a, gate_i, decay_param, w_out, gain_mlp, w_gate, w_up, w_down):
    seq_rows = seq_in.shape[0]
    position = jnp.arange(seq_rows, dtype=jnp.int32)
    normed = low(rms_scale(seq_in, gain_pre))
    x_branch = low(low_back(jnp.einsum('td,dhc->thc', normed, w_x, precision=highest)))
    y_branch = low_back(jnp.einsum('td,dhc->thc', normed, w_y, precision=highest))
    gated = jax.nn.gelu(y_branch, approximate=True)
    padded = jnp.pad(x_branch, ((CONV - 1, 0), (0, 0), (0, 0)))
    conv_out = jnp.zeros_like(x_branch)
    for offset in range(CONV):
        window = padded[CONV - 1 - offset:CONV - 1 - offset + seq_rows]
        inside = (position >= offset).astype(jnp.float32)[:, None, None]
        conv_out = conv_out + conv_w[offset] * window * inside
    conv_out = low(conv_out)
    rate_pre = low_back(jnp.einsum('thk,hkc->thc', conv_out, gate_a, precision=highest))
    input_pre = low_back(jnp.einsum('thk,hkc->thc', conv_out, gate_i, precision=highest))
    log_decay = -8.0 * jax.nn.softplus(decay_param) * jax.nn.sigmoid(rate_pre)
    decays = jnp.where((position == 0)[:, None, None], 0.0, jnp.exp(log_decay))
    scaling = jnp.sqrt(jnp.maximum(1.0 - decays * decays, 0.01))
    drives = scaling * jax.nn.sigmoid(input_pre) * conv_out
    states = recurrence(decays, drives)
    mixed = low(states * gated)
    branch = low_back(jnp.einsum('thc,hcd->td', mixed, w_out, precision=highest))
    middle = seq_in + branch
    normed_mlp = low(rms_scale(middle, gain_mlp))
    gate_pre = low_back(jnp.dot(normed_mlp, w_gate, precision=highest))
    up_pre = low_back(jnp.dot(normed_mlp, w_up, precision=highest))
    hidden = low(jax.nn.gelu(gate_pre, approximate=True) * up_pre)
    return middle + jnp.dot(hidden, w_down, precision=highest)

def reference(tokens_in, gain_pre, w_x, w_y, conv_w, gate_a, gate_i, decay_param, w_out, gain_mlp, w_gate, w_up, w_down, cotangent):
    params = tuple((value.astype(jnp.float32) for value in (gain_pre, w_x, w_y, conv_w, gate_a, gate_i, decay_param, w_out, gain_mlp, w_gate, w_up, w_down)))
    inputs = tokens_in.astype(jnp.float32).reshape(SEQS, LENGTH, D)
    cotangents = cotangent.astype(jnp.float32).reshape(SEQS, LENGTH, D)

    def one_sequence(running, pieces):
        seq_in, seq_cot = pieces
        result, pull = jax.vjp(forward, seq_in, *params)
        gradients = pull(seq_cot)
        running = tuple((earlier + gradient for earlier, gradient in zip(running, gradients[1:])))
        return (running, (result.astype(jnp.bfloat16), gradients[0]))
    initial = tuple((jnp.zeros_like(value) for value in params))
    totals, (results, input_grads) = lax.scan(one_sequence, initial, (inputs, cotangents))
    return (results.reshape(TOKENS, D), input_grads.reshape(TOKENS, D), totals[0], totals[1], totals[2], totals[3], totals[4], totals[5], totals[6], totals[7], totals[8], totals[9], totals[10], totals[11])
```

```python
import functools
import math

import jax
import jax.numpy as jnp
from jax import lax
from jax.experimental import pallas as pl
from jax.experimental.pallas import tpu as pltpu
from jax.sharding import PartitionSpec as P

CONV = 4
SEQS = 3
HALO = 16
epsilon = 1e-06
F32 = jnp.float32
BF16 = jnp.bfloat16
ROOT = math.sqrt(2.0 / math.pi)
BOTH = ("seq", "tensor")


def dot_nn(a, b):
    return lax.dot_general(a, b, (((1,), (0,)), ((), ())), preferred_element_type=F32)


def dot_nt(a, b):
    return lax.dot_general(a, b, (((1,), (1,)), ((), ())), preferred_element_type=F32)


def dot_tn(a, b):
    return lax.dot_general(a, b, (((0,), (0,)), ((), ())), preferred_element_type=F32)


def rms_parts(values):
    scale = lax.rsqrt(jnp.mean(values * values, axis=-1, keepdims=True) + epsilon)
    return scale, values * scale


def rms_back(grad, gain, scale, unit):
    pulled = gain * grad
    inner = jnp.mean(pulled * unit, axis=-1, keepdims=True)
    return jnp.sum(grad * unit, axis=0), scale * (pulled - unit * inner)


def gelu_both(v):
    inner = v * v
    th = jnp.tanh(ROOT * (v + 0.044715 * v * inner))
    half = 0.5 * (1.0 + th)
    slope = half + 0.5 * v * (1.0 - th * th) * (ROOT * (1.0 + 3 * 0.044715 * inner))
    return v * half, slope


LABELS = ((1, 2, 3, 2), (2, 0, 1, 1), (3, 3, 0, 0))


def along(block, pairs):
    return lax.ppermute(block, "tensor", pairs)


def line_streams(own):
    right, left = [], []
    right.append(along(own, [(0, 1), (1, 2), (2, 3)]))
    left.append(along(own, [(1, 0), (2, 1), (3, 2)]))
    right.append(along(right[0], [(1, 2), (2, 3)]))
    left.append(along(left[0], [(1, 0), (2, 1)]))
    right.append(along(right[1], [(2, 3)]))
    left.append(along(left[1], [(1, 0)]))
    return right, left


def others(own):
    count = lax.axis_size("tensor")
    place = lax.axis_index("tensor")
    if count == 4:
        right, left = line_streams(own)
        first = jnp.where(place == 3, right[0], left[0])
        second = jnp.where(place == 0, left[1], jnp.where(place == 3, right[1], right[0]))
        third = jnp.where(
            place == 0, left[2], jnp.where(place == 1, left[1], jnp.where(place == 2, right[1], right[2]))
        )
        return [first, second, third]
    whole = lax.all_gather(own, "tensor", axis=0)
    return [lax.dynamic_index_in_dim(whole, (place + k) % count, 0, False) for k in range(1, count)]


def label_index(k):
    count = lax.axis_size("tensor")
    place = lax.axis_index("tensor")
    if count == 4:
        table = LABELS[k - 1]
        return jnp.where(
            place == 0, table[0], jnp.where(place == 1, table[1], jnp.where(place == 2, table[2], table[3]))
        )
    return (place + k) % count


def in_order(own):
    count = lax.axis_size("tensor")
    place = lax.axis_index("tensor")
    if count == 4:
        right, left = line_streams(own)
        rows = []
        for want in range(4):
            pick = own
            for at in range(4):
                if at < want:
                    pick = jnp.where(place == at, left[want - at - 1], pick)
                elif at > want:
                    pick = jnp.where(place == at, right[at - want - 1], pick)
            rows.append(pick)
        return jnp.stack(rows, 0)
    return lax.all_gather(own, "tensor", axis=0)


def line_sum(own, parts):
    count = lax.axis_size("tensor")
    place = lax.axis_index("tensor")
    if count == 4:
        first, second, third = parts
        end = (place == 0) | (place == 3)
        right = along(third, [(0, 1)])
        left = along(third, [(3, 2)])
        arrived = jnp.where(place == 1, right, left)
        send = jnp.where(
            end, second, (third.astype(F32) + arrived.astype(F32)).astype(BF16)
        )
        right = along(send, [(0, 1), (1, 2)])
        left = along(send, [(3, 2), (2, 1)])
        send_right = (first.astype(F32) + right.astype(F32)).astype(BF16)
        send_left = (
            jnp.where(place == 3, first, second).astype(F32) + left.astype(F32)
        ).astype(BF16)
        right = along(send_right, [(0, 1), (1, 2), (2, 3)])
        left = along(send_left, [(3, 2), (2, 1), (1, 0)])
        return own.astype(F32) + right.astype(F32) + left.astype(F32)
    stack = jnp.zeros((count,) + own.shape, BF16)
    stack = lax.dynamic_update_index_in_dim(stack, own.astype(BF16), place, 0)
    for k in range(1, count):
        stack = lax.dynamic_update_index_in_dim(stack, parts[k - 1], label_index(k), 0)
    return lax.psum_scatter(stack, "tensor", scatter_dimension=0, tiled=False).astype(F32)


MESH = pl.DeviceIdType.MESH


def ring_places():
    s, t = lax.axis_index("seq"), lax.axis_index("tensor")
    c, x, y = s % 2, (s // 2) % 2, s // 4
    return s, t, c, x, y


def greet(targets):
    barrier = pltpu.get_barrier_semaphore()
    for target in targets:
        pl.semaphore_signal(barrier, inc=1, device_id=target, device_id_type=MESH)
    pl.semaphore_wait(barrier, len(targets))


def gather_kernel(count, *refs):
    weights, cot = refs[:count], refs[count]
    full, cots = refs[count + 1 : 2 * count + 1], refs[2 * count + 1]
    rest = refs[2 * count + 2 :]
    stage, (cot_stage, local_sem, send_sem, recv_sem, cot_send, cot_recv) = rest[:count], rest[count:]
    s, t, c, x, y = ring_places()
    s_core, s_x, s_y = s + 1 - 2 * c, s + 2 - 4 * x, s + 4 - 8 * y
    s_far = s_x + 4 - 8 * y
    right, left = (s, t + 1), (s, t - 1)
    near_x, near_y, core = (s_x, t), (s_y, t), (s_core, t)
    greet([(s, (t + 1) % 4), (s, (t + 3) % 4), near_x, near_y, core])
    sent = []

    def slot(w, tt, ss):
        return full[w].at[:, tt, ss]

    def copy(w, src, tt, ss, kind, target):
        return pltpu.make_async_remote_copy(
            src_ref=src, dst_ref=slot(w, tt, ss), send_sem=send_sem.at[w, tt, kind],
            recv_sem=recv_sem.at[w, tt, ss], device_id=target, device_id_type=MESH,
        )

    def arrived(w, tt, ss):
        copy(w, slot(w, tt, ss), tt, ss, 0, core).wait_recv()

    def send(w, src, tt, ss, kind, target, when=None):
        def go():
            copy(w, src, tt, ss, kind, target).start()

        def done():
            copy(w, src, tt, ss, kind, target).wait_send()

        if when is None:
            go()
            sent.append(done)
        else:
            pl.when(when)(go)
            sent.append(lambda: pl.when(when)(done))

    def spread(w, src, tt):
        send(w, src, tt, s, 2, near_x)
        send(w, src, tt, s, 3, near_y)
        send(w, src, tt, s, 4, core)

    def open_line(w):
        own = weights[w].at[:, s]
        send(w, own, t, s, 0, right, t < 3)
        send(w, own, t, s, 1, left, t > 0)
        spread(w, own, t)

    def line_events(w):
        for k in (1, 2, 3):
            for way in (-1, 1):
                tt = t + way * k

                def event(tt=tt, way=way, tail=sent):
                    arrived(w, tt, s)
                    if way < 0:
                        pl.when(t < 3)(lambda: copy(w, slot(w, tt, s), tt, s, 0, right).start())
                    else:
                        pl.when(t > 0)(lambda: copy(w, slot(w, tt, s), tt, s, 1, left).start())
                    copy(w, slot(w, tt, s), tt, s, 2, near_x).start()
                    copy(w, slot(w, tt, s), tt, s, 3, near_y).start()
                    copy(w, slot(w, tt, s), tt, s, 4, core).start()

                def finish(tt=tt, way=way):
                    if way < 0:
                        pl.when(t < 3)(lambda: copy(w, slot(w, tt, s), tt, s, 0, right).wait_send())
                    else:
                        pl.when(t > 0)(lambda: copy(w, slot(w, tt, s), tt, s, 1, left).wait_send())
                    for kind, target in ((2, near_x), (3, near_y), (4, core)):
                        copy(w, slot(w, tt, s), tt, s, kind, target).wait_send()

                ok = tt >= 0 if way < 0 else tt <= 3
                pl.when(ok)(event)
                sent.append(lambda ok=ok, finish=finish: pl.when(ok)(finish))

    def plane_events(w):
        for tt in range(4):
            arrived(w, tt, s_x)
            send(w, slot(w, tt, s_x), tt, s_x, 6, core)
            if tt % 2 == 0:
                send(w, slot(w, tt, s_x), tt, s_x, 5, near_y)
            arrived(w, tt, s_y)
            send(w, slot(w, tt, s_y), tt, s_y, 8, core)
            if tt % 2 == 1:
                send(w, slot(w, tt, s_y), tt, s_y, 7, near_x)

    def far_events(w):
        for tt in range(4):
            arrived(w, tt, s_far)
            send(w, slot(w, tt, s_far), tt, s_far, 9, core)

    def core_events(w):
        for tt in range(4):
            for base in (s, s_x, s_y, s_far):
                arrived(w, tt, base + 1 - 2 * c)

    def cot_copy(src, tt, kind, target):
        return pltpu.make_async_remote_copy(
            src_ref=src, dst_ref=cots.at[tt], send_sem=cot_send.at[tt, kind],
            recv_sem=cot_recv.at[tt], device_id=target, device_id_type=MESH,
        )

    def cot_open():
        pl.when(t < 3)(lambda: cot_copy(cot, t, 0, right).start())
        pl.when(t > 0)(lambda: cot_copy(cot, t, 1, left).start())
        sent.append(lambda: pl.when(t < 3)(lambda: cot_copy(cot, t, 0, right).wait_send()))
        sent.append(lambda: pl.when(t > 0)(lambda: cot_copy(cot, t, 1, left).wait_send()))

    def cot_events(k):
        for way in (-1, 1):
            tt = t + way * k
            kind, target = (0, right) if way < 0 else (1, left)
            more = t < 3 if way < 0 else t > 0

            def event(tt=tt, kind=kind, target=target, more=more):
                cot_copy(cots.at[tt], tt, kind, target).wait_recv()
                pl.when(more)(lambda: cot_copy(cots.at[tt], tt, kind, target).start())

            def finish(tt=tt, kind=kind, target=target, more=more):
                pl.when(more)(lambda: cot_copy(cots.at[tt], tt, kind, target).wait_send())

            ok = tt >= 0 if way < 0 else tt <= 3
            pl.when(ok)(event)
            sent.append(lambda ok=ok, finish=finish: pl.when(ok)(finish))

    into = [pltpu.make_async_copy(weights[w].at[:, s], stage[w], local_sem.at[w]) for w in range(count)]
    into.append(pltpu.make_async_copy(cot, cot_stage, local_sem.at[count]))
    out = [pltpu.make_async_copy(stage[w], slot(w, t, s), local_sem.at[w]) for w in range(count)]
    out.append(pltpu.make_async_copy(cot_stage, cots.at[t], local_sem.at[count]))

    for w in range(count):
        open_line(w)
    for move in into:
        move.start()
    line_events(0)
    line_events(1)
    for a, b in zip(into, out):
        a.wait()
        b.start()
    cot_open()
    plane_events(0)
    line_events(2)
    far_events(0)
    plane_events(1)
    line_events(3)
    far_events(1)
    cot_events(1)
    plane_events(2)
    far_events(2)
    cot_events(2)
    plane_events(3)
    cot_events(3)
    far_events(3)
    for w in range(count):
        core_events(w)
    for move in out:
        move.wait()
    for done in sent:
        done()


def gather_all(weights, cotangent):
    n_ten, n_seq = lax.axis_size("tensor"), lax.axis_size("seq")
    if not (n_ten == 4 and n_seq == 8):
        full = [jnp.moveaxis(lax.all_gather(w, "tensor", axis=0), 0, 1) for w in weights]
        return full, lax.all_gather(cotangent, "tensor", axis=0)
    count = len(weights)
    cut = [w.reshape(w.shape[0], 8, w.shape[1] // 8, w.shape[2]) for w in weights]
    anywhere = pl.BlockSpec(memory_space=pl.ANY)
    outs = [jax.ShapeDtypeStruct((w.shape[0], 4) + w.shape[1:], w.dtype) for w in cut]
    outs.append(jax.ShapeDtypeStruct((4,) + cotangent.shape, cotangent.dtype))
    got = pl.pallas_call(
        functools.partial(gather_kernel, count),
        out_shape=outs,
        in_specs=[anywhere] * (count + 1),
        out_specs=[anywhere] * (count + 1),
        scratch_shapes=[pltpu.VMEM((w.shape[0],) + w.shape[2:], w.dtype) for w in cut]
        + [
            pltpu.VMEM(cotangent.shape, cotangent.dtype),
            pltpu.SemaphoreType.DMA((count + 1,)),
            pltpu.SemaphoreType.DMA((count, 4, 10)),
            pltpu.SemaphoreType.DMA((count, 4, 8)),
            pltpu.SemaphoreType.DMA((4, 2)),
            pltpu.SemaphoreType.DMA((4,)),
        ],
        compiler_params=pltpu.CompilerParams(collective_id=1, has_side_effects=True),
        name="gather",
    )(*cut, cotangent)
    full = [g.reshape(w.shape[0], 4, w.shape[1], w.shape[2]) for g, w in zip(got, weights)]
    return full, got[count]


def carry_kernel(reach, reverse, carry_ref, out_ref, send_sem, recv_sem):
    n_ten = lax.axis_size("tensor")
    devices = n_ten * lax.axis_size("seq")
    me = lax.axis_index("seq") * n_ten + lax.axis_index("tensor")
    way = -1 if reverse else 1

    def place(linear):
        return linear // n_ten, linear % n_ten

    greet([place((me - way * k + devices) % devices) for k in range(1, reach + 1)])

    def copy(k):
        return pltpu.make_async_remote_copy(
            src_ref=carry_ref, dst_ref=out_ref.at[k - 1], send_sem=send_sem.at[k - 1],
            recv_sem=recv_sem.at[k - 1], device_id=place((me + way * k + devices) % devices),
            device_id_type=MESH,
        )

    def there(k, back):
        spot = me - way * k if back else me + way * k
        return (spot >= 0) & (spot < devices)

    for k in range(1, reach + 1):
        pl.when(there(k, False))(lambda k=k: copy(k).start())
    for k in range(1, reach + 1):
        pl.when(there(k, True))(lambda k=k: copy(k).wait_recv())
        pl.when(there(k, False))(lambda k=k: copy(k).wait_send())


def entering(carry, reach, linear, devices, reverse):
    channels = carry.shape[1]
    vmem = pl.BlockSpec(memory_space=pltpu.VMEM)
    got = pl.pallas_call(
        functools.partial(carry_kernel, reach, reverse),
        out_shape=jax.ShapeDtypeStruct((reach, 2, channels), F32),
        in_specs=[vmem],
        out_specs=vmem,
        scratch_shapes=[pltpu.SemaphoreType.DMA((reach,)), pltpu.SemaphoreType.DMA((reach,))],
        compiler_params=pltpu.CompilerParams(
            collective_id=3 if reverse else 2, has_side_effects=True
        ),
        name="carry_back" if reverse else "carry",
    )(carry)
    state = jnp.zeros((1, channels), F32)
    for k in range(reach, 0, -1):
        source = linear + k if reverse else linear - k
        there = (source >= 0) & (source < devices)
        state = jnp.where(there, got[k - 1, 0:1] * state + got[k - 1, 1:2], state)
    return state


def pick4(t, a, b, c, d):
    return jnp.where(t == 0, a, jnp.where(t == 1, b, jnp.where(t == 2, c, d)))


def reduce_kernel(count, rows, cols, blocks, out_ref, *refs):
    (
        top_x, low_y, mine, far_x, far_y, from_x, from_y, total,
        line_send, line_recv, load_sem, out_sem, send_sem, recv_sem, zs_sem, zr_sem,
    ) = refs
    s, t, c, x, y = ring_places()
    p = s // 2
    p_x, p_y = p + 1 - 2 * x, p + 2 - 4 * y
    p_far = p_x + 2 - 4 * y
    near_x, near_y = (s + 2 - 4 * x, t), (s + 4 - 8 * y, t)
    right, left = (s, t + 1), (s, t - 1)
    greet([(s, (t + 1) % 4), (s, (t + 3) % 4), near_x, near_y])
    half = rows // 2
    order = (pick4(t, 3, 3, 0, 0), pick4(t, 2, 0, 1, 1), pick4(t, 1, 2, 3, 2), t)
    work = [(w, i) for w in range(count) for i in range(4)]

    def block(w, i, q, lower, tall):
        column = pl.multiple_of(order[i] * cols, 128)
        row = pl.multiple_of(64 * c + lower * half, 16)
        return blocks.at[w, q, pl.ds(row, tall), pl.ds(column, cols)]

    def loads(n):
        w, i = work[n]
        return (
            pltpu.make_async_copy(block(w, i, p_x, 1, half), top_x.at[n], load_sem.at[n, 0]),
            pltpu.make_async_copy(block(w, i, p_y, 0, half), low_y.at[n], load_sem.at[n, 1]),
            pltpu.make_async_copy(block(w, i, p, 0, rows), mine.at[n], load_sem.at[n, 2]),
        )

    def remote(n, src, dst, k, target):
        return pltpu.make_async_remote_copy(
            src_ref=src, dst_ref=dst, send_sem=send_sem.at[n, k], recv_sem=recv_sem.at[n, k],
            device_id=target, device_id_type=MESH,
        )

    def directs(n):
        w, i = work[n]
        return (
            remote(n, block(w, i, p_far, 0, half), far_x.at[n], 0, near_x),
            remote(n, block(w, i, p_far, 1, half), far_y.at[n], 1, near_y),
            remote(n, block(w, i, p_x, 0, half), from_x.at[n, pl.ds(0, half)], 2, near_x),
            remote(n, block(w, i, p_y, 1, half), from_y.at[n, pl.ds(half, half)], 3, near_y),
        )

    def seconds(n):
        return (
            remote(n, top_x.at[n], from_x.at[n, pl.ds(half, half)], 4, near_x),
            remote(n, low_y.at[n], from_y.at[n, pl.ds(0, half)], 5, near_y),
        )

    def begin(n):
        if n < len(work):
            for move in loads(n) + directs(n):
                move.start()

    def forward(n):
        first, second = directs(n)[:2]
        a, b = loads(n)[:2]
        b.wait()
        first.wait_recv()
        low_y[n] = (low_y[n].astype(F32) + far_x[n].astype(F32)).astype(BF16)
        seconds(n)[1].start()
        a.wait()
        second.wait_recv()
        top_x[n] = (top_x[n].astype(F32) + far_y[n].astype(F32)).astype(BF16)
        seconds(n)[0].start()

    def hop(w, k, target, way):
        return pltpu.make_async_remote_copy(
            src_ref=line_send.at[w, k], dst_ref=line_recv.at[w, k], send_sem=zs_sem.at[w, k],
            recv_sem=zr_sem.at[w, k], device_id=target, device_id_type=MESH,
        )

    def finish(n):
        w, i = work[n]
        loads(n)[2].wait()
        for move in directs(n)[2:] + seconds(n):
            move.wait_recv()
        value = (
            mine[n].astype(F32) + from_x[n].astype(F32) + from_y[n].astype(F32)
        )
        if i == 0:

            @pl.when(t == 0)
            def _():
                line_send[w, 0] = value.astype(BF16)
                hop(w, 0, right, 0).start()

            @pl.when(t == 3)
            def _():
                line_send[w, 1] = value.astype(BF16)
                hop(w, 1, left, 1).start()

            @pl.when(t == 1)
            def _():
                hop(w, 0, right, 0).wait_recv()
                line_send[w, 2] = (value + line_recv[w, 0].astype(F32)).astype(BF16)
                hop(w, 2, right, 0).start()

            @pl.when(t == 2)
            def _():
                hop(w, 1, left, 1).wait_recv()
                line_send[w, 3] = (value + line_recv[w, 1].astype(F32)).astype(BF16)
                hop(w, 3, left, 1).start()

        if i == 1:

            @pl.when(t == 0)
            def _():
                line_send[w, 2] = value.astype(BF16)
                hop(w, 2, right, 0).start()

            @pl.when(t == 3)
            def _():
                line_send[w, 3] = value.astype(BF16)
                hop(w, 3, left, 1).start()

            @pl.when((t == 1) | (t == 2))
            def _():
                hop(w, 3, left, 1).wait_recv()
                line_send[w, 5] = (value + line_recv[w, 3].astype(F32)).astype(BF16)
                hop(w, 5, left, 1).start()

        if i == 2:

            @pl.when(t == 0)
            def _():
                line_send[w, 4] = value.astype(BF16)
                hop(w, 4, right, 0).start()

            @pl.when(t == 3)
            def _():
                line_send[w, 5] = value.astype(BF16)
                hop(w, 5, left, 1).start()

            @pl.when((t == 1) | (t == 2))
            def _():
                hop(w, 2, right, 0).wait_recv()
                line_send[w, 4] = (value + line_recv[w, 2].astype(F32)).astype(BF16)
                hop(w, 4, right, 0).start()

        if i == 3:
            total[w] = value

    def close(w):
        @pl.when(t > 0)
        def _():
            hop(w, 4, right, 0).wait_recv()
            total[w] = total[w] + line_recv[w, 4].astype(F32)

        @pl.when(t < 3)
        def _():
            hop(w, 5, left, 1).wait_recv()
            total[w] = total[w] + line_recv[w, 5].astype(F32)

        pltpu.make_async_copy(total.at[w], out_ref.at[w], out_sem.at[w]).start()

    for n in range(3):
        begin(n)
    for n in range(len(work)):
        forward(n)
        begin(n + 3)
        if n >= 2:
            finish(n - 2)
    finish(len(work) - 2)
    finish(len(work) - 1)
    for w in range(count):
        close(w)
    for n in range(len(work)):
        for move in directs(n) + seconds(n):
            move.wait_send()
    for w in range(count):
        for k, ok in (
            (0, t == 0), (1, t == 3), (2, t < 2), (3, t > 1), (4, t < 3), (5, t > 0),
        ):
            pl.when(ok)(lambda k=k: hop(w, k, right, 0).wait_send())
        pltpu.make_async_copy(total.at[w], out_ref.at[w], out_sem.at[w]).wait()


def reduce_all(blocks, cols, number):
    count = blocks.shape[0]
    rows = blocks.shape[2] - 64
    half, steps = rows // 2, 4 * count
    anywhere = pl.BlockSpec(memory_space=pl.ANY)

    def room(*dims):
        return pltpu.VMEM(dims, BF16)

    return pl.pallas_call(
        functools.partial(reduce_kernel, count, rows, cols),
        out_shape=jax.ShapeDtypeStruct((count, rows, cols), F32),
        in_specs=[anywhere],
        out_specs=anywhere,
        scratch_shapes=[
            room(steps, half, cols), room(steps, half, cols), room(steps, rows, cols),
            room(steps, half, cols), room(steps, half, cols),
            room(steps, rows, cols), room(steps, rows, cols),
            pltpu.VMEM((count, rows, cols), F32),
            room(count, 6, rows, cols), room(count, 6, rows, cols),
            pltpu.SemaphoreType.DMA((steps, 3)),
            pltpu.SemaphoreType.DMA((count,)),
            pltpu.SemaphoreType.DMA((steps, 6)),
            pltpu.SemaphoreType.DMA((steps, 6)),
            pltpu.SemaphoreType.DMA((count, 6)),
            pltpu.SemaphoreType.DMA((count, 6)),
        ],
        compiler_params=pltpu.CompilerParams(
            collective_id=number, has_side_effects=True, vmem_limit_bytes=60 << 20
        ),
        name="reduce",
    )(blocks)


def flip_core(block):
    count = lax.axis_size("seq")
    return lax.ppermute(block, "seq", [(i, i + 1 - 2 * (i % 2)) for i in range(count)])


def chunk_scan(a_ref, d_ref, p_ref, s_ref, reverse):
    tiles, rows, wide = a_ref.shape
    run = rows // 8

    def first(i, carry):
        r = run - 1 - i if reverse else i
        here = pl.ds(r, 8, stride=run)
        after = []
        for b in range(tiles):
            prod, state = carry[b]
            a = a_ref[b, here, :]
            prod = prod * a
            state = a * state + d_ref[b, here, :]
            a_ref[b, here, :] = prod
            d_ref[b, here, :] = state
            after.append((prod, state))
        return tuple(after)

    start = (jnp.ones((8, wide), F32), jnp.zeros((8, wide), F32))
    ends = lax.fori_loop(0, run, first, (start,) * tiles, unroll=4)
    leads, totals = [], []
    for b in range(tiles):
        prod, state = ends[b]
        enter_p, enter_s = [None] * 8, [None] * 8
        now_p, now_s = jnp.ones((1, wide), F32), jnp.zeros((1, wide), F32)
        for c in range(7, -1, -1) if reverse else range(8):
            enter_p[c], enter_s[c] = now_p, now_s
            now_p, now_s = now_p * prod[c : c + 1], prod[c : c + 1] * now_s + state[c : c + 1]
        leads.append((jnp.concatenate(enter_p, 0), jnp.concatenate(enter_s, 0)))
        totals.append((now_p, now_s))

    def second(r, _):
        here = pl.ds(r, 8, stride=run)
        for b in range(tiles):
            p = a_ref[b, here, :]
            a_ref[b, here, :] = p * leads[b][0]
            d_ref[b, here, :] = d_ref[b, here, :] + p * leads[b][1]
        return 0

    lax.fori_loop(0, run, second, 0, unroll=4)
    for b in range(tiles):
        p_ref[:, b * wide : (b + 1) * wide] = a_ref[b]
        s_ref[:, b * wide : (b + 1) * wide] = d_ref[b]
    return jnp.concatenate([p for p, _ in totals], 1), jnp.concatenate([v for _, v in totals], 1)


def tiled_store(ref, value):
    tiles, _, wide = ref.shape
    for b in range(tiles):
        ref[b] = value[:, b * wide : (b + 1) * wide]


def positions(base_ref, rows, lanes, length):
    place = lax.broadcasted_iota(jnp.int32, (rows, lanes), 0) + base_ref[0]
    return jnp.where(place >= length, place - length, place)


def forward_kernel(
    length, local, base_ref, x_ref, cw_ref, rate_gain_ref, g_ref, sel_ref,
    conv_ref, rate_ref, in_ref, p_ref, s_ref, carry_ref, w_ref, a_ref, d_ref,
):
    rows, lanes = conv_ref.shape
    spot = positions(base_ref, rows, lanes, length)
    x = x_ref[...].astype(F32)
    total = cw_ref[0:1, :] * x[HALO:]
    for k in range(1, CONV):
        moved = pltpu.roll(x, k, 0)[HALO:]
        total = total + jnp.where(spot >= k, cw_ref[k : k + 1, :] * moved, 0.0)
    conv = total.astype(BF16)
    conv_ref[...] = conv
    join = sel_ref.shape[0]
    wide = jnp.dot(g_ref[0], sel_ref[0], preferred_element_type=F32)
    for q in range(1, join):
        other = jnp.dot(g_ref[0], sel_ref[q], preferred_element_type=F32)
        which = lax.broadcasted_iota(jnp.int32, wide.shape, 0) // local % join
        wide = jnp.where(which == q, other, wide)
    gates = wide.astype(BF16)
    w_ref[0] = gates
    pre = lax.dot_general(conv, gates, (((1,), (1,)), ((), ())), preferred_element_type=F32)
    rate, inp = pre[:, :lanes], pre[:, lanes:]
    rate_ref[...] = rate
    in_ref[...] = inp
    decay = jnp.where(spot == 0, 0.0, jnp.exp(rate_gain_ref[...] * jax.nn.sigmoid(rate)))
    tiled_store(a_ref, decay)
    tiled_store(
        d_ref,
        jnp.sqrt(jnp.maximum(1.0 - decay * decay, 0.01)) * jax.nn.sigmoid(inp) * conv.astype(F32),
    )
    prod, state = chunk_scan(a_ref, d_ref, p_ref, s_ref, False)
    carry_ref[0:1, :] = prod
    carry_ref[1:2, :] = state


def middle_kernel(
    length, base_ref, mg_ref, y_ref, p_ref, s_ref, enter_ref, rate_ref, rate_gain_ref,
    ylow_ref, bp_ref, bs_ref, carry_ref, a_ref, d_ref,
):
    rows, lanes = mg_ref.shape
    spot = positions(base_ref, rows, lanes, length)
    states = s_ref[...] + p_ref[...] * enter_ref[...]
    value, slope = gelu_both(y_ref[...])
    grad = mg_ref[...]
    ylow_ref[...] = (grad * states * slope).astype(BF16)
    tiled_store(d_ref, grad * value)
    decay = jnp.where(spot == 0, 0.0, jnp.exp(rate_gain_ref[...] * jax.nn.sigmoid(rate_ref[...])))
    row = lax.broadcasted_iota(jnp.int32, (rows, lanes), 0)
    tiled_store(a_ref, jnp.where(row == rows - 1, 1.0, pltpu.roll(decay, rows - 1, 0)))
    prod, state = chunk_scan(a_ref, d_ref, bp_ref, bs_ref, True)
    carry_ref[0:1, :] = decay[0:1] * prod
    carry_ref[1:2, :] = decay[0:1] * state


def backward_kernel(
    length, local, base_ref, bp_ref, bs_ref, leave_ref, p_ref, s_ref, enter_ref, rate_ref, in_ref,
    conv_ref, rate_gain_ref, w_ref, cw_ref, x_ref, sel_ref,
    gates_ref, xback_ref, edge_ref, small_ref,
):
    rows, lanes = bp_ref.shape
    spot = positions(base_ref, rows, lanes, length)
    row = lax.broadcasted_iota(jnp.int32, (rows, lanes), 0)
    adjoint = bs_ref[...] + bp_ref[...] * leave_ref[...]
    states = s_ref[...] + p_ref[...] * enter_ref[...]
    before = jnp.where(row == 0, enter_ref[...], pltpu.roll(states, 1, 0))
    gain = rate_gain_ref[...]
    sig_r = jax.nn.sigmoid(rate_ref[...])
    sig_i = jax.nn.sigmoid(in_ref[...])
    conv = conv_ref[...]
    conv_f = conv.astype(F32)
    decay = jnp.where(spot == 0, 0.0, jnp.exp(gain * sig_r))
    room = 1.0 - decay * decay
    scale = jnp.sqrt(jnp.maximum(room, 0.01))
    pulled = adjoint * sig_i
    slope = jnp.where(room > 0.01, -decay / scale, 0.0)
    decay_grad = adjoint * before + pulled * conv_f * slope
    log_grad = decay_grad * decay
    pull_r = log_grad * sig_r
    rate_back = (pull_r * gain * (1.0 - sig_r)).astype(BF16)
    conv_direct = pulled * scale
    in_back = (conv_direct * conv_f * (1.0 - sig_i)).astype(BF16)
    both = jnp.concatenate([rate_back, in_back], 1)
    join = sel_ref.shape[0]
    for q in range(join):
        some = lax.dot_general(
            conv, sel_ref[q], (((1,), (1,)), ((), ())), preferred_element_type=F32
        ).astype(BF16)
        part = lax.dot_general(both, some, (((0,), (0,)), ((), ())), preferred_element_type=F32)
        if q == 0:
            gate_sum = part
        else:
            which = lax.broadcasted_iota(jnp.int32, part.shape, 0) // local % join
            gate_sum = jnp.where(which == q, part, gate_sum)
    gates_ref[0] = gate_sum.astype(BF16)
    grad = conv_direct + lax.dot_general(
        both, w_ref[0], (((1,), (0,)), ((), ())), preferred_element_type=F32
    )
    x = x_ref[...].astype(F32)
    zeros = jnp.zeros((HALO, lanes), F32)
    out = jnp.concatenate([zeros, grad * cw_ref[0:1, :]], 0)
    small_ref[0:1, :] = jnp.sum(grad * x[HALO:], axis=0, keepdims=True)
    for k in range(1, CONV):
        masked = jnp.where(spot >= k, grad, 0.0)
        small_ref[k : k + 1, :] = jnp.sum(
            masked * pltpu.roll(x, k, 0)[HALO:], axis=0, keepdims=True
        )
        tall = jnp.concatenate([zeros, masked * cw_ref[k : k + 1, :]], 0)
        out = out + pltpu.roll(tall, rows + HALO - k, 0)
    small_ref[CONV : CONV + 1, :] = jnp.sum(pull_r, axis=0, keepdims=True)
    small_ref[CONV + 1 : 8, :] = jnp.zeros((7 - CONV, lanes), F32)
    edge_ref[...] = out[:HALO]
    xback_ref[...] = out[HALO:]


def lane_call(kernel, grid, lanes, base, operands, outputs, scratch, flops):
    def spec(shape):
        if len(shape) == 3 and shape[0] != grid:
            return pl.BlockSpec(shape, lambda j, *_: (0, 0, 0))
        if len(shape) == 3:
            return pl.BlockSpec((1,) + shape[1:], lambda j, *_: (j, 0, 0))
        return pl.BlockSpec((shape[0], lanes), lambda j, *_: (0, j))

    moved = sum(math.prod(a.shape) * a.dtype.itemsize for a in list(operands) + list(outputs))
    return pl.pallas_call(
        kernel,
        grid_spec=pltpu.PrefetchScalarGridSpec(
            num_scalar_prefetch=1,
            grid=(grid,),
            in_specs=[spec(a.shape) for a in operands],
            out_specs=[spec(a.shape) for a in outputs],
            scratch_shapes=scratch,
        ),
        out_shape=outputs,
        compiler_params=pltpu.CompilerParams(
            dimension_semantics=("arbitrary",), vmem_limit_bytes=56 << 20
        ),
        cost_estimate=pl.CostEstimate(flops=flops, bytes_accessed=moved, transcendentals=0),
    )(base, *operands)


def weight_grads(pairs):
    n_ten, n_seq = lax.axis_size("tensor"), lax.axis_size("seq")
    if n_ten == 4 and n_seq == 8:
        core = lax.axis_index("seq") % 2
        share = pairs[0][0].shape[1] // n_seq
        blocks = []
        for a, b in pairs:
            a = jnp.concatenate([a, flip_core(a)], 0)
            b = jnp.concatenate([b, flip_core(b)], 0)
            windows = [
                lax.dynamic_slice_in_dim(a, 2 * share * q + (share - 64) * core, share + 64, 1)
                for q in range(4)
            ]
            blocks.append(dot_tn(jnp.concatenate(windows, 1), b).astype(BF16))
        blocks = jnp.stack(blocks, 0).reshape(len(pairs), 4, share + 64, -1)
        return reduce_all(blocks, blocks.shape[3] // n_ten, 4)
    out = []
    for a, b in pairs:
        grad = lax.psum_scatter(dot_tn(a, b).astype(BF16), "seq", scatter_dimension=0, tiled=True)
        out.append(lax.psum_scatter(grad, "tensor", scatter_dimension=1, tiled=True).astype(F32))
    return out


def shards(
    tokens_in, gain_pre, w_x, w_y, conv_w, gate_a, gate_i, decay_param, w_out,
    gain_mlp, w_gate, w_up, w_down, cotangent,
):
    rows, width = tokens_in.shape
    heads, local = w_x.shape[1:]
    n_ten, n_seq = lax.axis_size("tensor"), lax.axis_size("seq")
    devices = n_ten * n_seq
    place, run = lax.axis_index("tensor"), lax.axis_index("seq")
    linear = run * n_ten + place
    length = devices * rows // SEQS
    base = jnp.reshape((linear * rows) % length, (1,)).astype(jnp.int32)
    join = 128 // local if local < 128 and heads % (128 // local) == 0 else 1
    groups, chunk = heads // join, join * local
    lanes = n_ten * chunk
    channels = groups * lanes

    def shape(dims, kind=F32):
        return jax.ShapeDtypeStruct(dims, kind)

    def columns(local_array):
        n = local_array.shape[0]
        whole = lax.all_gather(local_array.reshape(n, groups, chunk), "tensor", axis=2)
        return whole.reshape(n, channels)

    def own_columns(array):
        n = array.shape[0]
        split = array.reshape(n, groups, n_ten, chunk)
        return lax.dynamic_index_in_dim(split, place, 2, False).reshape(n, heads, local)

    def by_place(array):
        return jnp.concatenate(
            [
                array[:, (j * n_ten + t) * chunk : (j * n_ten + t + 1) * chunk]
                for t in range(n_ten)
                for j in range(groups)
            ],
            1,
        )

    gate_rows = jnp.stack([gate_a, gate_i], 0).swapaxes(2, 3).reshape(2 * heads, local, n_ten * local)
    (all_gates, full_x, full_y, full_out), cots = gather_all(
        [
            gate_rows,
            jnp.transpose(w_x, (1, 2, 0)).reshape(groups, chunk, width),
            jnp.transpose(w_y, (1, 2, 0)).reshape(groups, chunk, width),
            w_out.reshape(groups, chunk, width),
        ],
        cotangent,
    )
    full_x, full_y, full_out = (w.reshape(channels, width) for w in (full_x, full_y, full_out))
    gates = all_gates.reshape(2, groups, join, n_ten, local, n_ten * local)
    gates = jnp.transpose(gates, (1, 0, 3, 2, 4, 5)).reshape(groups, 2 * lanes, n_ten * local)
    key = jnp.arange(n_ten * local)[None, :, None]
    lane = jnp.arange(lanes)[None, None, :]
    member = jnp.arange(join)[:, None, None]
    select = (
        (lane // chunk == key // local) & (lane % local == key % local) & (lane // local % join == member)
    ).astype(BF16)
    small = columns(jnp.concatenate([conv_w, decay_param[None]], 0))
    conv_full, decay_full = small[:CONV], small[CONV : CONV + 1]
    conv_rows = jnp.concatenate([conv_full, jnp.zeros((8 - CONV, channels), F32)], 0)
    rate_gain = -8.0 * jax.nn.softplus(decay_full)

    halo = lax.ppermute(tokens_in[rows - HALO :], BOTH, [(i, i + 1) for i in range(devices - 1)])
    own_in = tokens_in.astype(F32)
    in_scale, in_unit = rms_parts(own_in)
    normed = (in_unit * gain_pre).astype(BF16)
    normed_halo = (rms_parts(halo.astype(F32))[1] * gain_pre).astype(BF16)
    x_long = dot_nt(jnp.concatenate([normed_halo, normed], 0), full_x).astype(BF16)
    y_branch = dot_nt(normed, full_y)
    scratch = [pltpu.VMEM((lanes // 128, rows, 128), F32)] * 2
    conv_out, rate_pre, input_pre, products, partial, carry, wide_gates = lane_call(
        functools.partial(forward_kernel, length, local), groups, lanes, base,
        (x_long, conv_rows, rate_gain, gates, select),
        [
            shape((rows, channels), BF16),
            shape((rows, channels)),
            shape((rows, channels)),
            shape((rows, channels)),
            shape((rows, channels)),
            shape((2, channels)),
            shape((groups, 2 * lanes, lanes), BF16),
        ],
        scratch, 4 * rows * lanes * channels,
    )
    reach = min(-(-length // rows), devices - 1)
    enter = entering(carry, reach, linear, devices, False)
    states = partial + products * enter
    mixed = (states * jax.nn.gelu(y_branch, approximate=True)).astype(BF16)
    middle = own_in + dot_nn(mixed, full_out)
    mid_scale, mid_unit = rms_parts(middle)
    normed_mlp = (mid_unit * gain_mlp).astype(BF16)

    cots = [cotangent] + [
        lax.dynamic_index_in_dim(cots, label_index(k), 0, False) for k in range(1, n_ten)
    ]
    tokens = [normed_mlp] + others(normed_mlp)
    hiddens, gate_grads, up_grads, downs, pulls = [], [], [], [], []
    for n, c in zip(tokens, cots):
        gate_vals, up_vals = dot_nn(n, w_gate), dot_nn(n, w_up)
        value, slope = gelu_both(gate_vals)
        hidden = (value * up_vals).astype(BF16)
        hidden_grad = dot_nt(c, w_down)
        gate_grad = (hidden_grad * up_vals * slope).astype(BF16)
        up_grad = (hidden_grad * value).astype(BF16)
        hiddens.append(hidden)
        gate_grads.append(gate_grad)
        up_grads.append(up_grad)
        pulls.append(dot_nt(gate_grad, w_gate) + dot_nt(up_grad, w_up))
        downs.append(dot_nn(hidden, w_down))
    mlp_input = line_sum(pulls[0], [p.astype(BF16) for p in pulls[1:]])
    down = line_sum(downs[0], [d.astype(BF16) for d in downs[1:]])
    block_out = (middle + down).astype(BF16)

    cot_rows = jnp.concatenate(cots, 0)
    token_rows = jnp.concatenate(tokens, 0)
    hidden_rows = jnp.concatenate(hiddens, 0)
    grad_down = dot_tn(hidden_rows, cot_rows).astype(BF16)
    grad_gate = dot_tn(token_rows, jnp.concatenate(gate_grads, 0)).astype(BF16)
    grad_up = dot_tn(token_rows, jnp.concatenate(up_grads, 0)).astype(BF16)
    grad_down = lax.psum_scatter(grad_down, "seq", scatter_dimension=1, tiled=True)
    grad_gate = lax.psum_scatter(grad_gate, "seq", scatter_dimension=0, tiled=True)
    grad_up = lax.psum_scatter(grad_up, "seq", scatter_dimension=0, tiled=True)

    gain_mlp_part, mid_back = rms_back(mlp_input, gain_mlp, mid_scale, mid_unit)
    middle_grad = cotangent.astype(F32) + mid_back
    middle_low = middle_grad.astype(BF16)
    mixed_grad = dot_nt(middle_low, full_out)
    y_low, back_products, back_partial, carry = lane_call(
        functools.partial(middle_kernel, length), groups, lanes, base,
        (mixed_grad, y_branch, products, partial, enter, rate_pre, rate_gain),
        [
            shape((rows, channels), BF16),
            shape((rows, channels)),
            shape((rows, channels)),
            shape((2, channels)),
        ],
        scratch, 60 * rows * channels,
    )
    leave = entering(carry, reach, linear, devices, True)
    gate_parts, x_back, edge, sums = lane_call(
        functools.partial(backward_kernel, length, local), groups, lanes, base,
        (
            back_products, back_partial, leave, products, partial, enter, rate_pre, input_pre,
            conv_out, rate_gain, wide_gates, conv_rows, x_long, select,
        ),
        [
            shape((groups, 2 * lanes, n_ten * local), BF16),
            shape((rows, channels)),
            shape((HALO, channels)),
            shape((8, channels)),
        ],
        [], 8 * rows * lanes * channels,
    )
    edge = lax.ppermute(edge, BOTH, [(i + 1, i) for i in range(devices - 1)])
    x_low = jnp.concatenate(
        [x_back[: rows - HALO], x_back[rows - HALO :] + edge], 0
    ).astype(BF16)

    pairs = ((middle_low, mixed), (normed, y_low), (normed, x_low))
    grads = weight_grads([(a, by_place(b)) for a, b in pairs])
    grad_out, grad_y, grad_x = grads
    normed_grad = dot_nn(x_low, full_x) + dot_nn(y_low, full_y)
    gain_pre_part, in_back = rms_back(normed_grad, gain_pre, in_scale, in_unit)
    input_grad = middle_grad + in_back

    split = gate_parts.reshape(groups, 2, n_ten, join, local, n_ten * local)
    diagonal = jnp.transpose(split, (2, 1, 0, 3, 4, 5)).reshape(n_ten, 2 * heads * local, n_ten * local)
    gate_sum = lax.psum_scatter(diagonal, "tensor", scatter_dimension=0, tiled=False)
    gate_sum = lax.psum_scatter(gate_sum, "seq", scatter_dimension=1, tiled=True)
    gate_sum = jnp.swapaxes(gate_sum.reshape(2, heads, local, -1), 2, 3).astype(F32)
    packed = jnp.concatenate([sums[: CONV + 1], gain_pre_part[None], gain_mlp_part[None]], 0)
    packed = lax.psum(packed, BOTH)
    conv_sum = own_columns(packed[:CONV])
    decay_sum = own_columns(packed[CONV : CONV + 1] * (-8.0 * jax.nn.sigmoid(decay_full)))[0]
    share = local // n_seq
    grad_conv = lax.dynamic_slice_in_dim(conv_sum, run * share, share, 2)
    grad_decay = lax.dynamic_slice_in_dim(decay_sum, run * share, share, 1)
    grad_gain_mlp = lax.dynamic_slice_in_dim(
        packed[CONV + 2], run * (width // n_seq), width // n_seq, 0
    )

    def weight(grad):
        return grad.T.reshape(heads, local, -1)

    return (
        block_out,
        input_grad,
        packed[CONV + 1],
        jnp.transpose(weight(grad_x), (2, 0, 1)),
        jnp.transpose(weight(grad_y), (2, 0, 1)),
        grad_conv,
        gate_sum[0],
        gate_sum[1],
        grad_decay,
        weight(grad_out),
        grad_gain_mlp,
        grad_gate.astype(F32),
        grad_up.astype(F32),
        grad_down.astype(F32),
    )


def solution(mesh):
    placed = (
        P(("seq", "tensor"), None),
        P(),
        P(None, None, "tensor"),
        P(None, None, "tensor"),
        P(None, None, "tensor"),
        P(None, None, "tensor"),
        P(None, None, "tensor"),
        P(None, "tensor"),
        P(None, "tensor", None),
        P(),
        P(None, "tensor"),
        P(None, "tensor"),
        P("tensor", None),
        P(("seq", "tensor"), None),
    )
    return jax.shard_map(
        shards,
        mesh=mesh,
        in_specs=placed,
        out_specs=(
            P(("seq", "tensor"), None),
            P(("seq", "tensor"), None),
            P(),
            P("seq", None, "tensor"),
            P("seq", None, "tensor"),
            P(None, None, ("tensor", "seq")),
            P(None, "seq", "tensor"),
            P(None, "seq", "tensor"),
            P(None, ("tensor", "seq")),
            P(None, "tensor", "seq"),
            P("seq"),
            P("seq", "tensor"),
            P("seq", "tensor"),
            P("tensor", "seq"),
        ),
        check_vma=False,
    )
```

```python
import functools
import math

import jax
import jax.numpy as jnp
from jax import lax
from jax.experimental import pallas as pl
from jax.experimental.pallas import tpu as pltpu
from jax.sharding import PartitionSpec as P

CONV = 4
SEQS = 3
HALO = 16
epsilon = 1e-06
F32 = jnp.float32
BF16 = jnp.bfloat16
ROOT = math.sqrt(2.0 / math.pi)
BOTH = ("seq", "tensor")


def dot_nn(a, b):
    return lax.dot_general(a, b, (((1,), (0,)), ((), ())), preferred_element_type=F32)


def dot_nt(a, b):
    return lax.dot_general(a, b, (((1,), (1,)), ((), ())), preferred_element_type=F32)


def dot_tn(a, b):
    return lax.dot_general(a, b, (((0,), (0,)), ((), ())), preferred_element_type=F32)


def rms_parts(values):
    scale = lax.rsqrt(jnp.mean(values * values, axis=-1, keepdims=True) + epsilon)
    return scale, values * scale


def rms_back(grad, gain, scale, unit):
    pulled = gain * grad
    inner = jnp.mean(pulled * unit, axis=-1, keepdims=True)
    return jnp.sum(grad * unit, axis=0), scale * (pulled - unit * inner)


def gelu_both(v):
    inner = v * v
    th = jnp.tanh(ROOT * (v + 0.044715 * v * inner))
    half = 0.5 * (1.0 + th)
    slope = half + 0.5 * v * (1.0 - th * th) * (ROOT * (1.0 + 3 * 0.044715 * inner))
    return v * half, slope


LABELS = ((1, 2, 3, 2), (2, 0, 1, 1), (3, 3, 0, 0))


def along(block, pairs):
    return lax.ppermute(block, "tensor", pairs)


def line_streams(own):
    right, left = [], []
    right.append(along(own, [(0, 1), (1, 2), (2, 3)]))
    left.append(along(own, [(1, 0), (2, 1), (3, 2)]))
    right.append(along(right[0], [(1, 2), (2, 3)]))
    left.append(along(left[0], [(1, 0), (2, 1)]))
    right.append(along(right[1], [(2, 3)]))
    left.append(along(left[1], [(1, 0)]))
    return right, left


def others(own):
    count = lax.axis_size("tensor")
    place = lax.axis_index("tensor")
    if count == 4:
        right, left = line_streams(own)
        first = jnp.where(place == 3, right[0], left[0])
        second = jnp.where(place == 0, left[1], jnp.where(place == 3, right[1], right[0]))
        third = jnp.where(
            place == 0, left[2], jnp.where(place == 1, left[1], jnp.where(place == 2, right[1], right[2]))
        )
        return [first, second, third]
    whole = lax.all_gather(own, "tensor", axis=0)
    return [lax.dynamic_index_in_dim(whole, (place + k) % count, 0, False) for k in range(1, count)]


def label_index(k):
    count = lax.axis_size("tensor")
    place = lax.axis_index("tensor")
    if count == 4:
        table = LABELS[k - 1]
        return jnp.where(
            place == 0, table[0], jnp.where(place == 1, table[1], jnp.where(place == 2, table[2], table[3]))
        )
    return (place + k) % count


def in_order(own):
    count = lax.axis_size("tensor")
    place = lax.axis_index("tensor")
    if count == 4:
        right, left = line_streams(own)
        rows = []
        for want in range(4):
            pick = own
            for at in range(4):
                if at < want:
                    pick = jnp.where(place == at, left[want - at - 1], pick)
                elif at > want:
                    pick = jnp.where(place == at, right[at - want - 1], pick)
            rows.append(pick)
        return jnp.stack(rows, 0)
    return lax.all_gather(own, "tensor", axis=0)


def line_sum(own, parts):
    count = lax.axis_size("tensor")
    place = lax.axis_index("tensor")
    if count == 4:
        first, second, third = parts
        end = (place == 0) | (place == 3)
        right = along(third, [(0, 1)])
        left = along(third, [(3, 2)])
        arrived = jnp.where(place == 1, right, left)
        send = jnp.where(
            end, second, (third.astype(F32) + arrived.astype(F32)).astype(BF16)
        )
        right = along(send, [(0, 1), (1, 2)])
        left = along(send, [(3, 2), (2, 1)])
        send_right = (first.astype(F32) + right.astype(F32)).astype(BF16)
        send_left = (
            jnp.where(place == 3, first, second).astype(F32) + left.astype(F32)
        ).astype(BF16)
        right = along(send_right, [(0, 1), (1, 2), (2, 3)])
        left = along(send_left, [(3, 2), (2, 1), (1, 0)])
        return own.astype(F32) + right.astype(F32) + left.astype(F32)
    stack = jnp.zeros((count,) + own.shape, BF16)
    stack = lax.dynamic_update_index_in_dim(stack, own.astype(BF16), place, 0)
    for k in range(1, count):
        stack = lax.dynamic_update_index_in_dim(stack, parts[k - 1], label_index(k), 0)
    return lax.psum_scatter(stack, "tensor", scatter_dimension=0, tiled=False).astype(F32)


MESH = pl.DeviceIdType.MESH


def ring_places():
    s, t = lax.axis_index("seq"), lax.axis_index("tensor")
    c, x, y = s % 2, (s // 2) % 2, s // 4
    return s, t, c, x, y


def greet(targets):
    barrier = pltpu.get_barrier_semaphore()
    for target in targets:
        pl.semaphore_signal(barrier, inc=1, device_id=target, device_id_type=MESH)
    pl.semaphore_wait(barrier, len(targets))


def gather_kernel(count, *refs):
    weights, (small, cot, tokens) = refs[:count], refs[count : count + 3]
    full = refs[count + 3 : 2 * count + 3]
    smalls, cots, halo = refs[2 * count + 3 : 2 * count + 6]
    rest = refs[2 * count + 6 :]
    stage, rest = rest[: count + 2], rest[count + 2 :]
    local_sem, send_sem, recv_sem, line_send, line_recv, halo_sem = rest
    s, t, c, x, y = ring_places()
    s_core, s_x, s_y = s + 1 - 2 * c, s + 2 - 4 * x, s + 4 - 8 * y
    s_far = s_x + 4 - 8 * y
    right, left = (s, t + 1), (s, t - 1)
    near_x, near_y, core = (s_x, t), (s_y, t), (s_core, t)
    linear = 4 * s + t
    after, before = (linear + 1) % 32, (linear + 31) % 32
    greet(
        [(s, (t + 1) % 4), (s, (t + 3) % 4), near_x, near_y, core, (before // 4, before % 4)]
    )
    sent = []
    tail_rows = halo.shape[0]
    onward = pltpu.make_async_remote_copy(
        src_ref=tokens.at[pl.ds(tokens.shape[0] - tail_rows, tail_rows)], dst_ref=halo,
        send_sem=halo_sem.at[0], recv_sem=halo_sem.at[1],
        device_id=(after // 4, after % 4), device_id_type=MESH,
    )
    pl.when(linear < 31)(onward.start)

    def slot(w, tt, ss):
        return full[w].at[:, tt, ss]

    def copy(w, src, tt, ss, kind, target):
        return pltpu.make_async_remote_copy(
            src_ref=src, dst_ref=slot(w, tt, ss), send_sem=send_sem.at[w, tt, kind],
            recv_sem=recv_sem.at[w, tt, ss], device_id=target, device_id_type=MESH,
        )

    def arrived(w, tt, ss):
        copy(w, slot(w, tt, ss), tt, ss, 0, core).wait_recv()

    def send(w, src, tt, ss, kind, target, when=None):
        def go():
            copy(w, src, tt, ss, kind, target).start()

        def done():
            copy(w, src, tt, ss, kind, target).wait_send()

        if when is None:
            go()
            sent.append(done)
        else:
            pl.when(when)(go)
            sent.append(lambda: pl.when(when)(done))

    def spread(w, src, tt):
        send(w, src, tt, s, 2, near_x)
        send(w, src, tt, s, 3, near_y)
        send(w, src, tt, s, 4, core)

    def open_line(w):
        own = weights[w].at[:, s]
        send(w, own, t, s, 0, right, t < 3)
        send(w, own, t, s, 1, left, t > 0)
        spread(w, own, t)

    def line_events(w):
        for k in (1, 2, 3):
            for way in (-1, 1):
                tt = t + way * k

                def event(tt=tt, way=way, tail=sent):
                    arrived(w, tt, s)
                    if way < 0:
                        pl.when(t < 3)(lambda: copy(w, slot(w, tt, s), tt, s, 0, right).start())
                    else:
                        pl.when(t > 0)(lambda: copy(w, slot(w, tt, s), tt, s, 1, left).start())
                    copy(w, slot(w, tt, s), tt, s, 2, near_x).start()
                    copy(w, slot(w, tt, s), tt, s, 3, near_y).start()
                    copy(w, slot(w, tt, s), tt, s, 4, core).start()

                def finish(tt=tt, way=way):
                    if way < 0:
                        pl.when(t < 3)(lambda: copy(w, slot(w, tt, s), tt, s, 0, right).wait_send())
                    else:
                        pl.when(t > 0)(lambda: copy(w, slot(w, tt, s), tt, s, 1, left).wait_send())
                    for kind, target in ((2, near_x), (3, near_y), (4, core)):
                        copy(w, slot(w, tt, s), tt, s, kind, target).wait_send()

                ok = tt >= 0 if way < 0 else tt <= 3
                pl.when(ok)(event)
                sent.append(lambda ok=ok, finish=finish: pl.when(ok)(finish))

    def plane_events(w):
        for tt in range(4):
            arrived(w, tt, s_x)
            send(w, slot(w, tt, s_x), tt, s_x, 6, core)
            if tt % 2 == 0:
                send(w, slot(w, tt, s_x), tt, s_x, 5, near_y)
            arrived(w, tt, s_y)
            send(w, slot(w, tt, s_y), tt, s_y, 8, core)
            if tt % 2 == 1:
                send(w, slot(w, tt, s_y), tt, s_y, 7, near_x)

    def far_events(w):
        for tt in range(4):
            arrived(w, tt, s_far)
            send(w, slot(w, tt, s_far), tt, s_far, 9, core)

    def core_events(w):
        for tt in range(4):
            for base in (s, s_x, s_y, s_far):
                arrived(w, tt, base + 1 - 2 * c)

    lines = ((small, smalls), (cot, cots))

    def line_copy(v, src, tt, kind, target):
        return pltpu.make_async_remote_copy(
            src_ref=src, dst_ref=lines[v][1].at[tt], send_sem=line_send.at[v, tt, kind],
            recv_sem=line_recv.at[v, tt], device_id=target, device_id_type=MESH,
        )

    def open_other(v):
        own = lines[v][0]
        pl.when(t < 3)(lambda: line_copy(v, own, t, 0, right).start())
        pl.when(t > 0)(lambda: line_copy(v, own, t, 1, left).start())
        sent.append(lambda: pl.when(t < 3)(lambda: line_copy(v, own, t, 0, right).wait_send()))
        sent.append(lambda: pl.when(t > 0)(lambda: line_copy(v, own, t, 1, left).wait_send()))

    def other_events(v, k):
        whole = lines[v][1]
        for way in (-1, 1):
            tt = t + way * k
            kind, target = (0, right) if way < 0 else (1, left)
            more = t < 3 if way < 0 else t > 0

            def event(tt=tt, kind=kind, target=target, more=more):
                line_copy(v, whole.at[tt], tt, kind, target).wait_recv()
                pl.when(more)(lambda: line_copy(v, whole.at[tt], tt, kind, target).start())

            def finish(tt=tt, kind=kind, target=target, more=more):
                pl.when(more)(lambda: line_copy(v, whole.at[tt], tt, kind, target).wait_send())

            ok = tt >= 0 if way < 0 else tt <= 3
            pl.when(ok)(event)
            sent.append(lambda ok=ok, finish=finish: pl.when(ok)(finish))

    into = [pltpu.make_async_copy(weights[w].at[:, s], stage[w], local_sem.at[w]) for w in range(count)]
    out = [pltpu.make_async_copy(stage[w], slot(w, t, s), local_sem.at[w]) for w in range(count)]
    for v, (own, whole) in enumerate(lines):
        into.append(pltpu.make_async_copy(own, stage[count + v], local_sem.at[count + v]))
        out.append(pltpu.make_async_copy(stage[count + v], whole.at[t], local_sem.at[count + v]))

    open_other(0)
    for w in range(count):
        open_line(w)
    for move in into:
        move.start()
    line_events(0)
    line_events(1)
    for a, b in zip(into, out):
        a.wait()
        b.start()
    open_other(1)
    plane_events(0)
    line_events(2)
    far_events(0)
    plane_events(1)
    line_events(3)
    far_events(1)
    other_events(1, 1)
    plane_events(2)
    far_events(2)
    other_events(1, 2)
    plane_events(3)
    for k in (1, 2, 3):
        other_events(0, k)
    other_events(1, 3)
    far_events(3)
    for w in range(count):
        core_events(w)
    for move in out:
        move.wait()
    for done in sent:
        done()
    pl.when(linear > 0)(onward.wait_recv)
    pl.when(linear < 31)(onward.wait_send)


def gather_all(weights, small, cotangent, tokens, tail_rows):
    n_ten, n_seq = lax.axis_size("tensor"), lax.axis_size("seq")
    if not (n_ten == 4 and n_seq == 8):
        full = [jnp.moveaxis(lax.all_gather(w, "tensor", axis=0), 0, 1) for w in weights]
        devices = n_ten * n_seq
        halo = lax.ppermute(
            tokens[tokens.shape[0] - tail_rows :], BOTH, [(i, i + 1) for i in range(devices - 1)]
        )
        whole = (lax.all_gather(a, "tensor", axis=0) for a in (small, cotangent))
        return full, *whole, halo
    count = len(weights)
    cut = [w.reshape(w.shape[0], 8, w.shape[1] // 8, w.shape[2]) for w in weights]
    anywhere = pl.BlockSpec(memory_space=pl.ANY)
    outs = [jax.ShapeDtypeStruct((w.shape[0], 4) + w.shape[1:], w.dtype) for w in cut]
    outs += [jax.ShapeDtypeStruct((4,) + a.shape, a.dtype) for a in (small, cotangent)]
    outs.append(jax.ShapeDtypeStruct((tail_rows, tokens.shape[1]), tokens.dtype))
    dma = pltpu.SemaphoreType.DMA
    got = pl.pallas_call(
        functools.partial(gather_kernel, count),
        out_shape=outs,
        in_specs=[anywhere] * (count + 3),
        out_specs=[anywhere] * (count + 3),
        scratch_shapes=[pltpu.VMEM((w.shape[0],) + w.shape[2:], w.dtype) for w in cut]
        + [pltpu.VMEM(a.shape, a.dtype) for a in (small, cotangent)]
        + [
            dma((count + 2,)), dma((count, 4, 10)), dma((count, 4, 8)),
            dma((2, 4, 2)), dma((2, 4)), dma((2,)),
        ],
        compiler_params=pltpu.CompilerParams(collective_id=1, has_side_effects=True),
        name="gather",
    )(*cut, small, cotangent, tokens)
    full = [g.reshape(w.shape[0], 4, w.shape[1], w.shape[2]) for g, w in zip(got, weights)]
    return full, *got[count:]


def carry_kernel(reach, reverse, carry_ref, out_ref, send_sem, recv_sem):
    n_ten = lax.axis_size("tensor")
    devices = n_ten * lax.axis_size("seq")
    me = lax.axis_index("seq") * n_ten + lax.axis_index("tensor")
    way = -1 if reverse else 1

    def place(linear):
        return linear // n_ten, linear % n_ten

    greet([place((me - way * k + devices) % devices) for k in range(1, reach + 1)])

    def copy(k):
        return pltpu.make_async_remote_copy(
            src_ref=carry_ref, dst_ref=out_ref.at[k - 1], send_sem=send_sem.at[k - 1],
            recv_sem=recv_sem.at[k - 1], device_id=place((me + way * k + devices) % devices),
            device_id_type=MESH,
        )

    def there(k, back):
        spot = me - way * k if back else me + way * k
        return (spot >= 0) & (spot < devices)

    for k in range(1, reach + 1):
        pl.when(there(k, False))(lambda k=k: copy(k).start())
    for k in range(1, reach + 1):
        pl.when(there(k, True))(lambda k=k: copy(k).wait_recv())
        pl.when(there(k, False))(lambda k=k: copy(k).wait_send())


def entering(carry, reach, linear, devices, reverse):
    channels = carry.shape[1]
    vmem = pl.BlockSpec(memory_space=pltpu.VMEM)
    got = pl.pallas_call(
        functools.partial(carry_kernel, reach, reverse),
        out_shape=jax.ShapeDtypeStruct((reach, 2, channels), F32),
        in_specs=[vmem],
        out_specs=vmem,
        scratch_shapes=[pltpu.SemaphoreType.DMA((reach,)), pltpu.SemaphoreType.DMA((reach,))],
        compiler_params=pltpu.CompilerParams(
            collective_id=3 if reverse else 2, has_side_effects=True
        ),
        name="carry_back" if reverse else "carry",
    )(carry)
    state = jnp.zeros((1, channels), F32)
    for k in range(reach, 0, -1):
        source = linear + k if reverse else linear - k
        there = (source >= 0) & (source < devices)
        state = jnp.where(there, got[k - 1, 0:1] * state + got[k - 1, 1:2], state)
    return state


def pick4(t, a, b, c, d):
    return jnp.where(t == 0, a, jnp.where(t == 1, b, jnp.where(t == 2, c, d)))


def tail_kernel(lefts, rows, groups, chunk, share, *refs):
    n_a, n_b = max(lefts) + 1, len(lefts)
    a_refs, b_refs, out_ref = refs[:n_a], refs[n_a : n_a + n_b], refs[n_a + n_b]
    (
        a_all, b_all, product, to_x, to_y, to_far, far_x, far_y, from_x, from_y, total,
        line_send, line_recv, fill_sem, out_sem, pair_send, pair_recv,
        send_sem, recv_sem, zs_sem, zr_sem,
    ) = refs[n_a + n_b + 1 :]
    cols = groups * chunk
    s, t = lax.axis_index("seq"), lax.axis_index("tensor")
    c, x, y = s % 2, (s // 2) % 2, s // 4
    p = s // 2
    p_x, p_y = p + 1 - 2 * x, p + 2 - 4 * y
    p_far = p_x + 2 - 4 * y
    near_x, near_y, core = (s + 2 - 4 * x, t), (s + 4 - 8 * y, t), (s + 1 - 2 * c, t)
    right, left = (s, t + 1), (s, t - 1)
    greet([(s, (t + 1) % 4), (s, (t + 3) % 4), near_x, near_y, core])
    half = share // 2
    steps = 4 * n_b

    def fill_b(w, k):
        tt, j = k // groups, k % groups
        return pltpu.make_async_copy(
            b_refs[w].at[:, pl.ds(pl.multiple_of((j * 4 + tt) * chunk, 128), chunk)],
            b_all.at[w, tt, pl.ds(0, rows), pl.ds(pl.multiple_of(j * chunk, 128), chunk)],
            fill_sem.at[n_a + w, k],
        )

    def fill_a(v):
        return pltpu.make_async_copy(a_refs[v], a_all.at[v, pl.ds(0, rows)], fill_sem.at[v, 0])

    def pair_a(v):
        return pltpu.make_async_remote_copy(
            src_ref=a_refs[v], dst_ref=a_all.at[v, pl.ds(rows, rows)],
            send_sem=pair_send.at[v, 0], recv_sem=pair_recv.at[v, 0],
            device_id=core, device_id_type=MESH,
        )

    def pair_b(w, k):
        return pltpu.make_async_remote_copy(
            src_ref=b_all.at[w, k, pl.ds(0, rows)], dst_ref=b_all.at[w, k, pl.ds(rows, rows)],
            send_sem=pair_send.at[n_a + w, k], recv_sem=pair_recv.at[n_a + w, k],
            device_id=core, device_id_type=MESH,
        )

    for w in range(n_b):
        if w == 0 or lefts[w] != lefts[w - 1]:
            pair_a(lefts[w]).start()
            fill_a(lefts[w]).start()

        @pl.loop(0, 4 * groups)
        def _(k, w=w):
            fill_b(w, k).start()

    for w in range(n_b):

        @pl.loop(0, 4 * groups)
        def _(k, w=w):
            fill_b(w, k).wait()

        @pl.loop(0, 4)
        def _(k, w=w):
            pair_b(w, k).start()

    for v in range(n_a):
        fill_a(v).wait()
        pair_a(v).wait_recv()

    def dest(n):
        i = n % 4
        third, second, first = pick4(t, 3, 3, 0, 0), pick4(t, 2, 0, 1, 1), pick4(t, 1, 2, 3, 2)
        return pick4(i, third, second, first, t)

    def make(n, q):
        w = n // 4
        start = pl.multiple_of(2 * share * q + (share - 64) * c, 128)
        v = sum(jnp.where(w >= k, lefts[k] - (lefts[k - 1] if k else 0), 0) for k in range(n_b))
        lhs = a_all[v, :, pl.ds(start, share + 64)]
        rhs = b_all[w, dest(n)]
        product[...] = lax.dot_general(lhs, rhs, (((0,), (0,)), ((), ())), preferred_element_type=F32)
        return product[pl.ds(pl.multiple_of(64 * c, 64), share), :]

    def remote(n, src, dst, k, target):
        return pltpu.make_async_remote_copy(
            src_ref=src, dst_ref=dst, send_sem=send_sem.at[n, k], recv_sem=recv_sem.at[n, k],
            device_id=target, device_id_type=MESH,
        )

    def directs(n):
        return (
            remote(n, to_far.at[n, pl.ds(0, half)], far_x.at[n], 0, near_x),
            remote(n, to_far.at[n, pl.ds(half, half)], far_y.at[n], 1, near_y),
            remote(n, to_x.at[n, pl.ds(0, half)], from_x.at[n, pl.ds(0, half)], 2, near_x),
            remote(n, to_y.at[n, pl.ds(half, half)], from_y.at[n, pl.ds(half, half)], 3, near_y),
        )

    def seconds(n):
        return (
            remote(n, to_x.at[n, pl.ds(half, half)], from_x.at[n, pl.ds(half, half)], 4, near_x),
            remote(n, to_y.at[n, pl.ds(0, half)], from_y.at[n, pl.ds(0, half)], 5, near_y),
        )

    def begin(n):
        pair_b(n // 4, dest(n)).wait_recv()
        to_far[n] = make(n, p_far).astype(BF16)
        directs(n)[0].start()
        directs(n)[1].start()
        to_x[n] = make(n, p_x).astype(BF16)
        directs(n)[2].start()
        to_y[n] = make(n, p_y).astype(BF16)
        directs(n)[3].start()

    def forward(n):
        first, second = directs(n)[:2]
        first.wait_recv()
        to_y[n, pl.ds(0, half)] = (
            to_y[n, pl.ds(0, half)].astype(F32) + far_x[n].astype(F32)
        ).astype(BF16)
        seconds(n)[1].start()
        second.wait_recv()
        to_x[n, pl.ds(half, half)] = (
            to_x[n, pl.ds(half, half)].astype(F32) + far_y[n].astype(F32)
        ).astype(BF16)
        seconds(n)[0].start()

    def hop(w, out, into, target):
        return pltpu.make_async_remote_copy(
            src_ref=line_send.at[w, out], dst_ref=line_recv.at[w, into],
            send_sem=zs_sem.at[w, out], recv_sem=zr_sem.at[w, into],
            device_id=target, device_id_type=MESH,
        )

    end = (t == 0) | (t == 3)

    def finish(n):
        w, i = n // 4, n % 4
        mine = make(n, p)
        for move in directs(n)[2:] + seconds(n):
            move.wait_recv()
        total[w] = mine + from_x[n].astype(F32) + from_y[n].astype(F32)

        @pl.when((i < 3) & end)
        def _():
            line_send[w, i] = total[w].astype(BF16)

        @pl.when((i == 0) & (t == 0))
        def _():
            hop(w, 0, 0, right).start()

        @pl.when((i == 0) & (t == 3))
        def _():
            hop(w, 0, 0, left).start()

        @pl.when((i == 1) & (t == 0))
        def _():
            hop(w, 1, 1, right).start()

        @pl.when((i == 1) & (t == 3))
        def _():
            hop(w, 1, 2, left).start()

        @pl.when((i == 2) & (t == 0))
        def _():
            hop(w, 2, 3, right).start()

        @pl.when((i == 2) & (t == 3))
        def _():
            hop(w, 2, 4, left).start()

        @pl.when((i == 0) & (t == 1))
        def _():
            hop(w, 0, 0, right).wait_recv()
            line_send[w, 0] = (total[w] + line_recv[w, 0].astype(F32)).astype(BF16)
            hop(w, 0, 1, right).start()

        @pl.when((i == 0) & (t == 2))
        def _():
            hop(w, 0, 0, left).wait_recv()
            line_send[w, 0] = (total[w] + line_recv[w, 0].astype(F32)).astype(BF16)
            hop(w, 0, 2, left).start()

        @pl.when((i == 1) & ~end)
        def _():
            hop(w, 1, 2, left).wait_recv()
            line_send[w, 1] = (total[w] + line_recv[w, 2].astype(F32)).astype(BF16)
            hop(w, 1, 4, left).start()

        @pl.when((i == 2) & ~end)
        def _():
            hop(w, 1, 1, right).wait_recv()
            line_send[w, 2] = (total[w] + line_recv[w, 1].astype(F32)).astype(BF16)
            hop(w, 2, 3, right).start()

    @pl.loop(0, steps + 3)
    def _(n):
        @pl.when(n < steps)
        def _():
            begin(n)

        @pl.when((n >= 1) & (n <= steps))
        def _():
            forward(n - 1)

        @pl.when(n >= 3)
        def _():
            finish(n - 3)

    def result(w):
        return pltpu.make_async_copy(total.at[w], out_ref.at[w], out_sem.at[w])

    for w in range(n_b):

        @pl.when(t > 0)
        def _(w=w):
            hop(w, 2, 3, right).wait_recv()
            total[w] = total[w] + line_recv[w, 3].astype(F32)

        @pl.when(t < 3)
        def _(w=w):
            hop(w, 2, 4, left).wait_recv()
            total[w] = total[w] + line_recv[w, 4].astype(F32)

        result(w).start()

    @pl.loop(0, steps)
    def _(n):
        for move in directs(n) + seconds(n):
            move.wait_send()

    for w in range(n_b):
        for k in range(3):
            hop(w, k, 0, right).wait_send()
        result(w).wait()

        @pl.loop(0, 4)
        def _(k, w=w):
            pair_b(w, k).wait_send()

    for v in range(n_a):
        pair_a(v).wait_send()


def weight_grads(lefts, a_list, b_list, groups):
    n_ten, n_seq = lax.axis_size("tensor"), lax.axis_size("seq")
    rows, width = a_list[0].shape
    channels = b_list[0].shape[1]
    chunk = channels // groups // n_ten
    share = width // n_seq
    if not (n_ten == 4 and n_seq == 8):
        out = []
        for v, b in zip(lefts, b_list):
            b = jnp.swapaxes(b.reshape(rows, groups, n_ten, chunk), 1, 2).reshape(rows, channels)
            grad = dot_tn(a_list[v], b).astype(BF16)
            grad = lax.psum_scatter(grad, "seq", scatter_dimension=0, tiled=True)
            out.append(lax.psum_scatter(grad, "tensor", scatter_dimension=1, tiled=True).astype(F32))
        return out
    count, cols = len(b_list), groups * chunk
    half, steps = share // 2, 4 * count
    anywhere = pl.BlockSpec(memory_space=pl.ANY)
    dma = pltpu.SemaphoreType.DMA

    def room(*dims):
        return pltpu.VMEM(dims, BF16)

    both = len(a_list) + count
    return pl.pallas_call(
        functools.partial(tail_kernel, lefts, rows, groups, chunk, share),
        out_shape=jax.ShapeDtypeStruct((count, share, cols), F32),
        in_specs=[anywhere] * both,
        out_specs=anywhere,
        scratch_shapes=[
            room(len(a_list), 2 * rows, width), room(count, 4, 2 * rows, cols),
            pltpu.VMEM((share + 64, cols), F32),
            room(steps, share, cols), room(steps, share, cols), room(steps, share, cols),
            room(steps, half, cols), room(steps, half, cols),
            room(steps, share, cols), room(steps, share, cols),
            pltpu.VMEM((count, share, cols), F32),
            room(count, 3, share, cols), room(count, 5, share, cols),
            dma((both, 4 * groups)), dma((count,)), dma((both, 4)), dma((both, 4)),
            dma((steps, 6)), dma((steps, 6)), dma((count, 3)), dma((count, 5)),
        ],
        compiler_params=pltpu.CompilerParams(
            collective_id=4, has_side_effects=True, vmem_limit_bytes=67043328
        ),
        name="tail",
    )(*a_list, *b_list)


def chunk_scan(a_ref, d_ref, p_ref, s_ref, reverse):
    tiles, rows, wide = a_ref.shape
    run = rows // 8

    def first(i, carry):
        r = run - 1 - i if reverse else i
        here = pl.ds(r, 8, stride=run)
        after = []
        for b in range(tiles):
            prod, state = carry[b]
            a = a_ref[b, here, :]
            prod = prod * a
            state = a * state + d_ref[b, here, :]
            a_ref[b, here, :] = prod
            d_ref[b, here, :] = state
            after.append((prod, state))
        return tuple(after)

    start = (jnp.ones((8, wide), F32), jnp.zeros((8, wide), F32))
    ends = lax.fori_loop(0, run, first, (start,) * tiles, unroll=4)
    leads, totals = [], []
    for b in range(tiles):
        prod, state = ends[b]
        enter_p, enter_s = [None] * 8, [None] * 8
        now_p, now_s = jnp.ones((1, wide), F32), jnp.zeros((1, wide), F32)
        for c in range(7, -1, -1) if reverse else range(8):
            enter_p[c], enter_s[c] = now_p, now_s
            now_p, now_s = now_p * prod[c : c + 1], prod[c : c + 1] * now_s + state[c : c + 1]
        leads.append((jnp.concatenate(enter_p, 0), jnp.concatenate(enter_s, 0)))
        totals.append((now_p, now_s))

    def second(r, _):
        here = pl.ds(r, 8, stride=run)
        for b in range(tiles):
            p = a_ref[b, here, :]
            a_ref[b, here, :] = p * leads[b][0]
            d_ref[b, here, :] = d_ref[b, here, :] + p * leads[b][1]
        return 0

    lax.fori_loop(0, run, second, 0, unroll=4)
    for b in range(tiles):
        p_ref[:, b * wide : (b + 1) * wide] = a_ref[b]
        s_ref[:, b * wide : (b + 1) * wide] = d_ref[b]
    return jnp.concatenate([p for p, _ in totals], 1), jnp.concatenate([v for _, v in totals], 1)


def tiled_store(ref, value):
    tiles, _, wide = ref.shape
    for b in range(tiles):
        ref[b] = value[:, b * wide : (b + 1) * wide]


def positions(base_ref, rows, lanes, length):
    place = lax.broadcasted_iota(jnp.int32, (rows, lanes), 0) + base_ref[0]
    return jnp.where(place >= length, place - length, place)


def forward_kernel(
    length, local, base_ref, x_ref, cw_ref, rate_gain_ref, g_ref, sel_ref,
    conv_ref, rate_ref, in_ref, p_ref, s_ref, carry_ref, w_ref, a_ref, d_ref,
):
    rows, lanes = conv_ref.shape
    spot = positions(base_ref, rows, lanes, length)
    x = x_ref[...].astype(F32)
    total = cw_ref[0:1, :] * x[HALO:]
    for k in range(1, CONV):
        moved = pltpu.roll(x, k, 0)[HALO:]
        total = total + jnp.where(spot >= k, cw_ref[k : k + 1, :] * moved, 0.0)
    conv = total.astype(BF16)
    conv_ref[...] = conv
    join = sel_ref.shape[0]
    wide = jnp.dot(g_ref[0], sel_ref[0], preferred_element_type=F32)
    for q in range(1, join):
        other = jnp.dot(g_ref[0], sel_ref[q], preferred_element_type=F32)
        which = lax.broadcasted_iota(jnp.int32, wide.shape, 0) // local % join
        wide = jnp.where(which == q, other, wide)
    gates = wide.astype(BF16)
    w_ref[0] = gates
    pre = lax.dot_general(conv, gates, (((1,), (1,)), ((), ())), preferred_element_type=F32)
    rate, inp = pre[:, :lanes], pre[:, lanes:]
    rate_ref[...] = rate
    in_ref[...] = inp
    decay = jnp.where(spot == 0, 0.0, jnp.exp(rate_gain_ref[...] * jax.nn.sigmoid(rate)))
    tiled_store(a_ref, decay)
    tiled_store(
        d_ref,
        jnp.sqrt(jnp.maximum(1.0 - decay * decay, 0.01)) * jax.nn.sigmoid(inp) * conv.astype(F32),
    )
    prod, state = chunk_scan(a_ref, d_ref, p_ref, s_ref, False)
    carry_ref[0:1, :] = prod
    carry_ref[1:2, :] = state


def middle_kernel(
    length, base_ref, mg_ref, y_ref, p_ref, s_ref, enter_ref, rate_ref, rate_gain_ref,
    ylow_ref, bp_ref, bs_ref, carry_ref, a_ref, d_ref,
):
    rows, lanes = mg_ref.shape
    spot = positions(base_ref, rows, lanes, length)
    states = s_ref[...] + p_ref[...] * enter_ref[...]
    value, slope = gelu_both(y_ref[...])
    grad = mg_ref[...]
    ylow_ref[...] = (grad * states * slope).astype(BF16)
    tiled_store(d_ref, grad * value)
    decay = jnp.where(spot == 0, 0.0, jnp.exp(rate_gain_ref[...] * jax.nn.sigmoid(rate_ref[...])))
    row = lax.broadcasted_iota(jnp.int32, (rows, lanes), 0)
    tiled_store(a_ref, jnp.where(row == rows - 1, 1.0, pltpu.roll(decay, rows - 1, 0)))
    prod, state = chunk_scan(a_ref, d_ref, bp_ref, bs_ref, True)
    carry_ref[0:1, :] = decay[0:1] * prod
    carry_ref[1:2, :] = decay[0:1] * state


def backward_kernel(
    length, local, base_ref, bp_ref, bs_ref, leave_ref, p_ref, s_ref, enter_ref, rate_ref, in_ref,
    conv_ref, rate_gain_ref, w_ref, cw_ref, x_ref, sel_ref,
    gates_ref, xback_ref, edge_ref, small_ref,
):
    rows, lanes = bp_ref.shape
    spot = positions(base_ref, rows, lanes, length)
    row = lax.broadcasted_iota(jnp.int32, (rows, lanes), 0)
    adjoint = bs_ref[...] + bp_ref[...] * leave_ref[...]
    states = s_ref[...] + p_ref[...] * enter_ref[...]
    before = jnp.where(row == 0, enter_ref[...], pltpu.roll(states, 1, 0))
    gain = rate_gain_ref[...]
    sig_r = jax.nn.sigmoid(rate_ref[...])
    sig_i = jax.nn.sigmoid(in_ref[...])
    conv = conv_ref[...]
    conv_f = conv.astype(F32)
    decay = jnp.where(spot == 0, 0.0, jnp.exp(gain * sig_r))
    room = 1.0 - decay * decay
    scale = jnp.sqrt(jnp.maximum(room, 0.01))
    pulled = adjoint * sig_i
    slope = jnp.where(room > 0.01, -decay / scale, 0.0)
    decay_grad = adjoint * before + pulled * conv_f * slope
    log_grad = decay_grad * decay
    pull_r = log_grad * sig_r
    rate_back = (pull_r * gain * (1.0 - sig_r)).astype(BF16)
    conv_direct = pulled * scale
    in_back = (conv_direct * conv_f * (1.0 - sig_i)).astype(BF16)
    both = jnp.concatenate([rate_back, in_back], 1)
    join = sel_ref.shape[0]
    for q in range(join):
        some = lax.dot_general(
            conv, sel_ref[q], (((1,), (1,)), ((), ())), preferred_element_type=F32
        ).astype(BF16)
        part = lax.dot_general(some, both, (((0,), (0,)), ((), ())), preferred_element_type=F32)
        if q == 0:
            gate_sum = part
        else:
            which = lax.broadcasted_iota(jnp.int32, part.shape, 1) // local % join
            gate_sum = jnp.where(which == q, part, gate_sum)
    gates_ref[0] = gate_sum.astype(BF16)
    grad = conv_direct + lax.dot_general(
        both, w_ref[0], (((1,), (0,)), ((), ())), preferred_element_type=F32
    )
    x = x_ref[...].astype(F32)
    zeros = jnp.zeros((HALO, lanes), F32)
    out = jnp.concatenate([zeros, grad * cw_ref[0:1, :]], 0)
    small_ref[0:1, :] = jnp.sum(grad * x[HALO:], axis=0, keepdims=True)
    for k in range(1, CONV):
        masked = jnp.where(spot >= k, grad, 0.0)
        small_ref[k : k + 1, :] = jnp.sum(
            masked * pltpu.roll(x, k, 0)[HALO:], axis=0, keepdims=True
        )
        tall = jnp.concatenate([zeros, masked * cw_ref[k : k + 1, :]], 0)
        out = out + pltpu.roll(tall, rows + HALO - k, 0)
    small_ref[CONV : CONV + 1, :] = jnp.sum(pull_r, axis=0, keepdims=True)
    small_ref[CONV + 1 : 8, :] = jnp.zeros((7 - CONV, lanes), F32)
    edge_ref[...] = out[:HALO]
    xback_ref[...] = out[HALO:]


def lane_call(kernel, grid, lanes, base, operands, outputs, scratch, flops):
    def spec(shape):
        if len(shape) == 3 and shape[0] != grid:
            return pl.BlockSpec(shape, lambda j, *_: (0, 0, 0))
        if len(shape) == 3:
            return pl.BlockSpec((1,) + shape[1:], lambda j, *_: (j, 0, 0))
        return pl.BlockSpec((shape[0], lanes), lambda j, *_: (0, j))

    moved = sum(math.prod(a.shape) * a.dtype.itemsize for a in list(operands) + list(outputs))
    return pl.pallas_call(
        kernel,
        grid_spec=pltpu.PrefetchScalarGridSpec(
            num_scalar_prefetch=1,
            grid=(grid,),
            in_specs=[spec(a.shape) for a in operands],
            out_specs=[spec(a.shape) for a in outputs],
            scratch_shapes=scratch,
        ),
        out_shape=outputs,
        compiler_params=pltpu.CompilerParams(
            dimension_semantics=("arbitrary",), vmem_limit_bytes=56 << 20
        ),
        cost_estimate=pl.CostEstimate(flops=flops, bytes_accessed=moved, transcendentals=0),
    )(base, *operands)


def shards(
    tokens_in, gain_pre, w_x, w_y, conv_w, gate_a, gate_i, decay_param, w_out,
    gain_mlp, w_gate, w_up, w_down, cotangent,
):
    rows, width = tokens_in.shape
    heads, local = w_x.shape[1:]
    n_ten, n_seq = lax.axis_size("tensor"), lax.axis_size("seq")
    devices = n_ten * n_seq
    place, run = lax.axis_index("tensor"), lax.axis_index("seq")
    linear = run * n_ten + place
    length = devices * rows // SEQS
    base = jnp.reshape((linear * rows) % length, (1,)).astype(jnp.int32)
    join = 128 // local if local < 128 and heads % (128 // local) == 0 else 1
    groups, chunk = heads // join, join * local
    lanes = n_ten * chunk
    channels = groups * lanes

    def shape(dims, kind=F32):
        return jax.ShapeDtypeStruct(dims, kind)

    def own_columns(array):
        n = array.shape[0]
        split = array.reshape(n, groups, n_ten, chunk)
        return lax.dynamic_index_in_dim(split, place, 2, False).reshape(n, heads, local)

    gate_rows = jnp.stack([gate_a, gate_i], 0).swapaxes(2, 3).reshape(2 * heads, local, n_ten * local)
    params = jnp.concatenate([conv_w, decay_param[None]], 0).reshape(CONV + 1, heads * local)
    params = jnp.pad(params, ((0, 7 - CONV), (0, 0)))
    (all_gates, full_x, full_y, full_out), params, cots, halo = gather_all(
        [
            gate_rows,
            jnp.transpose(w_x, (1, 2, 0)).reshape(groups, chunk, width),
            jnp.transpose(w_y, (1, 2, 0)).reshape(groups, chunk, width),
            w_out.reshape(groups, chunk, width),
        ],
        params, cotangent, tokens_in, HALO,
    )
    halo = jnp.where(linear == 0, jnp.zeros_like(halo), halo)
    full_x, full_y, full_out = (w.reshape(channels, width) for w in (full_x, full_y, full_out))
    gates = all_gates.reshape(2, groups, join, n_ten, local, n_ten * local)
    gates = jnp.transpose(gates, (1, 0, 3, 2, 4, 5)).reshape(groups, 2 * lanes, n_ten * local)
    key = jnp.arange(n_ten * local)[None, :, None]
    lane = jnp.arange(lanes)[None, None, :]
    member = jnp.arange(join)[:, None, None]
    select = (
        (lane // chunk == key // local) & (lane % local == key % local) & (lane // local % join == member)
    ).astype(BF16)
    params = jnp.transpose(params.reshape(n_ten, 8, groups, chunk), (1, 2, 0, 3)).reshape(8, channels)
    conv_rows, decay_full = params, params[CONV : CONV + 1]
    rate_gain = -8.0 * jax.nn.softplus(decay_full)

    own_in = tokens_in.astype(F32)
    in_scale, in_unit = rms_parts(own_in)
    normed = (in_unit * gain_pre).astype(BF16)
    normed_halo = (rms_parts(halo.astype(F32))[1] * gain_pre).astype(BF16)
    x_long = dot_nt(jnp.concatenate([normed_halo, normed], 0), full_x).astype(BF16)
    y_branch = dot_nt(normed, full_y)
    scratch = [pltpu.VMEM((lanes // 128, rows, 128), F32)] * 2
    conv_out, rate_pre, input_pre, products, partial, carry, wide_gates = lane_call(
        functools.partial(forward_kernel, length, local), groups, lanes, base,
        (x_long, conv_rows, rate_gain, gates, select),
        [
            shape((rows, channels), BF16),
            shape((rows, channels)),
            shape((rows, channels)),
            shape((rows, channels)),
            shape((rows, channels)),
            shape((2, channels)),
            shape((groups, 2 * lanes, lanes), BF16),
        ],
        scratch, 4 * rows * lanes * channels,
    )
    reach = min(-(-length // rows), devices - 1)
    enter = entering(carry, reach, linear, devices, False)
    states = partial + products * enter
    mixed = (states * jax.nn.gelu(y_branch, approximate=True)).astype(BF16)
    middle = own_in + dot_nn(mixed, full_out)
    mid_scale, mid_unit = rms_parts(middle)
    normed_mlp = (mid_unit * gain_mlp).astype(BF16)

    cots = [cotangent] + [
        lax.dynamic_index_in_dim(cots, label_index(k), 0, False) for k in range(1, n_ten)
    ]
    tokens = [normed_mlp] + others(normed_mlp)
    hiddens, gate_grads, up_grads, downs, pulls = [], [], [], [], []
    for n, c in zip(tokens, cots):
        gate_vals, up_vals = dot_nn(n, w_gate), dot_nn(n, w_up)
        value, slope = gelu_both(gate_vals)
        hidden = (value * up_vals).astype(BF16)
        hidden_grad = dot_nt(c, w_down)
        gate_grad = (hidden_grad * up_vals * slope).astype(BF16)
        up_grad = (hidden_grad * value).astype(BF16)
        hiddens.append(hidden)
        gate_grads.append(gate_grad)
        up_grads.append(up_grad)
        pulls.append(dot_nt(gate_grad, w_gate) + dot_nt(up_grad, w_up))
        downs.append(dot_nn(hidden, w_down))
    mlp_input = line_sum(pulls[0], [p.astype(BF16) for p in pulls[1:]])
    down = line_sum(downs[0], [d.astype(BF16) for d in downs[1:]])
    block_out = (middle + down).astype(BF16)

    cot_rows = jnp.concatenate(cots, 0)
    token_rows = jnp.concatenate(tokens, 0)
    hidden_rows = jnp.concatenate(hiddens, 0)
    grad_down = dot_tn(hidden_rows, cot_rows).astype(BF16)
    grad_gate = dot_tn(token_rows, jnp.concatenate(gate_grads, 0)).astype(BF16)
    grad_up = dot_tn(token_rows, jnp.concatenate(up_grads, 0)).astype(BF16)
    gain_mlp_part, mid_back = rms_back(mlp_input, gain_mlp, mid_scale, mid_unit)
    middle_grad = cotangent.astype(F32) + mid_back
    middle_low, grad_down, grad_gate, grad_up = lax.optimization_barrier(
        (middle_grad.astype(BF16), grad_down, grad_gate, grad_up)
    )
    grad_down = lax.psum_scatter(grad_down, "seq", scatter_dimension=1, tiled=True)
    grad_gate = lax.psum_scatter(grad_gate, "seq", scatter_dimension=0, tiled=True)
    grad_up = lax.psum_scatter(grad_up, "seq", scatter_dimension=0, tiled=True)
    mixed_grad = dot_nt(middle_low, full_out)
    y_low, back_products, back_partial, carry = lane_call(
        functools.partial(middle_kernel, length), groups, lanes, base,
        (mixed_grad, y_branch, products, partial, enter, rate_pre, rate_gain),
        [
            shape((rows, channels), BF16),
            shape((rows, channels)),
            shape((rows, channels)),
            shape((2, channels)),
        ],
        scratch, 60 * rows * channels,
    )
    leave = entering(carry, reach, linear, devices, True)
    gate_parts, x_back, edge, sums = lane_call(
        functools.partial(backward_kernel, length, local), groups, lanes, base,
        (
            back_products, back_partial, leave, products, partial, enter, rate_pre, input_pre,
            conv_out, rate_gain, wide_gates, conv_rows, x_long, select,
        ),
        [
            shape((groups, n_ten * local, 2 * lanes), BF16),
            shape((rows, channels)),
            shape((HALO, channels)),
            shape((8, channels)),
        ],
        [], 8 * rows * lanes * channels,
    )
    edge = lax.ppermute(edge, BOTH, [(i + 1, i) for i in range(devices - 1)])
    x_low = jnp.concatenate(
        [x_back[: rows - HALO], x_back[rows - HALO :] + edge], 0
    ).astype(BF16)

    grad_out, grad_y, grad_x = weight_grads(
        (0, 1, 1), [middle_low, normed], [mixed, y_low, x_low], groups
    )
    normed_grad = dot_nn(x_low, full_x) + dot_nn(y_low, full_y)
    gain_pre_part, in_back = rms_back(normed_grad, gain_pre, in_scale, in_unit)
    input_grad = middle_grad + in_back

    part = n_ten * local // n_seq
    split = gate_parts.reshape(groups, n_seq, part, 2, n_ten, chunk)
    split = jnp.transpose(split, (1, 4, 0, 3, 2, 5)).reshape(devices, groups * 2 * part, chunk)
    gate_sum = lax.psum_scatter(split, BOTH, scatter_dimension=0, tiled=True).astype(F32)
    gate_sum = gate_sum.reshape(groups, 2, part, join, local)
    gate_sum = jnp.transpose(gate_sum, (1, 0, 3, 2, 4)).reshape(2, heads, part, local)
    packed = jnp.concatenate([sums[: CONV + 1], gain_pre_part[None], gain_mlp_part[None]], 0)
    packed = lax.psum(packed, BOTH)
    conv_sum = own_columns(packed[:CONV])
    decay_sum = own_columns(packed[CONV : CONV + 1] * (-8.0 * jax.nn.sigmoid(decay_full)))[0]
    share = local // n_seq
    grad_conv = lax.dynamic_slice_in_dim(conv_sum, run * share, share, 2)
    grad_decay = lax.dynamic_slice_in_dim(decay_sum, run * share, share, 1)
    grad_gain_mlp = lax.dynamic_slice_in_dim(
        packed[CONV + 2], run * (width // n_seq), width // n_seq, 0
    )

    def weight(grad):
        return grad.T.reshape(heads, local, -1)

    return (
        block_out,
        input_grad,
        packed[CONV + 1],
        jnp.transpose(weight(grad_x), (2, 0, 1)),
        jnp.transpose(weight(grad_y), (2, 0, 1)),
        grad_conv,
        gate_sum[0],
        gate_sum[1],
        grad_decay,
        weight(grad_out),
        grad_gain_mlp,
        grad_gate.astype(F32),
        grad_up.astype(F32),
        grad_down.astype(F32),
    )


def solution(mesh):
    placed = (
        P(("seq", "tensor"), None),
        P(),
        P(None, None, "tensor"),
        P(None, None, "tensor"),
        P(None, None, "tensor"),
        P(None, None, "tensor"),
        P(None, None, "tensor"),
        P(None, "tensor"),
        P(None, "tensor", None),
        P(),
        P(None, "tensor"),
        P(None, "tensor"),
        P("tensor", None),
        P(("seq", "tensor"), None),
    )
    return jax.shard_map(
        shards,
        mesh=mesh,
        in_specs=placed,
        out_specs=(
            P(("seq", "tensor"), None),
            P(("seq", "tensor"), None),
            P(),
            P("seq", None, "tensor"),
            P("seq", None, "tensor"),
            P(None, None, ("tensor", "seq")),
            P(None, "seq", "tensor"),
            P(None, "seq", "tensor"),
            P(None, ("tensor", "seq")),
            P(None, "tensor", "seq"),
            P("seq"),
            P("seq", "tensor"),
            P("seq", "tensor"),
            P("tensor", "seq"),
        ),
        check_vma=False,
    )
```

```python
import functools
import math

import jax
import jax.numpy as jnp
from jax import lax
from jax.experimental import pallas as pl
from jax.experimental.pallas import tpu as pltpu
from jax.sharding import PartitionSpec as P


CONV = 4
SEQS = 3
HALO = 16
epsilon = 1e-06
F32 = jnp.float32
BF16 = jnp.bfloat16
ROOT = math.sqrt(2.0 / math.pi)
BOTH = ("seq", "tensor")


def dot_nn(a, b):
    return lax.dot_general(a, b, (((1,), (0,)), ((), ())), preferred_element_type=F32)


def dot_nt(a, b):
    return lax.dot_general(a, b, (((1,), (1,)), ((), ())), preferred_element_type=F32)


def dot_tn(a, b):
    return lax.dot_general(a, b, (((0,), (0,)), ((), ())), preferred_element_type=F32)


def rms_parts(values):
    scale = lax.rsqrt(jnp.mean(values * values, axis=-1, keepdims=True) + epsilon)
    return scale, values * scale


def rms_back(grad, gain, scale, unit):
    pulled = gain * grad
    inner = jnp.mean(pulled * unit, axis=-1, keepdims=True)
    return jnp.sum(grad * unit, axis=0), scale * (pulled - unit * inner)


def gelu_both(v):
    inner = v * v
    th = jnp.tanh(ROOT * (v + 0.044715 * v * inner))
    half = 0.5 * (1.0 + th)
    slope = half + 0.5 * v * (1.0 - th * th) * (ROOT * (1.0 + 3 * 0.044715 * inner))
    return v * half, slope


LABELS = ((1, 2, 3, 2), (2, 0, 1, 1), (3, 3, 0, 0))


def along(block, pairs):
    return lax.ppermute(block, "tensor", pairs)


def line_streams(own):
    right, left = [], []
    right.append(along(own, [(0, 1), (1, 2), (2, 3)]))
    left.append(along(own, [(1, 0), (2, 1), (3, 2)]))
    right.append(along(right[0], [(1, 2), (2, 3)]))
    left.append(along(left[0], [(1, 0), (2, 1)]))
    right.append(along(right[1], [(2, 3)]))
    left.append(along(left[1], [(1, 0)]))
    return right, left


def others(own):
    count = lax.axis_size("tensor")
    place = lax.axis_index("tensor")
    if count == 4:
        right, left = line_streams(own)
        first = jnp.where(place == 3, right[0], left[0])
        second = jnp.where(place == 0, left[1], jnp.where(place == 3, right[1], right[0]))
        third = jnp.where(
            place == 0, left[2], jnp.where(place == 1, left[1], jnp.where(place == 2, right[1], right[2]))
        )
        return [first, second, third]
    whole = lax.all_gather(own, "tensor", axis=0)
    return [lax.dynamic_index_in_dim(whole, (place + k) % count, 0, False) for k in range(1, count)]


def label_index(k):
    count = lax.axis_size("tensor")
    place = lax.axis_index("tensor")
    if count == 4:
        table = LABELS[k - 1]
        return jnp.where(
            place == 0, table[0], jnp.where(place == 1, table[1], jnp.where(place == 2, table[2], table[3]))
        )
    return (place + k) % count


def line_sum(own, parts):
    count = lax.axis_size("tensor")
    place = lax.axis_index("tensor")
    if count == 4:
        first, second, third = parts
        end = (place == 0) | (place == 3)
        right = along(third, [(0, 1)])
        left = along(third, [(3, 2)])
        arrived = jnp.where(place == 1, right, left)
        send = jnp.where(
            end, second, (third.astype(F32) + arrived.astype(F32)).astype(BF16)
        )
        right = along(send, [(0, 1), (1, 2)])
        left = along(send, [(3, 2), (2, 1)])
        send_right = (first.astype(F32) + right.astype(F32)).astype(BF16)
        send_left = (
            jnp.where(place == 3, first, second).astype(F32) + left.astype(F32)
        ).astype(BF16)
        right = along(send_right, [(0, 1), (1, 2), (2, 3)])
        left = along(send_left, [(3, 2), (2, 1), (1, 0)])
        return own.astype(F32) + right.astype(F32) + left.astype(F32)
    stack = jnp.zeros((count,) + own.shape, BF16)
    stack = lax.dynamic_update_index_in_dim(stack, own.astype(BF16), place, 0)
    for k in range(1, count):
        stack = lax.dynamic_update_index_in_dim(stack, parts[k - 1], label_index(k), 0)
    return lax.psum_scatter(stack, "tensor", scatter_dimension=0, tiled=False).astype(F32)


MESH = pl.DeviceIdType.MESH


def ring_places():
    s, t = lax.axis_index("seq"), lax.axis_index("tensor")
    c, x, y = s % 2, (s // 2) % 2, s // 4
    return s, t, c, x, y


def greet(targets):
    barrier = pltpu.get_barrier_semaphore()
    for target in targets:
        pl.semaphore_signal(barrier, inc=1, device_id=target, device_id_type=MESH)
    pl.semaphore_wait(barrier, len(targets))


def gather_kernel(count, *refs):
    weights, (small, cot, tokens) = refs[:count], refs[count : count + 3]
    full = refs[count + 3 : 2 * count + 3]
    smalls, cots, halo = refs[2 * count + 3 : 2 * count + 6]
    rest = refs[2 * count + 6 :]
    stage, rest = rest[: count + 2], rest[count + 2 :]
    local_sem, send_sem, recv_sem, line_send, line_recv, halo_sem = rest
    s, t, c, x, y = ring_places()
    s_core, s_x, s_y = s + 1 - 2 * c, s + 2 - 4 * x, s + 4 - 8 * y
    s_far = s_x + 4 - 8 * y
    right, left = (s, t + 1), (s, t - 1)
    near_x, near_y, core = (s_x, t), (s_y, t), (s_core, t)
    linear = 4 * s + t
    after, before = (linear + 1) % 32, (linear + 31) % 32
    greet(
        [(s, (t + 1) % 4), (s, (t + 3) % 4), near_x, near_y, core, (before // 4, before % 4)]
    )
    sent = []
    tail_rows = halo.shape[0]
    onward = pltpu.make_async_remote_copy(
        src_ref=tokens.at[pl.ds(tokens.shape[0] - tail_rows, tail_rows)], dst_ref=halo,
        send_sem=halo_sem.at[0], recv_sem=halo_sem.at[1],
        device_id=(after // 4, after % 4), device_id_type=MESH,
    )
    pl.when(linear < 31)(onward.start)

    def slot(w, tt, ss):
        return full[w].at[:, tt, ss]

    def copy(w, src, tt, ss, kind, target):
        return pltpu.make_async_remote_copy(
            src_ref=src, dst_ref=slot(w, tt, ss), send_sem=send_sem.at[w, tt, kind],
            recv_sem=recv_sem.at[w, tt, ss], device_id=target, device_id_type=MESH,
        )

    def arrived(w, tt, ss):
        copy(w, slot(w, tt, ss), tt, ss, 0, core).wait_recv()

    def send(w, src, tt, ss, kind, target, when=None):
        def go():
            copy(w, src, tt, ss, kind, target).start()

        def done():
            copy(w, src, tt, ss, kind, target).wait_send()

        if when is None:
            go()
            sent.append(done)
        else:
            pl.when(when)(go)
            sent.append(lambda: pl.when(when)(done))

    def spread(w, src, tt):
        send(w, src, tt, s, 2, near_x)
        send(w, src, tt, s, 3, near_y)
        send(w, src, tt, s, 4, core)

    def open_line(w):
        own = weights[w].at[:, s]
        send(w, own, t, s, 0, right, t < 3)
        send(w, own, t, s, 1, left, t > 0)
        spread(w, own, t)

    def line_events(w):
        for k in (1, 2, 3):
            for way in (-1, 1):
                tt = t + way * k

                def event(tt=tt, way=way, tail=sent):
                    arrived(w, tt, s)
                    if way < 0:
                        pl.when(t < 3)(lambda: copy(w, slot(w, tt, s), tt, s, 0, right).start())
                    else:
                        pl.when(t > 0)(lambda: copy(w, slot(w, tt, s), tt, s, 1, left).start())
                    copy(w, slot(w, tt, s), tt, s, 2, near_x).start()
                    copy(w, slot(w, tt, s), tt, s, 3, near_y).start()
                    copy(w, slot(w, tt, s), tt, s, 4, core).start()

                def finish(tt=tt, way=way):
                    if way < 0:
                        pl.when(t < 3)(lambda: copy(w, slot(w, tt, s), tt, s, 0, right).wait_send())
                    else:
                        pl.when(t > 0)(lambda: copy(w, slot(w, tt, s), tt, s, 1, left).wait_send())
                    for kind, target in ((2, near_x), (3, near_y), (4, core)):
                        copy(w, slot(w, tt, s), tt, s, kind, target).wait_send()

                ok = tt >= 0 if way < 0 else tt <= 3
                pl.when(ok)(event)
                sent.append(lambda ok=ok, finish=finish: pl.when(ok)(finish))

    def plane_events(w):
        for tt in range(4):
            arrived(w, tt, s_x)
            send(w, slot(w, tt, s_x), tt, s_x, 6, core)
            if tt % 2 == 0:
                send(w, slot(w, tt, s_x), tt, s_x, 5, near_y)
            arrived(w, tt, s_y)
            send(w, slot(w, tt, s_y), tt, s_y, 8, core)
            if tt % 2 == 1:
                send(w, slot(w, tt, s_y), tt, s_y, 7, near_x)

    def far_events(w):
        for tt in range(4):
            arrived(w, tt, s_far)
            send(w, slot(w, tt, s_far), tt, s_far, 9, core)

    def core_events(w):
        for tt in range(4):
            for base in (s, s_x, s_y, s_far):
                arrived(w, tt, base + 1 - 2 * c)

    lines = ((small, smalls), (cot, cots))

    def line_copy(v, src, tt, kind, target):
        return pltpu.make_async_remote_copy(
            src_ref=src, dst_ref=lines[v][1].at[tt], send_sem=line_send.at[v, tt, kind],
            recv_sem=line_recv.at[v, tt], device_id=target, device_id_type=MESH,
        )

    def open_other(v):
        own = lines[v][0]
        pl.when(t < 3)(lambda: line_copy(v, own, t, 0, right).start())
        pl.when(t > 0)(lambda: line_copy(v, own, t, 1, left).start())
        sent.append(lambda: pl.when(t < 3)(lambda: line_copy(v, own, t, 0, right).wait_send()))
        sent.append(lambda: pl.when(t > 0)(lambda: line_copy(v, own, t, 1, left).wait_send()))

    def other_events(v, k):
        whole = lines[v][1]
        for way in (-1, 1):
            tt = t + way * k
            kind, target = (0, right) if way < 0 else (1, left)
            more = t < 3 if way < 0 else t > 0

            def event(tt=tt, kind=kind, target=target, more=more):
                line_copy(v, whole.at[tt], tt, kind, target).wait_recv()
                pl.when(more)(lambda: line_copy(v, whole.at[tt], tt, kind, target).start())

            def finish(tt=tt, kind=kind, target=target, more=more):
                pl.when(more)(lambda: line_copy(v, whole.at[tt], tt, kind, target).wait_send())

            ok = tt >= 0 if way < 0 else tt <= 3
            pl.when(ok)(event)
            sent.append(lambda ok=ok, finish=finish: pl.when(ok)(finish))

    into = [pltpu.make_async_copy(weights[w].at[:, s], stage[w], local_sem.at[w]) for w in range(count)]
    out = [pltpu.make_async_copy(stage[w], slot(w, t, s), local_sem.at[w]) for w in range(count)]
    for v, (own, whole) in enumerate(lines):
        into.append(pltpu.make_async_copy(own, stage[count + v], local_sem.at[count + v]))
        out.append(pltpu.make_async_copy(stage[count + v], whole.at[t], local_sem.at[count + v]))

    open_other(0)
    for w in range(count):
        open_line(w)
    for move in into:
        move.start()
    line_events(0)
    line_events(1)
    for a, b in zip(into, out):
        a.wait()
        b.start()
    open_other(1)
    plane_events(0)
    line_events(2)
    far_events(0)
    plane_events(1)
    line_events(3)
    far_events(1)
    other_events(1, 1)
    plane_events(2)
    far_events(2)
    other_events(1, 2)
    plane_events(3)
    for k in (1, 2, 3):
        other_events(0, k)
    other_events(1, 3)
    far_events(3)
    for w in range(count):
        core_events(w)
    for move in out:
        move.wait()
    for done in sent:
        done()
    pl.when(linear > 0)(onward.wait_recv)
    pl.when(linear < 31)(onward.wait_send)


def gather_all(weights, small, cotangent, tokens, tail_rows):
    n_ten, n_seq = lax.axis_size("tensor"), lax.axis_size("seq")
    if not (n_ten == 4 and n_seq == 8):
        full = [jnp.moveaxis(lax.all_gather(w, "tensor", axis=0), 0, 1) for w in weights]
        devices = n_ten * n_seq
        halo = lax.ppermute(
            tokens[tokens.shape[0] - tail_rows :], BOTH, [(i, i + 1) for i in range(devices - 1)]
        )
        whole = (lax.all_gather(a, "tensor", axis=0) for a in (small, cotangent))
        return full, *whole, halo
    count = len(weights)
    cut = [w.reshape(w.shape[0], 8, w.shape[1] // 8, w.shape[2]) for w in weights]
    anywhere = pl.BlockSpec(memory_space=pl.ANY)
    outs = [jax.ShapeDtypeStruct((w.shape[0], 4) + w.shape[1:], w.dtype) for w in cut]
    outs += [jax.ShapeDtypeStruct((4,) + a.shape, a.dtype) for a in (small, cotangent)]
    outs.append(jax.ShapeDtypeStruct((tail_rows, tokens.shape[1]), tokens.dtype))
    dma = pltpu.SemaphoreType.DMA
    got = pl.pallas_call(
        functools.partial(gather_kernel, count),
        out_shape=outs,
        in_specs=[anywhere] * (count + 3),
        out_specs=[anywhere] * (count + 3),
        scratch_shapes=[pltpu.VMEM((w.shape[0],) + w.shape[2:], w.dtype) for w in cut]
        + [pltpu.VMEM(a.shape, a.dtype) for a in (small, cotangent)]
        + [
            dma((count + 2,)), dma((count, 4, 10)), dma((count, 4, 8)),
            dma((2, 4, 2)), dma((2, 4)), dma((2,)),
        ],
        compiler_params=pltpu.CompilerParams(collective_id=1, has_side_effects=True),
        name="gather",
    )(*cut, small, cotangent, tokens)
    full = [g.reshape(w.shape[0], 4, w.shape[1], w.shape[2]) for g, w in zip(got, weights)]
    return full, *got[count:]


def carry_kernel(reach, reverse, carry_ref, out_ref, send_sem, recv_sem):
    n_ten = lax.axis_size("tensor")
    devices = n_ten * lax.axis_size("seq")
    me = lax.axis_index("seq") * n_ten + lax.axis_index("tensor")
    way = -1 if reverse else 1

    def place(linear):
        return linear // n_ten, linear % n_ten

    greet([place((me - way * k + devices) % devices) for k in range(1, reach + 1)])

    def copy(k):
        return pltpu.make_async_remote_copy(
            src_ref=carry_ref, dst_ref=out_ref.at[k - 1], send_sem=send_sem.at[k - 1],
            recv_sem=recv_sem.at[k - 1], device_id=place((me + way * k + devices) % devices),
            device_id_type=MESH,
        )

    def there(k, back):
        spot = me - way * k if back else me + way * k
        return (spot >= 0) & (spot < devices)

    for k in range(1, reach + 1):
        pl.when(there(k, False))(lambda k=k: copy(k).start())
    for k in range(1, reach + 1):
        pl.when(there(k, True))(lambda k=k: copy(k).wait_recv())
        pl.when(there(k, False))(lambda k=k: copy(k).wait_send())


def entering(carry, reach, linear, devices, reverse):
    channels = carry.shape[1]
    vmem = pl.BlockSpec(memory_space=pltpu.VMEM)
    got = pl.pallas_call(
        functools.partial(carry_kernel, reach, reverse),
        out_shape=jax.ShapeDtypeStruct((reach, 2, channels), F32),
        in_specs=[vmem],
        out_specs=vmem,
        scratch_shapes=[pltpu.SemaphoreType.DMA((reach,)), pltpu.SemaphoreType.DMA((reach,))],
        compiler_params=pltpu.CompilerParams(
            collective_id=3 if reverse else 2, has_side_effects=True
        ),
        name="carry_back" if reverse else "carry",
    )(carry)
    state = jnp.zeros((1, channels), F32)
    for k in range(reach, 0, -1):
        source = linear + k if reverse else linear - k
        there = (source >= 0) & (source < devices)
        state = jnp.where(there, got[k - 1, 0:1] * state + got[k - 1, 1:2], state)
    return state


def pick4(t, a, b, c, d):
    return jnp.where(t == 0, a, jnp.where(t == 1, b, jnp.where(t == 2, c, d)))


def tail_kernel(lefts, rows, groups, chunk, share, *refs):
    n_a, n_b = max(lefts) + 1, len(lefts)
    a_refs, b_refs, down_ref = refs[:n_a], refs[n_a : n_a + n_b], refs[n_a + n_b]
    out_ref, land_ref, relay_ref = refs[n_a + n_b + 1 : n_a + n_b + 4]
    (
        a_all, b_all, product, to_x, to_y, to_far, far_x, far_y, from_x, from_y, total,
        line_send, line_recv, fill_sem, out_sem, pair_send, pair_recv,
        send_sem, recv_sem, zs_sem, zr_sem,
        one, two, down_sem, down_send, down_recv,
    ) = refs[n_a + n_b + 4 :]
    s, t = lax.axis_index("seq"), lax.axis_index("tensor")
    c, x, y = s % 2, (s // 2) % 2, s // 4
    p = s // 2
    p_x, p_y = p + 1 - 2 * x, p + 2 - 4 * y
    p_far = p_x + 2 - 4 * y
    near_x, near_y, core = (s + 2 - 4 * x, t), (s + 4 - 8 * y, t), (s + 1 - 2 * c, t)
    right, left = (s, t + 1), (s, t - 1)
    greet([(s, (t + 1) % 4), (s, (t + 3) % 4), near_x, near_y, core])
    half = share // 2
    steps = 4 * n_b

    tile = down_ref.shape[2] // 4

    def columns(k):
        return pl.ds(pl.multiple_of(k * tile, 128), tile)

    def pass_down(label, k, way, added):
        src = relay_ref.at[label, :, columns(k)] if added else down_ref.at[label + 1, :, columns(k)]
        return pltpu.make_async_remote_copy(
            src_ref=src, dst_ref=land_ref.at[way, label, :, columns(k)],
            send_sem=down_send.at[label, k], recv_sem=down_recv.at[way, label, k],
            device_id=left if way else right, device_id_type=MESH,
        )

    def add_down(label, arrived, k, way):
        pass_down(arrived, k, way, False).wait_recv()
        loads = (
            pltpu.make_async_copy(down_ref.at[label + 1, :, columns(k)], one, down_sem.at[0]),
            pltpu.make_async_copy(land_ref.at[way, arrived, :, columns(k)], two, down_sem.at[1]),
        )
        for move in loads:
            move.start()
        for move in loads:
            move.wait()
        one[...] = (one[...].astype(F32) + two[...].astype(F32)).astype(BF16)
        store = pltpu.make_async_copy(one, relay_ref.at[label, :, columns(k)], down_sem.at[2])
        store.start()
        store.wait()
        pass_down(label, k, way, True).start()

    def down_steps(n):
        for label in (2, 1, 0):
            now = 2 - label

            @pl.when((n == now) & (t == 0))
            def _(label=label):
                for k in range(4):
                    pass_down(label, k, 0, False).start()

            @pl.when((n == now) & (t == 3))
            def _(label=label):
                for k in range(4):
                    pass_down(label, k, 1, False).start()

        k = n % 4
        pl.when((n // 4 == 1) & (t == 1))(lambda: add_down(2, 2, k, 0))
        pl.when((n // 4 == 1) & (t == 2))(lambda: add_down(2, 2, k, 1))
        pl.when((n // 4 == 2) & (t == 1))(lambda: add_down(0, 1, k, 0))
        pl.when((n // 4 == 2) & (t == 2))(lambda: add_down(1, 1, k, 1))
        pl.when((n // 4 == 2) & (t == 1))(lambda: add_down(1, 2, k, 1))
        pl.when((n // 4 == 2) & (t == 2))(lambda: add_down(0, 2, k, 0))

    def fill_b(w, k):
        tt, j = k // groups, k % groups
        return pltpu.make_async_copy(
            b_refs[w].at[:, pl.ds(pl.multiple_of((j * 4 + tt) * chunk, 128), chunk)],
            b_all.at[w, tt, pl.ds(0, rows), pl.ds(pl.multiple_of(j * chunk, 128), chunk)],
            fill_sem.at[n_a + w, k],
        )

    def fill_a(v):
        return pltpu.make_async_copy(a_refs[v], a_all.at[v, pl.ds(0, rows)], fill_sem.at[v, 0])

    def pair_a(v):
        return pltpu.make_async_remote_copy(
            src_ref=a_refs[v], dst_ref=a_all.at[v, pl.ds(rows, rows)],
            send_sem=pair_send.at[v, 0], recv_sem=pair_recv.at[v, 0],
            device_id=core, device_id_type=MESH,
        )

    def pair_b(w, k):
        return pltpu.make_async_remote_copy(
            src_ref=b_all.at[w, k, pl.ds(0, rows)], dst_ref=b_all.at[w, k, pl.ds(rows, rows)],
            send_sem=pair_send.at[n_a + w, k], recv_sem=pair_recv.at[n_a + w, k],
            device_id=core, device_id_type=MESH,
        )

    for w in range(n_b):
        if w == 0 or lefts[w] != lefts[w - 1]:
            pair_a(lefts[w]).start()
            fill_a(lefts[w]).start()

        @pl.loop(0, 4 * groups)
        def _(k, w=w):
            fill_b(w, k).start()

    for w in range(n_b):

        @pl.loop(0, 4 * groups)
        def _(k, w=w):
            fill_b(w, k).wait()

        @pl.loop(0, 4)
        def _(k, w=w):
            pair_b(w, k).start()

    for v in range(n_a):
        fill_a(v).wait()
        pair_a(v).wait_recv()

    def dest(n):
        i = n % 4
        third, second, first = pick4(t, 3, 3, 0, 0), pick4(t, 2, 0, 1, 1), pick4(t, 1, 2, 3, 2)
        return pick4(i, third, second, first, t)

    def make(n, q):
        w = n // 4
        start = pl.multiple_of(2 * share * q + (share - 64) * c, 128)
        v = sum(jnp.where(w >= k, lefts[k] - (lefts[k - 1] if k else 0), 0) for k in range(n_b))
        lhs = a_all[v, :, pl.ds(start, share + 64)]
        rhs = b_all[w, dest(n)]
        product[...] = lax.dot_general(lhs, rhs, (((0,), (0,)), ((), ())), preferred_element_type=F32)
        return product[pl.ds(pl.multiple_of(64 * c, 64), share), :]

    def remote(n, src, dst, k, target):
        return pltpu.make_async_remote_copy(
            src_ref=src, dst_ref=dst, send_sem=send_sem.at[n, k], recv_sem=recv_sem.at[n, k],
            device_id=target, device_id_type=MESH,
        )

    def directs(n):
        return (
            remote(n, to_far.at[n, pl.ds(0, half)], far_x.at[n], 0, near_x),
            remote(n, to_far.at[n, pl.ds(half, half)], far_y.at[n], 1, near_y),
            remote(n, to_x.at[n, pl.ds(0, half)], from_x.at[n, pl.ds(0, half)], 2, near_x),
            remote(n, to_y.at[n, pl.ds(half, half)], from_y.at[n, pl.ds(half, half)], 3, near_y),
        )

    def seconds(n):
        return (
            remote(n, to_x.at[n, pl.ds(half, half)], from_x.at[n, pl.ds(half, half)], 4, near_x),
            remote(n, to_y.at[n, pl.ds(0, half)], from_y.at[n, pl.ds(0, half)], 5, near_y),
        )

    def begin(n):
        pair_b(n // 4, dest(n)).wait_recv()
        to_far[n] = make(n, p_far).astype(BF16)
        directs(n)[0].start()
        directs(n)[1].start()
        to_x[n] = make(n, p_x).astype(BF16)
        directs(n)[2].start()
        to_y[n] = make(n, p_y).astype(BF16)
        directs(n)[3].start()

    def forward(n):
        first, second = directs(n)[:2]
        first.wait_recv()
        to_y[n, pl.ds(0, half)] = (
            to_y[n, pl.ds(0, half)].astype(F32) + far_x[n].astype(F32)
        ).astype(BF16)
        seconds(n)[1].start()
        second.wait_recv()
        to_x[n, pl.ds(half, half)] = (
            to_x[n, pl.ds(half, half)].astype(F32) + far_y[n].astype(F32)
        ).astype(BF16)
        seconds(n)[0].start()

    def hop(w, out, into, target):
        return pltpu.make_async_remote_copy(
            src_ref=line_send.at[w, out], dst_ref=line_recv.at[w, into],
            send_sem=zs_sem.at[w, out], recv_sem=zr_sem.at[w, into],
            device_id=target, device_id_type=MESH,
        )

    end = (t == 0) | (t == 3)

    def finish(n):
        w, i = n // 4, n % 4
        mine = make(n, p)
        for move in directs(n)[2:] + seconds(n):
            move.wait_recv()
        total[w] = mine + from_x[n].astype(F32) + from_y[n].astype(F32)

        @pl.when((i < 3) & end)
        def _():
            line_send[w, i] = total[w].astype(BF16)

        @pl.when((i == 0) & (t == 0))
        def _():
            hop(w, 0, 0, right).start()

        @pl.when((i == 0) & (t == 3))
        def _():
            hop(w, 0, 0, left).start()

        @pl.when((i == 1) & (t == 0))
        def _():
            hop(w, 1, 1, right).start()

        @pl.when((i == 1) & (t == 3))
        def _():
            hop(w, 1, 2, left).start()

        @pl.when((i == 2) & (t == 0))
        def _():
            hop(w, 2, 3, right).start()

        @pl.when((i == 2) & (t == 3))
        def _():
            hop(w, 2, 4, left).start()

        @pl.when((i == 0) & (t == 1))
        def _():
            hop(w, 0, 0, right).wait_recv()
            line_send[w, 0] = (total[w] + line_recv[w, 0].astype(F32)).astype(BF16)
            hop(w, 0, 1, right).start()

        @pl.when((i == 0) & (t == 2))
        def _():
            hop(w, 0, 0, left).wait_recv()
            line_send[w, 0] = (total[w] + line_recv[w, 0].astype(F32)).astype(BF16)
            hop(w, 0, 2, left).start()

        @pl.when((i == 1) & ~end)
        def _():
            hop(w, 1, 2, left).wait_recv()
            line_send[w, 1] = (total[w] + line_recv[w, 2].astype(F32)).astype(BF16)
            hop(w, 1, 4, left).start()

        @pl.when((i == 2) & ~end)
        def _():
            hop(w, 1, 1, right).wait_recv()
            line_send[w, 2] = (total[w] + line_recv[w, 1].astype(F32)).astype(BF16)
            hop(w, 2, 3, right).start()

    @pl.loop(0, steps + 3)
    def _(n):
        @pl.when(n < steps)
        def _():
            begin(n)

        @pl.when((n >= 1) & (n <= steps))
        def _():
            forward(n - 1)

        down_steps(n)

        @pl.when(n >= 3)
        def _():
            finish(n - 3)

    def result(w):
        return pltpu.make_async_copy(total.at[w], out_ref.at[w], out_sem.at[w])

    for w in range(n_b):

        @pl.when(t > 0)
        def _(w=w):
            hop(w, 2, 3, right).wait_recv()
            total[w] = total[w] + line_recv[w, 3].astype(F32)

        @pl.when(t < 3)
        def _(w=w):
            hop(w, 2, 4, left).wait_recv()
            total[w] = total[w] + line_recv[w, 4].astype(F32)

        result(w).start()

    @pl.loop(0, steps)
    def _(n):
        for move in directs(n) + seconds(n):
            move.wait_send()

    for w in range(n_b):
        for k in range(3):
            hop(w, k, 0, right).wait_send()
        result(w).wait()

        @pl.loop(0, 4)
        def _(k, w=w):
            pair_b(w, k).wait_send()

    for v in range(n_a):
        pair_a(v).wait_send()

    @pl.loop(0, 4)
    def _(k):
        for label in range(3):
            pass_down(label, k, 0, False).wait_send()
        for way, label, ok in (
            (0, 0, t > 0), (1, 0, t == 2), (1, 1, t < 2),
        ):
            pl.when(ok)(lambda way=way, label=label: pass_down(label, k, way, False).wait_recv())


def weight_grads(lefts, a_list, b_list, groups, downs):
    n_ten, n_seq = lax.axis_size("tensor"), lax.axis_size("seq")
    rows, width = a_list[0].shape
    channels = b_list[0].shape[1]
    chunk = channels // groups // n_ten
    share = width // n_seq
    if not (n_ten == 4 and n_seq == 8):
        out = []
        for v, b in zip(lefts, b_list):
            b = jnp.swapaxes(b.reshape(rows, groups, n_ten, chunk), 1, 2).reshape(rows, channels)
            grad = dot_tn(a_list[v], b).astype(BF16)
            grad = lax.psum_scatter(grad, "seq", scatter_dimension=0, tiled=True)
            out.append(lax.psum_scatter(grad, "tensor", scatter_dimension=1, tiled=True).astype(F32))
        return out, line_sum(downs[0], downs[1:])
    count, cols = len(b_list), groups * chunk
    half, steps = share // 2, 4 * count
    anywhere = pl.BlockSpec(memory_space=pl.ANY)
    dma = pltpu.SemaphoreType.DMA

    def room(*dims):
        return pltpu.VMEM(dims, BF16)

    both = len(a_list) + count
    grads, land, _ = pl.pallas_call(
        functools.partial(tail_kernel, lefts, rows, groups, chunk, share),
        out_shape=[
            jax.ShapeDtypeStruct((count, share, cols), F32),
            jax.ShapeDtypeStruct((2, 3, rows, width), BF16),
            jax.ShapeDtypeStruct((3, rows, width), BF16),
        ],
        in_specs=[anywhere] * (both + 1),
        out_specs=[anywhere] * 3,
        scratch_shapes=[
            room(len(a_list), 2 * rows, width), room(count, 4, 2 * rows, cols),
            pltpu.VMEM((share + 64, cols), F32),
            room(steps, share, cols), room(steps, share, cols), room(steps, share, cols),
            room(steps, half, cols), room(steps, half, cols),
            room(steps, share, cols), room(steps, share, cols),
            pltpu.VMEM((count, share, cols), F32),
            room(count, 3, share, cols), room(count, 5, share, cols),
            dma((both, 4 * groups)), dma((count,)), dma((both, 4)), dma((both, 4)),
            dma((steps, 6)), dma((steps, 6)), dma((count, 3)), dma((count, 5)),
            room(rows, width // 4), room(rows, width // 4), dma((3,)), dma((3, 4)), dma((2, 3, 4)),
        ],
        compiler_params=pltpu.CompilerParams(
            collective_id=4, has_side_effects=True, vmem_limit_bytes=67043328
        ),
        cost_estimate=pl.CostEstimate(
            flops=2 * count * rows * width * channels, bytes_accessed=1 << 29, transcendentals=0
        ),
        name="tail",
    )(*a_list, *b_list, downs)
    place = lax.axis_index("tensor")
    down = downs[0].astype(F32)
    for way, label, ok in ((0, 0, place > 0), (1, 0, place == 2), (1, 1, place < 2)):
        down = down + jnp.where(ok, land[way, label].astype(F32), 0.0)
    return grads, down


def feed_kernel(tiles, parts, own_ref, cots_ref, wg_ref, wu_ref, wd_ref, *refs):
    tokens_ref, hid_ref, gg_ref, ug_ref, sum_ref, down_ref = refs[:6]
    (
        wg, wu, wd, tok, cot, hid, gg, ug, part, land, total, down,
        load_sem, store_sem, sum_sem, ag_send, ag_recv, rs_send, rs_recv,
    ) = refs[6:]
    s, t = lax.axis_index("seq"), lax.axis_index("tensor")
    right, left = (s, t + 1), (s, t - 1)
    width, units = wg.shape
    span, cut = width // tiles, units // parts
    greet([(s, (t + 1) % 4), (s, (t + 3) % 4)])

    def pass_on(src, tt, kind):
        return pltpu.make_async_remote_copy(
            src_ref=src, dst_ref=tokens_ref.at[tt], send_sem=ag_send.at[tt, kind],
            recv_sem=ag_recv.at[tt], device_id=left if kind else right, device_id_type=MESH,
        )

    pl.when(t < 3)(lambda: pass_on(own_ref, t, 0).start())
    pl.when(t > 0)(lambda: pass_on(own_ref, t, 1).start())
    weights = [
        pltpu.make_async_copy(src, dst, load_sem.at[2 + k])
        for k, (src, dst) in enumerate(((wg_ref, wg), (wu_ref, wu), (wd_ref, wd)))
    ]
    for move in weights:
        move.start()

    def whose(i):
        third, second, first = pick4(t, 3, 3, 0, 0), pick4(t, 2, 0, 1, 1), pick4(t, 1, 2, 3, 2)
        return pick4(i, t, first, second, third)

    def stores(i):
        ch = whose(i)
        return [
            pltpu.make_async_copy(src, dst.at[ch], store_sem.at[k])
            for k, (src, dst) in enumerate(((hid, hid_ref), (gg, gg_ref), (ug, ug_ref)))
        ]

    def hop(label, k, way):
        return pltpu.make_async_remote_copy(
            src_ref=part.at[label, k], dst_ref=land.at[way, label, k],
            send_sem=rs_send.at[label, k], recv_sem=rs_recv.at[way, label, k],
            device_id=left if way else right, device_id_type=MESH,
        )

    def landed(label, k, way):
        hop(label, k, way).wait_recv()
        return land[way, label, k].astype(F32)

    def put_down(i):
        return pltpu.make_async_copy(down, down_ref.at[i], store_sem.at[4])

    def column(k, size):
        return pl.ds(pl.multiple_of(k * size, 128), size)

    def give(i, k, value):
        label = i - 1

        @pl.when(i == 0)
        def _():
            total[k] = value

        @pl.when((i > 0) & ((i < 3) | (t == 0) | (t == 3)))
        def _():
            part[label, k] = value.astype(BF16)

        @pl.when((i > 0) & (t == 0))
        def _():
            hop(label, k, 0).start()

        @pl.when((i > 0) & (t == 3))
        def _():
            hop(label, k, 1).start()

        @pl.when((i == 3) & (t == 1))
        def _():
            part[2, k] = (value + landed(2, k, 0)).astype(BF16)
            hop(2, k, 0).start()

        @pl.when((i == 3) & (t == 2))
        def _():
            part[2, k] = (value + landed(2, k, 1)).astype(BF16)
            hop(2, k, 1).start()

    @pl.loop(0, 4)
    def _(i):
        ch = whose(i)
        for way in (-1, 1):
            tt = t + way * i
            ok = (i > 0) & (tt >= 0) & (tt <= 3)

            @pl.when(ok)
            def _(tt=tt, way=way):
                pass_on(tokens_ref.at[tt], tt, 0).wait_recv()
                if way < 0:
                    pl.when(t < 3)(lambda: pass_on(tokens_ref.at[tt], tt, 0).start())
                else:
                    pl.when(t > 0)(lambda: pass_on(tokens_ref.at[tt], tt, 1).start())

        get_cot = pltpu.make_async_copy(cots_ref.at[ch], cot, load_sem.at[1])
        get_cot.start()

        @pl.when(i == 0)
        def _():
            move = pltpu.make_async_copy(own_ref, tok, load_sem.at[0])
            move.start()
            move.wait()
            pltpu.make_async_copy(tok, tokens_ref.at[t], store_sem.at[3]).start()
            for move in weights:
                move.wait()

        @pl.when(i == 1)
        def _():
            pltpu.make_async_copy(tok, tokens_ref.at[t], store_sem.at[3]).wait()

        @pl.when(i > 0)
        def _():
            move = pltpu.make_async_copy(tokens_ref.at[ch], tok, load_sem.at[0])
            move.start()
            move.wait()
            for store in stores(i - 1):
                store.wait()
            put_down(i - 1).wait()

        get_cot.wait()

        @pl.loop(0, parts)
        def _(f):
            here = column(f, cut)
            gate_vals = jnp.dot(tok[...], wg[:, here], preferred_element_type=F32)
            up_vals = jnp.dot(tok[...], wu[:, here], preferred_element_type=F32)
            back = lax.dot_general(
                cot[...], wd[here, :], (((1,), (1,)), ((), ())), preferred_element_type=F32
            )
            value, slope = gelu_both(gate_vals)
            hid[:, here] = (value * up_vals).astype(BF16)
            gg[:, here] = (back * up_vals * slope).astype(BF16)
            ug[:, here] = (back * value).astype(BF16)

        for store in stores(i):
            store.start()

        @pl.loop(0, tiles)
        def _(k):
            here = column(k, span)
            value = lax.dot_general(
                gg[...], wg[here, :], (((1,), (1,)), ((), ())), preferred_element_type=F32
            ) + lax.dot_general(
                ug[...], wu[here, :], (((1,), (1,)), ((), ())), preferred_element_type=F32
            )
            give(i, k, value)

        @pl.loop(0, tiles)
        def _(k):
            here = column(k, span)
            down[:, here] = jnp.dot(hid[...], wd[:, here], preferred_element_type=F32).astype(BF16)

        put_down(i).start()

    def add_and_send(k, label, arrived, way):
        part[label, k] = (part[label, k].astype(F32) + landed(arrived, k, way)).astype(BF16)
        hop(label, k, way).start()

    def add_total(k, label, way):
        total[k] = total[k] + landed(label, k, way)

    def put_sum(k):
        return pltpu.make_async_copy(total.at[k], sum_ref.at[:, column(k, span)], sum_sem.at[k])

    @pl.loop(0, tiles)
    def _(k):
        pl.when(t == 1)(lambda: add_and_send(k, 0, 1, 0))
        pl.when(t == 2)(lambda: add_and_send(k, 1, 1, 1))
        pl.when(t == 1)(lambda: add_and_send(k, 1, 2, 1))
        pl.when(t == 2)(lambda: add_and_send(k, 0, 2, 0))

    @pl.loop(0, tiles)
    def _(k):
        pl.when(t == 0)(lambda: add_total(k, 1, 1))
        pl.when(t > 0)(lambda: add_total(k, 0, 0))
        pl.when(t == 1)(lambda: add_total(k, 1, 1))
        pl.when(t == 2)(lambda: add_total(k, 0, 1))
        put_sum(k).start()

    @pl.loop(0, tiles)
    def _(k):
        put_sum(k).wait()
        for label in range(3):
            hop(label, k, 0).wait_send()

    put_down(3).wait()
    for store in stores(3):
        store.wait()
    pl.when(t < 3)(lambda: pass_on(own_ref, t, 0).wait_send())
    pl.when(t > 0)(lambda: pass_on(own_ref, t, 1).wait_send())
    for i in (1, 2, 3):
        pl.when((t - i >= 0) & (t < 3))(
            lambda i=i: pass_on(tokens_ref.at[t - i], t - i, 0).wait_send()
        )
        pl.when((t + i <= 3) & (t > 0))(
            lambda i=i: pass_on(tokens_ref.at[t + i], t + i, 1).wait_send()
        )


def feed_forward(own, cots, w_gate, w_up, w_down):
    rows, width = own.shape
    units = w_gate.shape[1]
    tiles, parts = 4, 5
    anywhere = pl.BlockSpec(memory_space=pl.ANY)
    dma = pltpu.SemaphoreType.DMA

    def room(*dims):
        return pltpu.VMEM(dims, BF16)

    def out(*dims, kind=BF16):
        return jax.ShapeDtypeStruct(dims, kind)

    flops = 2 * 4 * rows * width * units * 6
    got = pl.pallas_call(
        functools.partial(feed_kernel, tiles, parts),
        out_shape=[
            out(4, rows, width), out(4, rows, units), out(4, rows, units), out(4, rows, units),
            out(rows, width, kind=F32), out(4, rows, width),
        ],
        in_specs=[anywhere] * 5,
        out_specs=[anywhere] * 6,
        scratch_shapes=[
            room(width, units), room(width, units), room(units, width),
            room(rows, width), room(rows, width),
            room(rows, units), room(rows, units), room(rows, units),
            room(3, tiles, rows, width // tiles), room(2, 3, tiles, rows, width // tiles),
            pltpu.VMEM((tiles, rows, width // tiles), F32), room(rows, width),
            dma((5,)), dma((5,)), dma((tiles,)), dma((4, 2)), dma((4,)),
            dma((3, tiles)), dma((2, 3, tiles)),
        ],
        compiler_params=pltpu.CompilerParams(
            collective_id=5, has_side_effects=True, vmem_limit_bytes=67043328
        ),
        cost_estimate=pl.CostEstimate(flops=flops, bytes_accessed=3 << 27, transcendentals=0),
        name="feed",
    )(own, cots, w_gate, w_up, w_down)
    return got


def chunk_scan(a_ref, d_ref, p_ref, s_ref, reverse):
    tiles, rows, wide = a_ref.shape
    run = rows // 8

    def first(i, carry):
        r = run - 1 - i if reverse else i
        here = pl.ds(r, 8, stride=run)
        after = []
        for b in range(tiles):
            prod, state = carry[b]
            a = a_ref[b, here, :]
            prod = prod * a
            state = a * state + d_ref[b, here, :]
            a_ref[b, here, :] = prod
            d_ref[b, here, :] = state
            after.append((prod, state))
        return tuple(after)

    start = (jnp.ones((8, wide), F32), jnp.zeros((8, wide), F32))
    ends = lax.fori_loop(0, run, first, (start,) * tiles, unroll=4)
    leads, totals = [], []
    for b in range(tiles):
        prod, state = ends[b]
        enter_p, enter_s = [None] * 8, [None] * 8
        now_p, now_s = jnp.ones((1, wide), F32), jnp.zeros((1, wide), F32)
        for c in range(7, -1, -1) if reverse else range(8):
            enter_p[c], enter_s[c] = now_p, now_s
            now_p, now_s = now_p * prod[c : c + 1], prod[c : c + 1] * now_s + state[c : c + 1]
        leads.append((jnp.concatenate(enter_p, 0), jnp.concatenate(enter_s, 0)))
        totals.append((now_p, now_s))

    def second(r, _):
        here = pl.ds(r, 8, stride=run)
        for b in range(tiles):
            p = a_ref[b, here, :]
            a_ref[b, here, :] = p * leads[b][0]
            d_ref[b, here, :] = d_ref[b, here, :] + p * leads[b][1]
        return 0

    lax.fori_loop(0, run, second, 0, unroll=4)
    for b in range(tiles):
        p_ref[:, b * wide : (b + 1) * wide] = a_ref[b]
        s_ref[:, b * wide : (b + 1) * wide] = d_ref[b]
    return jnp.concatenate([p for p, _ in totals], 1), jnp.concatenate([v for _, v in totals], 1)


def tiled_store(ref, value):
    tiles, _, wide = ref.shape
    for b in range(tiles):
        ref[b] = value[:, b * wide : (b + 1) * wide]


def positions(base_ref, rows, lanes, length):
    place = lax.broadcasted_iota(jnp.int32, (rows, lanes), 0) + base_ref[0]
    return jnp.where(place >= length, place - length, place)


def forward_kernel(
    length, local, base_ref, x_ref, cw_ref, rate_gain_ref, g_ref, sel_ref,
    conv_ref, rate_ref, in_ref, p_ref, s_ref, carry_ref, w_ref, a_ref, d_ref,
):
    rows, lanes = conv_ref.shape
    spot = positions(base_ref, rows, lanes, length)
    x = x_ref[...].astype(F32)
    total = cw_ref[0:1, :] * x[HALO:]
    for k in range(1, CONV):
        moved = pltpu.roll(x, k, 0)[HALO:]
        total = total + jnp.where(spot >= k, cw_ref[k : k + 1, :] * moved, 0.0)
    conv = total.astype(BF16)
    conv_ref[...] = conv
    join = sel_ref.shape[0]
    wide = jnp.dot(g_ref[0], sel_ref[0], preferred_element_type=F32)
    for q in range(1, join):
        other = jnp.dot(g_ref[0], sel_ref[q], preferred_element_type=F32)
        which = lax.broadcasted_iota(jnp.int32, wide.shape, 0) // local % join
        wide = jnp.where(which == q, other, wide)
    gates = wide.astype(BF16)
    w_ref[0] = gates
    pre = lax.dot_general(conv, gates, (((1,), (1,)), ((), ())), preferred_element_type=F32)
    rate, inp = pre[:, :lanes], pre[:, lanes:]
    rate_ref[...] = rate
    in_ref[...] = inp
    decay = jnp.where(spot == 0, 0.0, jnp.exp(rate_gain_ref[...] * jax.nn.sigmoid(rate)))
    tiled_store(a_ref, decay)
    tiled_store(
        d_ref,
        jnp.sqrt(jnp.maximum(1.0 - decay * decay, 0.01)) * jax.nn.sigmoid(inp) * conv.astype(F32),
    )
    prod, state = chunk_scan(a_ref, d_ref, p_ref, s_ref, False)
    carry_ref[0:1, :] = prod
    carry_ref[1:2, :] = state


def middle_kernel(
    length, base_ref, mg_ref, y_ref, p_ref, s_ref, enter_ref, rate_ref, rate_gain_ref,
    ylow_ref, bp_ref, bs_ref, carry_ref, a_ref, d_ref,
):
    rows, lanes = mg_ref.shape
    spot = positions(base_ref, rows, lanes, length)
    states = s_ref[...] + p_ref[...] * enter_ref[...]
    value, slope = gelu_both(y_ref[...])
    grad = mg_ref[...]
    ylow_ref[...] = (grad * states * slope).astype(BF16)
    tiled_store(d_ref, grad * value)
    decay = jnp.where(spot == 0, 0.0, jnp.exp(rate_gain_ref[...] * jax.nn.sigmoid(rate_ref[...])))
    row = lax.broadcasted_iota(jnp.int32, (rows, lanes), 0)
    tiled_store(a_ref, jnp.where(row == rows - 1, 1.0, pltpu.roll(decay, rows - 1, 0)))
    prod, state = chunk_scan(a_ref, d_ref, bp_ref, bs_ref, True)
    carry_ref[0:1, :] = decay[0:1] * prod
    carry_ref[1:2, :] = decay[0:1] * state


def backward_kernel(
    length, local, base_ref, bp_ref, bs_ref, leave_ref, p_ref, s_ref, enter_ref, rate_ref, in_ref,
    conv_ref, rate_gain_ref, w_ref, cw_ref, x_ref, sel_ref,
    gates_ref, xback_ref, edge_ref, small_ref,
):
    rows, lanes = bp_ref.shape
    spot = positions(base_ref, rows, lanes, length)
    row = lax.broadcasted_iota(jnp.int32, (rows, lanes), 0)
    adjoint = bs_ref[...] + bp_ref[...] * leave_ref[...]
    states = s_ref[...] + p_ref[...] * enter_ref[...]
    before = jnp.where(row == 0, enter_ref[...], pltpu.roll(states, 1, 0))
    gain = rate_gain_ref[...]
    sig_r = jax.nn.sigmoid(rate_ref[...])
    sig_i = jax.nn.sigmoid(in_ref[...])
    conv = conv_ref[...]
    conv_f = conv.astype(F32)
    decay = jnp.where(spot == 0, 0.0, jnp.exp(gain * sig_r))
    room = 1.0 - decay * decay
    scale = jnp.sqrt(jnp.maximum(room, 0.01))
    pulled = adjoint * sig_i
    slope = jnp.where(room > 0.01, -decay / scale, 0.0)
    decay_grad = adjoint * before + pulled * conv_f * slope
    log_grad = decay_grad * decay
    pull_r = log_grad * sig_r
    rate_back = (pull_r * gain * (1.0 - sig_r)).astype(BF16)
    conv_direct = pulled * scale
    in_back = (conv_direct * conv_f * (1.0 - sig_i)).astype(BF16)
    both = jnp.concatenate([rate_back, in_back], 1)
    join = sel_ref.shape[0]
    for q in range(join):
        some = lax.dot_general(
            conv, sel_ref[q], (((1,), (1,)), ((), ())), preferred_element_type=F32
        ).astype(BF16)
        part = lax.dot_general(some, both, (((0,), (0,)), ((), ())), preferred_element_type=F32)
        if q == 0:
            gate_sum = part
        else:
            which = lax.broadcasted_iota(jnp.int32, part.shape, 1) // local % join
            gate_sum = jnp.where(which == q, part, gate_sum)
    gates_ref[0] = gate_sum.astype(BF16)
    grad = conv_direct + lax.dot_general(
        both, w_ref[0], (((1,), (0,)), ((), ())), preferred_element_type=F32
    )
    x = x_ref[...].astype(F32)
    zeros = jnp.zeros((HALO, lanes), F32)
    out = jnp.concatenate([zeros, grad * cw_ref[0:1, :]], 0)
    small_ref[0:1, :] = jnp.sum(grad * x[HALO:], axis=0, keepdims=True)
    for k in range(1, CONV):
        masked = jnp.where(spot >= k, grad, 0.0)
        small_ref[k : k + 1, :] = jnp.sum(
            masked * pltpu.roll(x, k, 0)[HALO:], axis=0, keepdims=True
        )
        tall = jnp.concatenate([zeros, masked * cw_ref[k : k + 1, :]], 0)
        out = out + pltpu.roll(tall, rows + HALO - k, 0)
    small_ref[CONV : CONV + 1, :] = jnp.sum(pull_r, axis=0, keepdims=True)
    small_ref[CONV + 1 : 8, :] = jnp.zeros((7 - CONV, lanes), F32)
    edge_ref[...] = out[:HALO]
    xback_ref[...] = out[HALO:]


def lane_call(kernel, grid, lanes, base, operands, outputs, scratch, flops):
    def spec(shape):
        if len(shape) == 3 and shape[0] != grid:
            return pl.BlockSpec(shape, lambda j, *_: (0, 0, 0))
        if len(shape) == 3:
            return pl.BlockSpec((1,) + shape[1:], lambda j, *_: (j, 0, 0))
        return pl.BlockSpec((shape[0], lanes), lambda j, *_: (0, j))

    moved = sum(math.prod(a.shape) * a.dtype.itemsize for a in list(operands) + list(outputs))
    return pl.pallas_call(
        kernel,
        grid_spec=pltpu.PrefetchScalarGridSpec(
            num_scalar_prefetch=1,
            grid=(grid,),
            in_specs=[spec(a.shape) for a in operands],
            out_specs=[spec(a.shape) for a in outputs],
            scratch_shapes=scratch,
        ),
        out_shape=outputs,
        compiler_params=pltpu.CompilerParams(
            dimension_semantics=("arbitrary",), vmem_limit_bytes=56 << 20
        ),
        cost_estimate=pl.CostEstimate(flops=flops, bytes_accessed=moved, transcendentals=0),
    )(base, *operands)


def shards(
    tokens_in, gain_pre, w_x, w_y, conv_w, gate_a, gate_i, decay_param, w_out,
    gain_mlp, w_gate, w_up, w_down, cotangent,
):
    rows, width = tokens_in.shape
    heads, local = w_x.shape[1:]
    n_ten, n_seq = lax.axis_size("tensor"), lax.axis_size("seq")
    devices = n_ten * n_seq
    place, run = lax.axis_index("tensor"), lax.axis_index("seq")
    linear = run * n_ten + place
    length = devices * rows // SEQS
    base = jnp.reshape((linear * rows) % length, (1,)).astype(jnp.int32)
    join = 128 // local if local < 128 and heads % (128 // local) == 0 else 1
    groups, chunk = heads // join, join * local
    lanes = n_ten * chunk
    channels = groups * lanes

    def shape(dims, kind=F32):
        return jax.ShapeDtypeStruct(dims, kind)

    def own_columns(array):
        n = array.shape[0]
        split = array.reshape(n, groups, n_ten, chunk)
        return lax.dynamic_index_in_dim(split, place, 2, False).reshape(n, heads, local)

    gate_rows = jnp.stack([gate_a, gate_i], 0).swapaxes(2, 3).reshape(2 * heads, local, n_ten * local)
    params = jnp.concatenate([conv_w, decay_param[None]], 0).reshape(CONV + 1, heads * local)
    params = jnp.pad(params, ((0, 7 - CONV), (0, 0)))
    (all_gates, full_x, full_y, full_out), params, cots, halo = gather_all(
        [
            gate_rows,
            jnp.transpose(w_x, (1, 2, 0)).reshape(groups, chunk, width),
            jnp.transpose(w_y, (1, 2, 0)).reshape(groups, chunk, width),
            w_out.reshape(groups, chunk, width),
        ],
        params, cotangent, tokens_in, HALO,
    )
    halo = jnp.where(linear == 0, jnp.zeros_like(halo), halo)
    full_x, full_y, full_out = (w.reshape(channels, width) for w in (full_x, full_y, full_out))
    gates = all_gates.reshape(2, groups, join, n_ten, local, n_ten * local)
    gates = jnp.transpose(gates, (1, 0, 3, 2, 4, 5)).reshape(groups, 2 * lanes, n_ten * local)
    key = jnp.arange(n_ten * local)[None, :, None]
    lane = jnp.arange(lanes)[None, None, :]
    member = jnp.arange(join)[:, None, None]
    select = (
        (lane // chunk == key // local) & (lane % local == key % local) & (lane // local % join == member)
    ).astype(BF16)
    params = jnp.transpose(params.reshape(n_ten, 8, groups, chunk), (1, 2, 0, 3)).reshape(8, channels)
    conv_rows, decay_full = params, params[CONV : CONV + 1]
    rate_gain = -8.0 * jax.nn.softplus(decay_full)

    own_in = tokens_in.astype(F32)
    in_scale, in_unit = rms_parts(own_in)
    normed = (in_unit * gain_pre).astype(BF16)
    normed_halo = (rms_parts(halo.astype(F32))[1] * gain_pre).astype(BF16)
    x_long = dot_nt(jnp.concatenate([normed_halo, normed], 0), full_x).astype(BF16)
    y_branch = dot_nt(normed, full_y)
    scratch = [pltpu.VMEM((lanes // 128, rows, 128), F32)] * 2
    conv_out, rate_pre, input_pre, products, partial, carry, wide_gates = lane_call(
        functools.partial(forward_kernel, length, local), groups, lanes, base,
        (x_long, conv_rows, rate_gain, gates, select),
        [
            shape((rows, channels), BF16),
            shape((rows, channels)),
            shape((rows, channels)),
            shape((rows, channels)),
            shape((rows, channels)),
            shape((2, channels)),
            shape((groups, 2 * lanes, lanes), BF16),
        ],
        scratch, 4 * rows * lanes * channels,
    )
    reach = min(-(-length // rows), devices - 1)
    enter = entering(carry, reach, linear, devices, False)
    states = partial + products * enter
    mixed = (states * jax.nn.gelu(y_branch, approximate=True)).astype(BF16)
    middle = own_in + dot_nn(mixed, full_out)
    mid_scale, mid_unit = rms_parts(middle)
    normed_mlp = (mid_unit * gain_mlp).astype(BF16)

    if n_ten == 4 and n_seq == 8:
        *kept, mlp_input, downs = feed_forward(normed_mlp, cots, w_gate, w_up, w_down)
        cot_rows = cots.reshape(n_ten * rows, width)
        token_rows, hidden_rows, gate_rows, up_rows = (
            a.reshape(n_ten * rows, a.shape[2]) for a in kept
        )
    else:
        cots = [cotangent] + [
            lax.dynamic_index_in_dim(cots, label_index(k), 0, False) for k in range(1, n_ten)
        ]
        tokens = [normed_mlp] + others(normed_mlp)
        hiddens, gate_grads, up_grads, downs, pulls = [], [], [], [], []
        for n, c in zip(tokens, cots):
            gate_vals, up_vals = dot_nn(n, w_gate), dot_nn(n, w_up)
            value, slope = gelu_both(gate_vals)
            hidden = (value * up_vals).astype(BF16)
            hidden_grad = dot_nt(c, w_down)
            gate_grad = (hidden_grad * up_vals * slope).astype(BF16)
            up_grad = (hidden_grad * value).astype(BF16)
            hiddens.append(hidden)
            gate_grads.append(gate_grad)
            up_grads.append(up_grad)
            pulls.append(dot_nt(gate_grad, w_gate) + dot_nt(up_grad, w_up))
            downs.append(dot_nn(hidden, w_down).astype(BF16))
        mlp_input = line_sum(pulls[0], [p.astype(BF16) for p in pulls[1:]])
        cot_rows, token_rows, hidden_rows, gate_rows, up_rows = (
            jnp.concatenate(a, 0) for a in (cots, tokens, hiddens, gate_grads, up_grads)
        )
    grad_down = dot_tn(hidden_rows, cot_rows).astype(BF16)
    grad_gate = dot_tn(token_rows, gate_rows).astype(BF16)
    grad_up = dot_tn(token_rows, up_rows).astype(BF16)
    gain_mlp_part, mid_back = rms_back(mlp_input, gain_mlp, mid_scale, mid_unit)
    middle_grad = cotangent.astype(F32) + mid_back
    middle_low, grad_down, grad_gate, grad_up = lax.optimization_barrier(
        (middle_grad.astype(BF16), grad_down, grad_gate, grad_up)
    )
    grad_down = lax.psum_scatter(grad_down, "seq", scatter_dimension=1, tiled=True)
    grad_gate = lax.psum_scatter(grad_gate, "seq", scatter_dimension=0, tiled=True)
    grad_up = lax.psum_scatter(grad_up, "seq", scatter_dimension=0, tiled=True)
    mixed_grad = dot_nt(middle_low, full_out)
    y_low, back_products, back_partial, carry = lane_call(
        functools.partial(middle_kernel, length), groups, lanes, base,
        (mixed_grad, y_branch, products, partial, enter, rate_pre, rate_gain),
        [
            shape((rows, channels), BF16),
            shape((rows, channels)),
            shape((rows, channels)),
            shape((2, channels)),
        ],
        scratch, 60 * rows * channels,
    )
    leave = entering(carry, reach, linear, devices, True)
    gate_parts, x_back, edge, sums = lane_call(
        functools.partial(backward_kernel, length, local), groups, lanes, base,
        (
            back_products, back_partial, leave, products, partial, enter, rate_pre, input_pre,
            conv_out, rate_gain, wide_gates, conv_rows, x_long, select,
        ),
        [
            shape((groups, n_ten * local, 2 * lanes), BF16),
            shape((rows, channels)),
            shape((HALO, channels)),
            shape((8, channels)),
        ],
        [], 8 * rows * lanes * channels,
    )
    edge = lax.ppermute(edge, BOTH, [(i + 1, i) for i in range(devices - 1)])
    x_low = jnp.concatenate(
        [x_back[: rows - HALO], x_back[rows - HALO :] + edge], 0
    ).astype(BF16)

    (grad_out, grad_y, grad_x), down = weight_grads(
        (0, 1, 1), [middle_low, normed], [mixed, y_low, x_low], groups, downs
    )
    block_out = (middle + down).astype(BF16)
    normed_grad = dot_nn(x_low, full_x) + dot_nn(y_low, full_y)
    gain_pre_part, in_back = rms_back(normed_grad, gain_pre, in_scale, in_unit)
    input_grad = middle_grad + in_back

    part = n_ten * local // n_seq
    split = gate_parts.reshape(groups, n_seq, part, 2, n_ten, chunk)
    split = jnp.transpose(split, (1, 4, 0, 3, 2, 5)).reshape(devices, groups * 2 * part, chunk)
    gate_sum = lax.psum_scatter(split, BOTH, scatter_dimension=0, tiled=True).astype(F32)
    gate_sum = gate_sum.reshape(groups, 2, part, join, local)
    gate_sum = jnp.transpose(gate_sum, (1, 0, 3, 2, 4)).reshape(2, heads, part, local)
    packed = jnp.concatenate([sums[: CONV + 1], gain_pre_part[None], gain_mlp_part[None]], 0)
    packed = lax.psum(packed, BOTH)
    conv_sum = own_columns(packed[:CONV])
    decay_sum = own_columns(packed[CONV : CONV + 1] * (-8.0 * jax.nn.sigmoid(decay_full)))[0]
    share = local // n_seq
    grad_conv = lax.dynamic_slice_in_dim(conv_sum, run * share, share, 2)
    grad_decay = lax.dynamic_slice_in_dim(decay_sum, run * share, share, 1)
    grad_gain_mlp = lax.dynamic_slice_in_dim(
        packed[CONV + 2], run * (width // n_seq), width // n_seq, 0
    )

    def weight(grad):
        return grad.T.reshape(heads, local, -1)

    return (
        block_out,
        input_grad,
        packed[CONV + 1],
        jnp.transpose(weight(grad_x), (2, 0, 1)),
        jnp.transpose(weight(grad_y), (2, 0, 1)),
        grad_conv,
        gate_sum[0],
        gate_sum[1],
        grad_decay,
        weight(grad_out),
        grad_gain_mlp,
        grad_gate.astype(F32),
        grad_up.astype(F32),
        grad_down.astype(F32),
    )


def solution(mesh):
    placed = (
        P(("seq", "tensor"), None),
        P(),
        P(None, None, "tensor"),
        P(None, None, "tensor"),
        P(None, None, "tensor"),
        P(None, None, "tensor"),
        P(None, None, "tensor"),
        P(None, "tensor"),
        P(None, "tensor", None),
        P(),
        P(None, "tensor"),
        P(None, "tensor"),
        P("tensor", None),
        P(("seq", "tensor"), None),
    )

    return jax.shard_map(
        shards,
        mesh=mesh,
        in_specs=placed,
        out_specs=(
            P(("seq", "tensor"), None),
            P(("seq", "tensor"), None),
            P(),
            P("seq", None, "tensor"),
            P("seq", None, "tensor"),
            P(None, None, ("tensor", "seq")),
            P(None, "seq", "tensor"),
            P(None, "seq", "tensor"),
            P(None, ("tensor", "seq")),
            P(None, "tensor", "seq"),
            P("seq"),
            P("seq", "tensor"),
            P("seq", "tensor"),
            P("tensor", "seq"),
        ),
        check_vma=False,
    )
```

```python
import functools
import math

import jax
import jax.numpy as jnp
from jax import lax
from jax.experimental import pallas as pl
from jax.experimental.pallas import tpu as pltpu
from jax.sharding import PartitionSpec as P

CONV = 4
SEQS = 3
HALO = 16
epsilon = 1e-06
F32 = jnp.float32
BF16 = jnp.bfloat16
ROOT = math.sqrt(2.0 / math.pi)
BOTH = ("seq", "tensor")


def dot_nn(a, b):
    return lax.dot_general(a, b, (((1,), (0,)), ((), ())), preferred_element_type=F32)


def dot_nt(a, b):
    return lax.dot_general(a, b, (((1,), (1,)), ((), ())), preferred_element_type=F32)


def dot_tn(a, b):
    return lax.dot_general(a, b, (((0,), (0,)), ((), ())), preferred_element_type=F32)


def rms_parts(values):
    scale = lax.rsqrt(jnp.mean(values * values, axis=-1, keepdims=True) + epsilon)
    return scale, values * scale


def rms_back(grad, gain, scale, unit):
    pulled = gain * grad
    inner = jnp.mean(pulled * unit, axis=-1, keepdims=True)
    return jnp.sum(grad * unit, axis=0), scale * (pulled - unit * inner)


def gelu_both(v):
    inner = v * v
    th = jnp.tanh(ROOT * (v + 0.044715 * v * inner))
    half = 0.5 * (1.0 + th)
    slope = half + 0.5 * v * (1.0 - th * th) * (ROOT * (1.0 + 3 * 0.044715 * inner))
    return v * half, slope


LABELS = ((1, 2, 3, 2), (2, 0, 1, 1), (3, 3, 0, 0))


def along(block, pairs):
    return lax.ppermute(block, "tensor", pairs)


def line_streams(own):
    right, left = [], []
    right.append(along(own, [(0, 1), (1, 2), (2, 3)]))
    left.append(along(own, [(1, 0), (2, 1), (3, 2)]))
    right.append(along(right[0], [(1, 2), (2, 3)]))
    left.append(along(left[0], [(1, 0), (2, 1)]))
    right.append(along(right[1], [(2, 3)]))
    left.append(along(left[1], [(1, 0)]))
    return right, left


def others(own):
    count = lax.axis_size("tensor")
    place = lax.axis_index("tensor")
    if count == 4:
        right, left = line_streams(own)
        first = jnp.where(place == 3, right[0], left[0])
        second = jnp.where(place == 0, left[1], jnp.where(place == 3, right[1], right[0]))
        third = jnp.where(
            place == 0, left[2], jnp.where(place == 1, left[1], jnp.where(place == 2, right[1], right[2]))
        )
        return [first, second, third]
    whole = lax.all_gather(own, "tensor", axis=0)
    return [lax.dynamic_index_in_dim(whole, (place + k) % count, 0, False) for k in range(1, count)]


def label_index(k):
    count = lax.axis_size("tensor")
    place = lax.axis_index("tensor")
    if count == 4:
        table = LABELS[k - 1]
        return jnp.where(
            place == 0, table[0], jnp.where(place == 1, table[1], jnp.where(place == 2, table[2], table[3]))
        )
    return (place + k) % count


def in_order(own):
    count = lax.axis_size("tensor")
    place = lax.axis_index("tensor")
    if count == 4:
        right, left = line_streams(own)
        rows = []
        for want in range(4):
            pick = own
            for at in range(4):
                if at < want:
                    pick = jnp.where(place == at, left[want - at - 1], pick)
                elif at > want:
                    pick = jnp.where(place == at, right[at - want - 1], pick)
            rows.append(pick)
        return jnp.stack(rows, 0)
    return lax.all_gather(own, "tensor", axis=0)


def line_sum(own, parts):
    count = lax.axis_size("tensor")
    place = lax.axis_index("tensor")
    if count == 4:
        first, second, third = parts
        end = (place == 0) | (place == 3)
        right = along(third, [(0, 1)])
        left = along(third, [(3, 2)])
        arrived = jnp.where(place == 1, right, left)
        send = jnp.where(
            end, second, (third.astype(F32) + arrived.astype(F32)).astype(BF16)
        )
        right = along(send, [(0, 1), (1, 2)])
        left = along(send, [(3, 2), (2, 1)])
        send_right = (first.astype(F32) + right.astype(F32)).astype(BF16)
        send_left = (
            jnp.where(place == 3, first, second).astype(F32) + left.astype(F32)
        ).astype(BF16)
        right = along(send_right, [(0, 1), (1, 2), (2, 3)])
        left = along(send_left, [(3, 2), (2, 1), (1, 0)])
        return own.astype(F32) + right.astype(F32) + left.astype(F32)
    stack = jnp.zeros((count,) + own.shape, BF16)
    stack = lax.dynamic_update_index_in_dim(stack, own.astype(BF16), place, 0)
    for k in range(1, count):
        stack = lax.dynamic_update_index_in_dim(stack, parts[k - 1], label_index(k), 0)
    return lax.psum_scatter(stack, "tensor", scatter_dimension=0, tiled=False).astype(F32)


MESH = pl.DeviceIdType.MESH


def ring_places():
    s, t = lax.axis_index("seq"), lax.axis_index("tensor")
    c, x, y = s % 2, (s // 2) % 2, s // 4
    return s, t, c, x, y


def greet(targets):
    barrier = pltpu.get_barrier_semaphore()
    for target in targets:
        pl.semaphore_signal(barrier, inc=1, device_id=target, device_id_type=MESH)
    pl.semaphore_wait(barrier, len(targets))


def gather_kernel(count, *refs):
    weights, (small, cot, tokens) = refs[:count], refs[count : count + 3]
    full = refs[count + 3 : 2 * count + 3]
    smalls, cots, halo = refs[2 * count + 3 : 2 * count + 6]
    rest = refs[2 * count + 6 :]
    stage, rest = rest[: count + 2], rest[count + 2 :]
    local_sem, send_sem, recv_sem, line_send, line_recv, halo_sem = rest
    s, t, c, x, y = ring_places()
    s_core, s_x, s_y = s + 1 - 2 * c, s + 2 - 4 * x, s + 4 - 8 * y
    s_far = s_x + 4 - 8 * y
    right, left = (s, t + 1), (s, t - 1)
    near_x, near_y, core = (s_x, t), (s_y, t), (s_core, t)
    linear = 4 * s + t
    after, before = (linear + 1) % 32, (linear + 31) % 32
    greet(
        [(s, (t + 1) % 4), (s, (t + 3) % 4), near_x, near_y, core, (before // 4, before % 4)]
    )
    sent = []
    tail_rows = halo.shape[0]
    onward = pltpu.make_async_remote_copy(
        src_ref=tokens.at[pl.ds(tokens.shape[0] - tail_rows, tail_rows)], dst_ref=halo,
        send_sem=halo_sem.at[0], recv_sem=halo_sem.at[1],
        device_id=(after // 4, after % 4), device_id_type=MESH,
    )
    pl.when(linear < 31)(onward.start)

    def slot(w, tt, ss):
        return full[w].at[:, tt, ss]

    def copy(w, src, tt, ss, kind, target):
        return pltpu.make_async_remote_copy(
            src_ref=src, dst_ref=slot(w, tt, ss), send_sem=send_sem.at[w, tt, kind],
            recv_sem=recv_sem.at[w, tt, ss], device_id=target, device_id_type=MESH,
        )

    def arrived(w, tt, ss):
        copy(w, slot(w, tt, ss), tt, ss, 0, core).wait_recv()

    def send(w, src, tt, ss, kind, target, when=None):
        def go():
            copy(w, src, tt, ss, kind, target).start()

        def done():
            copy(w, src, tt, ss, kind, target).wait_send()

        if when is None:
            go()
            sent.append(done)
        else:
            pl.when(when)(go)
            sent.append(lambda: pl.when(when)(done))

    def spread(w, src, tt):
        send(w, src, tt, s, 2, near_x)
        send(w, src, tt, s, 3, near_y)
        send(w, src, tt, s, 4, core)

    def open_line(w):
        own = weights[w].at[:, s]
        send(w, own, t, s, 0, right, t < 3)
        send(w, own, t, s, 1, left, t > 0)
        spread(w, own, t)

    def line_events(w):
        for k in (1, 2, 3):
            for way in (-1, 1):
                tt = t + way * k

                def event(tt=tt, way=way, tail=sent):
                    arrived(w, tt, s)
                    if way < 0:
                        pl.when(t < 3)(lambda: copy(w, slot(w, tt, s), tt, s, 0, right).start())
                    else:
                        pl.when(t > 0)(lambda: copy(w, slot(w, tt, s), tt, s, 1, left).start())
                    copy(w, slot(w, tt, s), tt, s, 2, near_x).start()
                    copy(w, slot(w, tt, s), tt, s, 3, near_y).start()
                    copy(w, slot(w, tt, s), tt, s, 4, core).start()

                def finish(tt=tt, way=way):
                    if way < 0:
                        pl.when(t < 3)(lambda: copy(w, slot(w, tt, s), tt, s, 0, right).wait_send())
                    else:
                        pl.when(t > 0)(lambda: copy(w, slot(w, tt, s), tt, s, 1, left).wait_send())
                    for kind, target in ((2, near_x), (3, near_y), (4, core)):
                        copy(w, slot(w, tt, s), tt, s, kind, target).wait_send()

                ok = tt >= 0 if way < 0 else tt <= 3
                pl.when(ok)(event)
                sent.append(lambda ok=ok, finish=finish: pl.when(ok)(finish))

    def plane_events(w):
        for tt in range(4):
            arrived(w, tt, s_x)
            send(w, slot(w, tt, s_x), tt, s_x, 6, core)
            if tt % 2 == 0:
                send(w, slot(w, tt, s_x), tt, s_x, 5, near_y)
            arrived(w, tt, s_y)
            send(w, slot(w, tt, s_y), tt, s_y, 8, core)
            if tt % 2 == 1:
                send(w, slot(w, tt, s_y), tt, s_y, 7, near_x)

    def far_events(w):
        for tt in range(4):
            arrived(w, tt, s_far)
            send(w, slot(w, tt, s_far), tt, s_far, 9, core)

    def core_events(w):
        for tt in range(4):
            for base in (s, s_x, s_y, s_far):
                arrived(w, tt, base + 1 - 2 * c)

    lines = ((small, smalls), (cot, cots))

    def line_copy(v, src, tt, kind, target):
        return pltpu.make_async_remote_copy(
            src_ref=src, dst_ref=lines[v][1].at[tt], send_sem=line_send.at[v, tt, kind],
            recv_sem=line_recv.at[v, tt], device_id=target, device_id_type=MESH,
        )

    def open_other(v):
        own = lines[v][0]
        pl.when(t < 3)(lambda: line_copy(v, own, t, 0, right).start())
        pl.when(t > 0)(lambda: line_copy(v, own, t, 1, left).start())
        sent.append(lambda: pl.when(t < 3)(lambda: line_copy(v, own, t, 0, right).wait_send()))
        sent.append(lambda: pl.when(t > 0)(lambda: line_copy(v, own, t, 1, left).wait_send()))

    def other_events(v, k):
        whole = lines[v][1]
        for way in (-1, 1):
            tt = t + way * k
            kind, target = (0, right) if way < 0 else (1, left)
            more = t < 3 if way < 0 else t > 0

            def event(tt=tt, kind=kind, target=target, more=more):
                line_copy(v, whole.at[tt], tt, kind, target).wait_recv()
                pl.when(more)(lambda: line_copy(v, whole.at[tt], tt, kind, target).start())

            def finish(tt=tt, kind=kind, target=target, more=more):
                pl.when(more)(lambda: line_copy(v, whole.at[tt], tt, kind, target).wait_send())

            ok = tt >= 0 if way < 0 else tt <= 3
            pl.when(ok)(event)
            sent.append(lambda ok=ok, finish=finish: pl.when(ok)(finish))

    into = [pltpu.make_async_copy(weights[w].at[:, s], stage[w], local_sem.at[w]) for w in range(count)]
    out = [pltpu.make_async_copy(stage[w], slot(w, t, s), local_sem.at[w]) for w in range(count)]
    for v, (own, whole) in enumerate(lines):
        into.append(pltpu.make_async_copy(own, stage[count + v], local_sem.at[count + v]))
        out.append(pltpu.make_async_copy(stage[count + v], whole.at[t], local_sem.at[count + v]))

    open_other(0)
    for w in range(count):
        open_line(w)
    for move in into:
        move.start()
    line_events(0)
    line_events(1)
    for a, b in zip(into, out):
        a.wait()
        b.start()
    open_other(1)
    plane_events(0)
    line_events(2)
    far_events(0)
    plane_events(1)
    line_events(3)
    far_events(1)
    other_events(1, 1)
    plane_events(2)
    far_events(2)
    other_events(1, 2)
    plane_events(3)
    for k in (1, 2, 3):
        other_events(0, k)
    other_events(1, 3)
    far_events(3)
    for w in range(count):
        core_events(w)
    for move in out:
        move.wait()
    for done in sent:
        done()
    pl.when(linear > 0)(onward.wait_recv)
    pl.when(linear < 31)(onward.wait_send)


def gather_all(weights, small, cotangent, tokens, tail_rows):
    n_ten, n_seq = lax.axis_size("tensor"), lax.axis_size("seq")
    if not (n_ten == 4 and n_seq == 8):
        full = [jnp.moveaxis(lax.all_gather(w, "tensor", axis=0), 0, 1) for w in weights]
        devices = n_ten * n_seq
        halo = lax.ppermute(
            tokens[tokens.shape[0] - tail_rows :], BOTH, [(i, i + 1) for i in range(devices - 1)]
        )
        whole = (lax.all_gather(a, "tensor", axis=0) for a in (small, cotangent))
        return full, *whole, halo
    count = len(weights)
    cut = [w.reshape(w.shape[0], 8, w.shape[1] // 8, w.shape[2]) for w in weights]
    anywhere = pl.BlockSpec(memory_space=pl.ANY)
    outs = [jax.ShapeDtypeStruct((w.shape[0], 4) + w.shape[1:], w.dtype) for w in cut]
    outs += [jax.ShapeDtypeStruct((4,) + a.shape, a.dtype) for a in (small, cotangent)]
    outs.append(jax.ShapeDtypeStruct((tail_rows, tokens.shape[1]), tokens.dtype))
    dma = pltpu.SemaphoreType.DMA
    got = pl.pallas_call(
        functools.partial(gather_kernel, count),
        out_shape=outs,
        in_specs=[anywhere] * (count + 3),
        out_specs=[anywhere] * (count + 3),
        scratch_shapes=[pltpu.VMEM((w.shape[0],) + w.shape[2:], w.dtype) for w in cut]
        + [pltpu.VMEM(a.shape, a.dtype) for a in (small, cotangent)]
        + [
            dma((count + 2,)), dma((count, 4, 10)), dma((count, 4, 8)),
            dma((2, 4, 2)), dma((2, 4)), dma((2,)),
        ],
        compiler_params=pltpu.CompilerParams(collective_id=1, has_side_effects=True),
        name="gather",
    )(*cut, small, cotangent, tokens)
    full = [g.reshape(w.shape[0], 4, w.shape[1], w.shape[2]) for g, w in zip(got, weights)]
    return full, *got[count:]


def carry_kernel(reach, reverse, carry_ref, out_ref, send_sem, recv_sem):
    n_ten = lax.axis_size("tensor")
    devices = n_ten * lax.axis_size("seq")
    me = lax.axis_index("seq") * n_ten + lax.axis_index("tensor")
    way = -1 if reverse else 1

    def place(linear):
        return linear // n_ten, linear % n_ten

    greet([place((me - way * k + devices) % devices) for k in range(1, reach + 1)])

    def copy(k):
        return pltpu.make_async_remote_copy(
            src_ref=carry_ref, dst_ref=out_ref.at[k - 1], send_sem=send_sem.at[k - 1],
            recv_sem=recv_sem.at[k - 1], device_id=place((me + way * k + devices) % devices),
            device_id_type=MESH,
        )

    def there(k, back):
        spot = me - way * k if back else me + way * k
        return (spot >= 0) & (spot < devices)

    for k in range(1, reach + 1):
        pl.when(there(k, False))(lambda k=k: copy(k).start())
    for k in range(1, reach + 1):
        pl.when(there(k, True))(lambda k=k: copy(k).wait_recv())
        pl.when(there(k, False))(lambda k=k: copy(k).wait_send())


def entering(carry, reach, linear, devices, reverse):
    channels = carry.shape[1]
    vmem = pl.BlockSpec(memory_space=pltpu.VMEM)
    got = pl.pallas_call(
        functools.partial(carry_kernel, reach, reverse),
        out_shape=jax.ShapeDtypeStruct((reach, 2, channels), F32),
        in_specs=[vmem],
        out_specs=vmem,
        scratch_shapes=[pltpu.SemaphoreType.DMA((reach,)), pltpu.SemaphoreType.DMA((reach,))],
        compiler_params=pltpu.CompilerParams(
            collective_id=3 if reverse else 2, has_side_effects=True
        ),
        name="carry_back" if reverse else "carry",
    )(carry)
    state = jnp.zeros((1, channels), F32)
    for k in range(reach, 0, -1):
        source = linear + k if reverse else linear - k
        there = (source >= 0) & (source < devices)
        state = jnp.where(there, got[k - 1, 0:1] * state + got[k - 1, 1:2], state)
    return state


def pick4(t, a, b, c, d):
    return jnp.where(t == 0, a, jnp.where(t == 1, b, jnp.where(t == 2, c, d)))


def tail_kernel(lefts, rows, groups, chunk, share, *refs):
    n_a, n_b = max(lefts) + 1, len(lefts)
    a_refs, b_refs = refs[:n_a], refs[n_a : n_a + n_b]
    down_ref, gates_ref, small_ref, out_ref, land_ref, gates_out, small_out = refs[
        n_a + n_b : n_a + n_b + 7
    ]
    (
        a_all, b_all, product, to_x, to_y, to_far, far_x, far_y, from_x, from_y, total,
        line_send, line_recv, fill_sem, out_sem, pair_send, pair_recv,
        send_sem, recv_sem, zs_sem, zr_sem,
        down_send, down_recv,
        g_core, g_own, g_far, g_from, g_line, g_total, g_load, g_send, g_recv,
        acc, got, line, small_total, s_load, s_send, s_recv,
    ) = refs[n_a + n_b + 7 :]
    cols = groups * chunk
    s, t = lax.axis_index("seq"), lax.axis_index("tensor")
    c, x, y = s % 2, (s // 2) % 2, s // 4
    p = s // 2
    p_x, p_y = p + 1 - 2 * x, p + 2 - 4 * y
    p_far = p_x + 2 - 4 * y
    near_x, near_y, core = (s + 2 - 4 * x, t), (s + 4 - 8 * y, t), (s + 1 - 2 * c, t)
    right, left = (s, t + 1), (s, t - 1)
    greet([(s, (t + k) % 4) for k in (1, 2, 3)] + [near_x, near_y, core])
    half = share // 2
    steps = 4 * n_b

    def pass_down(label):
        third, second, first = pick4(t, 3, 3, 0, 0), pick4(t, 2, 0, 1, 1), pick4(t, 1, 2, 3, 2)
        target = (first, second, third)[label]
        return pltpu.make_async_remote_copy(
            src_ref=down_ref.at[label + 1], dst_ref=land_ref.at[t], send_sem=down_send.at[label],
            recv_sem=down_recv.at[t], device_id=(s, target), device_id_type=MESH,
        )

    def down_here(tt):
        return pltpu.make_async_remote_copy(
            src_ref=down_ref.at[0], dst_ref=land_ref.at[tt], send_sem=down_send.at[0],
            recv_sem=down_recv.at[tt], device_id=core, device_id_type=MESH,
        )

    def g_copy(k, src, dst, target):
        return pltpu.make_async_remote_copy(
            src_ref=src, dst_ref=dst, send_sem=g_send.at[k], recv_sem=g_recv.at[k],
            device_id=target, device_id_type=MESH,
        )

    g_pair = g_copy(0, gates_ref.at[:, 1 - c], g_core, core)
    g_fill = pltpu.make_async_copy(gates_ref.at[:, c], g_own, g_load.at[0])
    g_fars = (
        g_copy(1, g_own.at[p_far, pl.ds(0, 2)], g_far.at[0], near_x),
        g_copy(2, g_own.at[p_far, pl.ds(2, 2)], g_far.at[1], near_y),
    )
    g_nears = (
        g_copy(3, g_own.at[p_x], g_from.at[0], near_x),
        g_copy(4, g_own.at[p_y], g_from.at[1], near_y),
    )

    def g_hop(k, back):
        other = (t - k + 4) % 4 if back else (t + k) % 4
        return pltpu.make_async_remote_copy(
            src_ref=g_own.at[p, other], dst_ref=g_line.at[other if back else t],
            send_sem=g_send.at[4 + k], recv_sem=g_recv.at[4 + k],
            device_id=(s, other), device_id_type=MESH,
        )

    g_store = pltpu.make_async_copy(g_total, gates_out, g_load.at[1])

    def s_copy(k, target):
        return pltpu.make_async_remote_copy(
            src_ref=acc.at[k], dst_ref=got.at[k], send_sem=s_send.at[k], recv_sem=s_recv.at[k],
            device_id=target, device_id_type=MESH,
        )

    s_turns = (s_copy(0, core), s_copy(1, near_x), s_copy(2, near_y))

    def s_hop(k, back):
        other = (t - k + 4) % 4 if back else (t + k) % 4
        return pltpu.make_async_remote_copy(
            src_ref=acc.at[3], dst_ref=line.at[other if back else t],
            send_sem=s_send.at[2 + k], recv_sem=s_recv.at[2 + k],
            device_id=(s, other), device_id_type=MESH,
        )

    s_fill = pltpu.make_async_copy(small_ref, acc.at[0], s_load.at[0])
    s_store = pltpu.make_async_copy(small_total, small_out, s_load.at[1])

    def small_steps(n):
        @pl.when(n == 0)
        def _():
            s_fill.wait()
            s_turns[0].start()

        @pl.when(n == 1)
        def _():
            s_turns[0].wait_recv()
            acc[1] = acc[0] + got[0]
            s_turns[1].start()
            g_fill.wait()
            g_pair.wait_recv()
            for q in range(4):
                g_own[q] = (g_own[q].astype(F32) + g_core[q].astype(F32)).astype(BF16)
            for move in g_fars:
                move.start()

        @pl.when(n == 2)
        def _():
            s_turns[1].wait_recv()
            acc[2] = acc[1] + got[1]
            s_turns[2].start()
            for move in g_fars:
                move.wait_recv()
            g_own[p_y, pl.ds(0, 2)] = (
                g_own[p_y, pl.ds(0, 2)].astype(F32) + g_far[0].astype(F32)
            ).astype(BF16)
            g_own[p_x, pl.ds(2, 2)] = (
                g_own[p_x, pl.ds(2, 2)].astype(F32) + g_far[1].astype(F32)
            ).astype(BF16)
            for move in g_nears:
                move.start()

        @pl.when(n == 3)
        def _():
            s_turns[2].wait_recv()
            acc[3] = acc[2] + got[2]
            line[t] = acc[3]
            for move in g_nears:
                move.wait_recv()
            g_own[p] = (
                g_own[p].astype(F32) + g_from[0].astype(F32) + g_from[1].astype(F32)
            ).astype(BF16)
            g_line[t] = g_own[p, t]
            for k in (1, 2, 3):
                s_hop(k, False).start()
                g_hop(k, False).start()

        @pl.when(n == 6)
        def _():
            for k in (1, 2, 3):
                s_hop(k, True).wait_recv()
                g_hop(k, True).wait_recv()
            small_total[...] = line[0] + line[1] + line[2] + line[3]
            g_total[...] = (
                g_line[0].astype(F32) + g_line[1].astype(F32)
                + g_line[2].astype(F32) + g_line[3].astype(F32)
            )
            s_store.start()
            g_store.start()

    s_fill.start()
    g_fill.start()
    g_pair.start()
    for label in (2, 1, 0):
        pass_down(label).start()

    def fill_b(w, k):
        tt, j = k // groups, k % groups
        return pltpu.make_async_copy(
            b_refs[w].at[:, pl.ds(pl.multiple_of((j * 4 + tt) * chunk, 128), chunk)],
            b_all.at[w, tt, pl.ds(0, rows), pl.ds(pl.multiple_of(j * chunk, 128), chunk)],
            fill_sem.at[n_a + w, k],
        )

    def fill_a(v):
        return pltpu.make_async_copy(a_refs[v], a_all.at[v, pl.ds(0, rows)], fill_sem.at[v, 0])

    def pair_a(v):
        return pltpu.make_async_remote_copy(
            src_ref=a_refs[v], dst_ref=a_all.at[v, pl.ds(rows, rows)],
            send_sem=pair_send.at[v, 0], recv_sem=pair_recv.at[v, 0],
            device_id=core, device_id_type=MESH,
        )

    def pair_b(w, k):
        return pltpu.make_async_remote_copy(
            src_ref=b_all.at[w, k, pl.ds(0, rows)], dst_ref=b_all.at[w, k, pl.ds(rows, rows)],
            send_sem=pair_send.at[n_a + w, k], recv_sem=pair_recv.at[n_a + w, k],
            device_id=core, device_id_type=MESH,
        )

    for w in range(n_b):
        if w == 0 or lefts[w] != lefts[w - 1]:
            pair_a(lefts[w]).start()
            fill_a(lefts[w]).start()

        @pl.loop(0, 4 * groups)
        def _(k, w=w):
            fill_b(w, k).start()

    for w in range(n_b):

        @pl.loop(0, 4 * groups)
        def _(k, w=w):
            fill_b(w, k).wait()

        @pl.loop(0, 4)
        def _(k, w=w):
            pair_b(w, k).start()

    for v in range(n_a):
        fill_a(v).wait()
        pair_a(v).wait_recv()

    def dest(n):
        i = n % 4
        third, second, first = pick4(t, 3, 3, 0, 0), pick4(t, 2, 0, 1, 1), pick4(t, 1, 2, 3, 2)
        return pick4(i, third, second, first, t)

    def make(n, q):
        w = n // 4
        start = pl.multiple_of(2 * share * q + (share - 64) * c, 128)
        v = sum(jnp.where(w >= k, lefts[k] - (lefts[k - 1] if k else 0), 0) for k in range(n_b))
        lhs = a_all[v, :, pl.ds(start, share + 64)]
        rhs = b_all[w, dest(n)]
        product[...] = lax.dot_general(lhs, rhs, (((0,), (0,)), ((), ())), preferred_element_type=F32)
        return product[pl.ds(pl.multiple_of(64 * c, 64), share), :]

    def remote(n, src, dst, k, target):
        return pltpu.make_async_remote_copy(
            src_ref=src, dst_ref=dst, send_sem=send_sem.at[n, k], recv_sem=recv_sem.at[n, k],
            device_id=target, device_id_type=MESH,
        )

    def directs(n):
        return (
            remote(n, to_far.at[n, pl.ds(0, half)], far_x.at[n], 0, near_x),
            remote(n, to_far.at[n, pl.ds(half, half)], far_y.at[n], 1, near_y),
            remote(n, to_x.at[n, pl.ds(0, half)], from_x.at[n, pl.ds(0, half)], 2, near_x),
            remote(n, to_y.at[n, pl.ds(half, half)], from_y.at[n, pl.ds(half, half)], 3, near_y),
        )

    def seconds(n):
        return (
            remote(n, to_x.at[n, pl.ds(half, half)], from_x.at[n, pl.ds(half, half)], 4, near_x),
            remote(n, to_y.at[n, pl.ds(0, half)], from_y.at[n, pl.ds(0, half)], 5, near_y),
        )

    def begin(n):
        pair_b(n // 4, dest(n)).wait_recv()
        to_far[n] = make(n, p_far).astype(BF16)
        directs(n)[0].start()
        directs(n)[1].start()
        to_x[n] = make(n, p_x).astype(BF16)
        directs(n)[2].start()
        to_y[n] = make(n, p_y).astype(BF16)
        directs(n)[3].start()

    def forward(n):
        first, second = directs(n)[:2]
        first.wait_recv()
        to_y[n, pl.ds(0, half)] = (
            to_y[n, pl.ds(0, half)].astype(F32) + far_x[n].astype(F32)
        ).astype(BF16)
        seconds(n)[1].start()
        second.wait_recv()
        to_x[n, pl.ds(half, half)] = (
            to_x[n, pl.ds(half, half)].astype(F32) + far_y[n].astype(F32)
        ).astype(BF16)
        seconds(n)[0].start()

    def hop(w, out, into, target):
        return pltpu.make_async_remote_copy(
            src_ref=line_send.at[w, out], dst_ref=line_recv.at[w, into],
            send_sem=zs_sem.at[w, out], recv_sem=zr_sem.at[w, into],
            device_id=target, device_id_type=MESH,
        )

    end = (t == 0) | (t == 3)

    def finish(n):
        w, i = n // 4, n % 4
        mine = make(n, p)
        for move in directs(n)[2:] + seconds(n):
            move.wait_recv()
        total[w] = mine + from_x[n].astype(F32) + from_y[n].astype(F32)

        @pl.when((i < 3) & end)
        def _():
            line_send[w, i] = total[w].astype(BF16)

        @pl.when((i == 0) & (t == 0))
        def _():
            hop(w, 0, 0, right).start()

        @pl.when((i == 0) & (t == 3))
        def _():
            hop(w, 0, 0, left).start()

        @pl.when((i == 1) & (t == 0))
        def _():
            hop(w, 1, 1, right).start()

        @pl.when((i == 1) & (t == 3))
        def _():
            hop(w, 1, 2, left).start()

        @pl.when((i == 2) & (t == 0))
        def _():
            hop(w, 2, 3, right).start()

        @pl.when((i == 2) & (t == 3))
        def _():
            hop(w, 2, 4, left).start()

        @pl.when((i == 0) & (t == 1))
        def _():
            hop(w, 0, 0, right).wait_recv()
            line_send[w, 0] = (total[w] + line_recv[w, 0].astype(F32)).astype(BF16)
            hop(w, 0, 1, right).start()

        @pl.when((i == 0) & (t == 2))
        def _():
            hop(w, 0, 0, left).wait_recv()
            line_send[w, 0] = (total[w] + line_recv[w, 0].astype(F32)).astype(BF16)
            hop(w, 0, 2, left).start()

        @pl.when((i == 1) & ~end)
        def _():
            hop(w, 1, 2, left).wait_recv()
            line_send[w, 1] = (total[w] + line_recv[w, 2].astype(F32)).astype(BF16)
            hop(w, 1, 4, left).start()

        @pl.when((i == 2) & ~end)
        def _():
            hop(w, 1, 1, right).wait_recv()
            line_send[w, 2] = (total[w] + line_recv[w, 1].astype(F32)).astype(BF16)
            hop(w, 2, 3, right).start()

    @pl.loop(0, steps + 3)
    def _(n):
        @pl.when(n < steps)
        def _():
            begin(n)

        @pl.when((n >= 1) & (n <= steps))
        def _():
            forward(n - 1)

        small_steps(n)

        @pl.when(n >= 3)
        def _():
            finish(n - 3)

    def result(w):
        return pltpu.make_async_copy(total.at[w], out_ref.at[w], out_sem.at[w])

    for w in range(n_b):

        @pl.when(t > 0)
        def _(w=w):
            hop(w, 2, 3, right).wait_recv()
            total[w] = total[w] + line_recv[w, 3].astype(F32)

        @pl.when(t < 3)
        def _(w=w):
            hop(w, 2, 4, left).wait_recv()
            total[w] = total[w] + line_recv[w, 4].astype(F32)

        result(w).start()

    @pl.loop(0, steps)
    def _(n):
        for move in directs(n) + seconds(n):
            move.wait_send()

    for w in range(n_b):
        for k in range(3):
            hop(w, k, 0, right).wait_send()
        result(w).wait()

        @pl.loop(0, 4)
        def _(k, w=w):
            pair_b(w, k).wait_send()

    for v in range(n_a):
        pair_a(v).wait_send()

    for label in range(3):
        pass_down(label).wait_send()
    for tt in range(4):
        pl.when(t != tt)(lambda tt=tt: down_here(tt).wait_recv())
    for move in (g_pair,) + g_fars + g_nears + s_turns:
        move.wait_send()
    for k in (1, 2, 3):
        s_hop(k, False).wait_send()
        g_hop(k, False).wait_send()
    s_store.wait()
    g_store.wait()


def weight_grads(lefts, a_list, b_list, groups, downs, blocks, small):
    n_ten, n_seq = lax.axis_size("tensor"), lax.axis_size("seq")
    rows, width = a_list[0].shape
    channels = b_list[0].shape[1]
    chunk = channels // groups // n_ten
    share = width // n_seq
    if not (n_ten == 4 and n_seq == 8):
        out = []
        for v, b in zip(lefts, b_list):
            b = jnp.swapaxes(b.reshape(rows, groups, n_ten, chunk), 1, 2).reshape(rows, channels)
            grad = dot_tn(a_list[v], b).astype(BF16)
            grad = lax.psum_scatter(grad, "seq", scatter_dimension=0, tiled=True)
            out.append(lax.psum_scatter(grad, "tensor", scatter_dimension=1, tiled=True).astype(F32))
        sums = lax.psum_scatter(blocks, BOTH, scatter_dimension=0, tiled=True)[0].astype(F32)
        return out, line_sum(downs[0], downs[1:]), sums, lax.psum(small, BOTH)
    count, cols = len(b_list), groups * chunk
    half, steps = share // 2, 4 * count
    anywhere = pl.BlockSpec(memory_space=pl.ANY)
    dma = pltpu.SemaphoreType.DMA

    def room(*dims):
        return pltpu.VMEM(dims, BF16)

    both = len(a_list) + count
    blocks = blocks.reshape((4, 2, 4) + blocks.shape[1:])
    piece = blocks.shape[3:]
    grads, land, block_sum, small_sum = pl.pallas_call(
        functools.partial(tail_kernel, lefts, rows, groups, chunk, share),
        out_shape=[
            jax.ShapeDtypeStruct((count, share, cols), F32),
            jax.ShapeDtypeStruct((4, rows, width), BF16),
            jax.ShapeDtypeStruct(piece, F32),
            jax.ShapeDtypeStruct(small.shape, F32),
        ],
        in_specs=[anywhere] * (both + 3),
        out_specs=[anywhere] * 4,
        scratch_shapes=[
            room(len(a_list), 2 * rows, width), room(count, 4, 2 * rows, cols),
            pltpu.VMEM((share + 64, cols), F32),
            room(steps, share, cols), room(steps, share, cols), room(steps, share, cols),
            room(steps, half, cols), room(steps, half, cols),
            room(steps, share, cols), room(steps, share, cols),
            pltpu.VMEM((count, share, cols), F32),
            room(count, 3, share, cols), room(count, 5, share, cols),
            dma((both, 4 * groups)), dma((count,)), dma((both, 4)), dma((both, 4)),
            dma((steps, 6)), dma((steps, 6)), dma((count, 3)), dma((count, 5)),
            dma((3,)), dma((4,)),
            room(4, 4, *piece), room(4, 4, *piece), room(2, 2, *piece), room(2, 4, *piece),
            room(4, *piece), pltpu.VMEM(piece, F32), dma((2,)), dma((8,)), dma((8,)),
            pltpu.VMEM((4,) + small.shape, F32), pltpu.VMEM((3,) + small.shape, F32),
            pltpu.VMEM((4,) + small.shape, F32), pltpu.VMEM(small.shape, F32),
            dma((2,)), dma((6,)), dma((6,)),
        ],
        compiler_params=pltpu.CompilerParams(
            collective_id=4, has_side_effects=True, vmem_limit_bytes=67043328
        ),
        cost_estimate=pl.CostEstimate(
            flops=2 * count * rows * width * channels, bytes_accessed=1 << 29, transcendentals=0
        ),
        name="tail",
    )(*a_list, *b_list, downs, blocks, small)
    place = lax.axis_index("tensor")
    down = downs[0].astype(F32)
    for k in range(4):
        down = down + jnp.where(place == k, 0.0, land[k].astype(F32))
    return grads, down, block_sum, small_sum


def feed_kernel(tiles, parts, own_ref, cots_ref, wg_ref, wu_ref, wd_ref, *refs):
    tokens_ref, hid_ref, gg_ref, ug_ref, sum_ref, down_ref = refs[:6]
    (
        wg, wu, wd, tok, cot, hid, gg, ug, part, land, total, down,
        load_sem, store_sem, sum_sem, ag_send, ag_recv, rs_send, rs_recv,
    ) = refs[6:]
    s, t = lax.axis_index("seq"), lax.axis_index("tensor")
    right, left = (s, t + 1), (s, t - 1)
    width, units = wg.shape
    span, cut = width // tiles, units // parts
    greet([(s, (t + 1) % 4), (s, (t + 3) % 4)])

    def pass_on(src, tt, kind):
        return pltpu.make_async_remote_copy(
            src_ref=src, dst_ref=tokens_ref.at[tt], send_sem=ag_send.at[tt, kind],
            recv_sem=ag_recv.at[tt], device_id=left if kind else right, device_id_type=MESH,
        )

    pl.when(t < 3)(lambda: pass_on(own_ref, t, 0).start())
    pl.when(t > 0)(lambda: pass_on(own_ref, t, 1).start())
    weights = [
        pltpu.make_async_copy(src, dst, load_sem.at[2 + k])
        for k, (src, dst) in enumerate(((wg_ref, wg), (wu_ref, wu), (wd_ref, wd)))
    ]
    for move in weights:
        move.start()

    def whose(i):
        third, second, first = pick4(t, 3, 3, 0, 0), pick4(t, 2, 0, 1, 1), pick4(t, 1, 2, 3, 2)
        return pick4(i, t, first, second, third)

    def stores(i):
        ch = whose(i)
        return [
            pltpu.make_async_copy(src, dst.at[ch], store_sem.at[k])
            for k, (src, dst) in enumerate(((hid, hid_ref), (gg, gg_ref), (ug, ug_ref)))
        ]

    def hop(label, k, way):
        return pltpu.make_async_remote_copy(
            src_ref=part.at[label, k], dst_ref=land.at[way, label, k],
            send_sem=rs_send.at[label, k], recv_sem=rs_recv.at[way, label, k],
            device_id=left if way else right, device_id_type=MESH,
        )

    def landed(label, k, way):
        hop(label, k, way).wait_recv()
        return land[way, label, k].astype(F32)

    def put_down(i):
        return pltpu.make_async_copy(down, down_ref.at[i], store_sem.at[4])

    def column(k, size):
        return pl.ds(pl.multiple_of(k * size, 128), size)

    def give(i, k, value):
        label = i - 1

        @pl.when(i == 0)
        def _():
            total[k] = value

        @pl.when((i > 0) & ((i < 3) | (t == 0) | (t == 3)))
        def _():
            part[label, k] = value.astype(BF16)

        @pl.when((i > 0) & (t == 0))
        def _():
            hop(label, k, 0).start()

        @pl.when((i > 0) & (t == 3))
        def _():
            hop(label, k, 1).start()

        @pl.when((i == 3) & (t == 1))
        def _():
            part[2, k] = (value + landed(2, k, 0)).astype(BF16)
            hop(2, k, 0).start()

        @pl.when((i == 3) & (t == 2))
        def _():
            part[2, k] = (value + landed(2, k, 1)).astype(BF16)
            hop(2, k, 1).start()

    @pl.loop(0, 4)
    def _(i):
        ch = whose(i)
        for way in (-1, 1):
            tt = t + way * i
            ok = (i > 0) & (tt >= 0) & (tt <= 3)

            @pl.when(ok)
            def _(tt=tt, way=way):
                pass_on(tokens_ref.at[tt], tt, 0).wait_recv()
                if way < 0:
                    pl.when(t < 3)(lambda: pass_on(tokens_ref.at[tt], tt, 0).start())
                else:
                    pl.when(t > 0)(lambda: pass_on(tokens_ref.at[tt], tt, 1).start())

        get_cot = pltpu.make_async_copy(cots_ref.at[ch], cot, load_sem.at[1])
        get_cot.start()

        @pl.when(i == 0)
        def _():
            move = pltpu.make_async_copy(own_ref, tok, load_sem.at[0])
            move.start()
            move.wait()
            pltpu.make_async_copy(tok, tokens_ref.at[t], store_sem.at[3]).start()
            for move in weights:
                move.wait()

        @pl.when(i == 1)
        def _():
            pltpu.make_async_copy(tok, tokens_ref.at[t], store_sem.at[3]).wait()

        @pl.when(i > 0)
        def _():
            move = pltpu.make_async_copy(tokens_ref.at[ch], tok, load_sem.at[0])
            move.start()
            move.wait()
            for store in stores(i - 1):
                store.wait()
            put_down(i - 1).wait()

        get_cot.wait()

        @pl.loop(0, parts)
        def _(f):
            here = column(f, cut)
            gate_vals = jnp.dot(tok[...], wg[:, here], preferred_element_type=F32)
            up_vals = jnp.dot(tok[...], wu[:, here], preferred_element_type=F32)
            back = lax.dot_general(
                cot[...], wd[here, :], (((1,), (1,)), ((), ())), preferred_element_type=F32
            )
            value, slope = gelu_both(gate_vals)
            hid[:, here] = (value * up_vals).astype(BF16)
            gg[:, here] = (back * up_vals * slope).astype(BF16)
            ug[:, here] = (back * value).astype(BF16)

        for store in stores(i):
            store.start()

        @pl.loop(0, tiles)
        def _(k):
            here = column(k, span)
            value = lax.dot_general(
                gg[...], wg[here, :], (((1,), (1,)), ((), ())), preferred_element_type=F32
            ) + lax.dot_general(
                ug[...], wu[here, :], (((1,), (1,)), ((), ())), preferred_element_type=F32
            )
            give(i, k, value)

        @pl.loop(0, tiles)
        def _(k):
            here = column(k, span)
            down[:, here] = jnp.dot(hid[...], wd[:, here], preferred_element_type=F32).astype(BF16)

        put_down(i).start()

    def add_and_send(k, label, arrived, way):
        part[label, k] = (part[label, k].astype(F32) + landed(arrived, k, way)).astype(BF16)
        hop(label, k, way).start()

    def add_total(k, label, way):
        total[k] = total[k] + landed(label, k, way)

    def put_sum(k):
        return pltpu.make_async_copy(total.at[k], sum_ref.at[:, column(k, span)], sum_sem.at[k])

    @pl.loop(0, tiles)
    def _(k):
        pl.when(t == 1)(lambda: add_and_send(k, 0, 1, 0))
        pl.when(t == 2)(lambda: add_and_send(k, 1, 1, 1))
        pl.when(t == 1)(lambda: add_and_send(k, 1, 2, 1))
        pl.when(t == 2)(lambda: add_and_send(k, 0, 2, 0))

    @pl.loop(0, tiles)
    def _(k):
        pl.when(t == 0)(lambda: add_total(k, 1, 1))
        pl.when(t > 0)(lambda: add_total(k, 0, 0))
        pl.when(t == 1)(lambda: add_total(k, 1, 1))
        pl.when(t == 2)(lambda: add_total(k, 0, 1))
        put_sum(k).start()

    @pl.loop(0, tiles)
    def _(k):
        put_sum(k).wait()
        for label in range(3):
            hop(label, k, 0).wait_send()

    put_down(3).wait()
    for store in stores(3):
        store.wait()
    pl.when(t < 3)(lambda: pass_on(own_ref, t, 0).wait_send())
    pl.when(t > 0)(lambda: pass_on(own_ref, t, 1).wait_send())
    for i in (1, 2, 3):
        pl.when((t - i >= 0) & (t < 3))(
            lambda i=i: pass_on(tokens_ref.at[t - i], t - i, 0).wait_send()
        )
        pl.when((t + i <= 3) & (t > 0))(
            lambda i=i: pass_on(tokens_ref.at[t + i], t + i, 1).wait_send()
        )


def feed_forward(own, cots, w_gate, w_up, w_down):
    rows, width = own.shape
    units = w_gate.shape[1]
    tiles, parts = 4, 5
    anywhere = pl.BlockSpec(memory_space=pl.ANY)
    dma = pltpu.SemaphoreType.DMA

    def room(*dims):
        return pltpu.VMEM(dims, BF16)

    def out(*dims, kind=BF16):
        return jax.ShapeDtypeStruct(dims, kind)

    flops = 2 * 4 * rows * width * units * 6
    got = pl.pallas_call(
        functools.partial(feed_kernel, tiles, parts),
        out_shape=[
            out(4, rows, width), out(4, rows, units), out(4, rows, units), out(4, rows, units),
            out(rows, width, kind=F32), out(4, rows, width),
        ],
        in_specs=[anywhere] * 5,
        out_specs=[anywhere] * 6,
        scratch_shapes=[
            room(width, units), room(width, units), room(units, width),
            room(rows, width), room(rows, width),
            room(rows, units), room(rows, units), room(rows, units),
            room(3, tiles, rows, width // tiles), room(2, 3, tiles, rows, width // tiles),
            pltpu.VMEM((tiles, rows, width // tiles), F32), room(rows, width),
            dma((5,)), dma((5,)), dma((tiles,)), dma((4, 2)), dma((4,)),
            dma((3, tiles)), dma((2, 3, tiles)),
        ],
        compiler_params=pltpu.CompilerParams(
            collective_id=5, has_side_effects=True, vmem_limit_bytes=67043328
        ),
        cost_estimate=pl.CostEstimate(flops=flops, bytes_accessed=3 << 27, transcendentals=0),
        name="feed",
    )(own, cots, w_gate, w_up, w_down)
    return got


def chunk_scan(a_ref, d_ref, p_ref, s_ref, reverse):
    tiles, rows, wide = a_ref.shape
    run = rows // 8

    def first(i, carry):
        r = run - 1 - i if reverse else i
        here = pl.ds(r, 8, stride=run)
        after = []
        for b in range(tiles):
            prod, state = carry[b]
            a = a_ref[b, here, :]
            prod = prod * a
            state = a * state + d_ref[b, here, :]
            a_ref[b, here, :] = prod
            d_ref[b, here, :] = state
            after.append((prod, state))
        return tuple(after)

    start = (jnp.ones((8, wide), F32), jnp.zeros((8, wide), F32))
    ends = lax.fori_loop(0, run, first, (start,) * tiles, unroll=4)
    leads, totals = [], []
    for b in range(tiles):
        prod, state = ends[b]
        enter_p, enter_s = [None] * 8, [None] * 8
        now_p, now_s = jnp.ones((1, wide), F32), jnp.zeros((1, wide), F32)
        for c in range(7, -1, -1) if reverse else range(8):
            enter_p[c], enter_s[c] = now_p, now_s
            now_p, now_s = now_p * prod[c : c + 1], prod[c : c + 1] * now_s + state[c : c + 1]
        leads.append((jnp.concatenate(enter_p, 0), jnp.concatenate(enter_s, 0)))
        totals.append((now_p, now_s))

    def second(r, _):
        here = pl.ds(r, 8, stride=run)
        for b in range(tiles):
            p = a_ref[b, here, :]
            a_ref[b, here, :] = p * leads[b][0]
            d_ref[b, here, :] = d_ref[b, here, :] + p * leads[b][1]
        return 0

    lax.fori_loop(0, run, second, 0, unroll=4)
    for b in range(tiles):
        p_ref[:, b * wide : (b + 1) * wide] = a_ref[b]
        s_ref[:, b * wide : (b + 1) * wide] = d_ref[b]
    return jnp.concatenate([p for p, _ in totals], 1), jnp.concatenate([v for _, v in totals], 1)


def tiled_store(ref, value):
    tiles, _, wide = ref.shape
    for b in range(tiles):
        ref[b] = value[:, b * wide : (b + 1) * wide]


def positions(base_ref, rows, lanes, length):
    place = lax.broadcasted_iota(jnp.int32, (rows, lanes), 0) + base_ref[0]
    return jnp.where(place >= length, place - length, place)


def forward_kernel(
    length, local, base_ref, x_ref, cw_ref, rate_gain_ref, g_ref, sel_ref,
    conv_ref, rate_ref, in_ref, p_ref, s_ref, carry_ref, w_ref, a_ref, d_ref,
):
    rows, lanes = conv_ref.shape
    spot = positions(base_ref, rows, lanes, length)
    x = x_ref[...].astype(F32)
    total = cw_ref[0:1, :] * x[HALO:]
    for k in range(1, CONV):
        moved = pltpu.roll(x, k, 0)[HALO:]
        total = total + jnp.where(spot >= k, cw_ref[k : k + 1, :] * moved, 0.0)
    conv = total.astype(BF16)
    conv_ref[...] = conv
    join = sel_ref.shape[0]
    wide = jnp.dot(g_ref[0], sel_ref[0], preferred_element_type=F32)
    for q in range(1, join):
        other = jnp.dot(g_ref[0], sel_ref[q], preferred_element_type=F32)
        which = lax.broadcasted_iota(jnp.int32, wide.shape, 0) // local % join
        wide = jnp.where(which == q, other, wide)
    gates = wide.astype(BF16)
    w_ref[0] = gates
    pre = lax.dot_general(conv, gates, (((1,), (1,)), ((), ())), preferred_element_type=F32)
    rate, inp = pre[:, :lanes], pre[:, lanes:]
    rate_ref[...] = rate
    in_ref[...] = inp
    decay = jnp.where(spot == 0, 0.0, jnp.exp(rate_gain_ref[...] * jax.nn.sigmoid(rate)))
    tiled_store(a_ref, decay)
    tiled_store(
        d_ref,
        jnp.sqrt(jnp.maximum(1.0 - decay * decay, 0.01)) * jax.nn.sigmoid(inp) * conv.astype(F32),
    )
    prod, state = chunk_scan(a_ref, d_ref, p_ref, s_ref, False)
    carry_ref[0:1, :] = prod
    carry_ref[1:2, :] = state


def middle_kernel(
    length, base_ref, mg_ref, y_ref, p_ref, s_ref, enter_ref, rate_ref, rate_gain_ref,
    ylow_ref, bp_ref, bs_ref, carry_ref, a_ref, d_ref,
):
    rows, lanes = mg_ref.shape
    spot = positions(base_ref, rows, lanes, length)
    states = s_ref[...] + p_ref[...] * enter_ref[...]
    value, slope = gelu_both(y_ref[...])
    grad = mg_ref[...]
    ylow_ref[...] = (grad * states * slope).astype(BF16)
    tiled_store(d_ref, grad * value)
    decay = jnp.where(spot == 0, 0.0, jnp.exp(rate_gain_ref[...] * jax.nn.sigmoid(rate_ref[...])))
    row = lax.broadcasted_iota(jnp.int32, (rows, lanes), 0)
    tiled_store(a_ref, jnp.where(row == rows - 1, 1.0, pltpu.roll(decay, rows - 1, 0)))
    prod, state = chunk_scan(a_ref, d_ref, bp_ref, bs_ref, True)
    carry_ref[0:1, :] = decay[0:1] * prod
    carry_ref[1:2, :] = decay[0:1] * state


def backward_kernel(
    length, local, base_ref, bp_ref, bs_ref, leave_ref, p_ref, s_ref, enter_ref, rate_ref, in_ref,
    conv_ref, rate_gain_ref, w_ref, cw_ref, x_ref, sel_ref,
    gates_ref, xback_ref, edge_ref, small_ref,
):
    rows, lanes = bp_ref.shape
    spot = positions(base_ref, rows, lanes, length)
    row = lax.broadcasted_iota(jnp.int32, (rows, lanes), 0)
    adjoint = bs_ref[...] + bp_ref[...] * leave_ref[...]
    states = s_ref[...] + p_ref[...] * enter_ref[...]
    before = jnp.where(row == 0, enter_ref[...], pltpu.roll(states, 1, 0))
    gain = rate_gain_ref[...]
    sig_r = jax.nn.sigmoid(rate_ref[...])
    sig_i = jax.nn.sigmoid(in_ref[...])
    conv = conv_ref[...]
    conv_f = conv.astype(F32)
    decay = jnp.where(spot == 0, 0.0, jnp.exp(gain * sig_r))
    room = 1.0 - decay * decay
    scale = jnp.sqrt(jnp.maximum(room, 0.01))
    pulled = adjoint * sig_i
    slope = jnp.where(room > 0.01, -decay / scale, 0.0)
    decay_grad = adjoint * before + pulled * conv_f * slope
    log_grad = decay_grad * decay
    pull_r = log_grad * sig_r
    rate_back = (pull_r * gain * (1.0 - sig_r)).astype(BF16)
    conv_direct = pulled * scale
    in_back = (conv_direct * conv_f * (1.0 - sig_i)).astype(BF16)
    both = jnp.concatenate([rate_back, in_back], 1)
    join = sel_ref.shape[0]
    for q in range(join):
        some = lax.dot_general(
            conv, sel_ref[q], (((1,), (1,)), ((), ())), preferred_element_type=F32
        ).astype(BF16)
        part = lax.dot_general(some, both, (((0,), (0,)), ((), ())), preferred_element_type=F32)
        if q == 0:
            gate_sum = part
        else:
            which = lax.broadcasted_iota(jnp.int32, part.shape, 1) // local % join
            gate_sum = jnp.where(which == q, part, gate_sum)
    gates_ref[0] = gate_sum.astype(BF16)
    grad = conv_direct + lax.dot_general(
        both, w_ref[0], (((1,), (0,)), ((), ())), preferred_element_type=F32
    )
    x = x_ref[...].astype(F32)
    zeros = jnp.zeros((HALO, lanes), F32)
    out = jnp.concatenate([zeros, grad * cw_ref[0:1, :]], 0)
    small_ref[0:1, :] = jnp.sum(grad * x[HALO:], axis=0, keepdims=True)
    for k in range(1, CONV):
        masked = jnp.where(spot >= k, grad, 0.0)
        small_ref[k : k + 1, :] = jnp.sum(
            masked * pltpu.roll(x, k, 0)[HALO:], axis=0, keepdims=True
        )
        tall = jnp.concatenate([zeros, masked * cw_ref[k : k + 1, :]], 0)
        out = out + pltpu.roll(tall, rows + HALO - k, 0)
    small_ref[CONV : CONV + 1, :] = jnp.sum(pull_r, axis=0, keepdims=True)
    small_ref[CONV + 1 : 8, :] = jnp.zeros((7 - CONV, lanes), F32)
    edge_ref[...] = out[:HALO]
    xback_ref[...] = out[HALO:]


def lane_call(kernel, grid, lanes, base, operands, outputs, scratch, flops):
    def spec(shape):
        if len(shape) == 3 and shape[0] != grid:
            return pl.BlockSpec(shape, lambda j, *_: (0, 0, 0))
        if len(shape) == 3:
            return pl.BlockSpec((1,) + shape[1:], lambda j, *_: (j, 0, 0))
        return pl.BlockSpec((shape[0], lanes), lambda j, *_: (0, j))

    moved = sum(math.prod(a.shape) * a.dtype.itemsize for a in list(operands) + list(outputs))
    return pl.pallas_call(
        kernel,
        grid_spec=pltpu.PrefetchScalarGridSpec(
            num_scalar_prefetch=1,
            grid=(grid,),
            in_specs=[spec(a.shape) for a in operands],
            out_specs=[spec(a.shape) for a in outputs],
            scratch_shapes=scratch,
        ),
        out_shape=outputs,
        compiler_params=pltpu.CompilerParams(
            dimension_semantics=("arbitrary",), vmem_limit_bytes=56 << 20
        ),
        cost_estimate=pl.CostEstimate(flops=flops, bytes_accessed=moved, transcendentals=0),
    )(base, *operands)


def shards(
    tokens_in, gain_pre, w_x, w_y, conv_w, gate_a, gate_i, decay_param, w_out,
    gain_mlp, w_gate, w_up, w_down, cotangent,
):
    rows, width = tokens_in.shape
    heads, local = w_x.shape[1:]
    n_ten, n_seq = lax.axis_size("tensor"), lax.axis_size("seq")
    devices = n_ten * n_seq
    place, run = lax.axis_index("tensor"), lax.axis_index("seq")
    linear = run * n_ten + place
    length = devices * rows // SEQS
    base = jnp.reshape((linear * rows) % length, (1,)).astype(jnp.int32)
    join = 128 // local if local < 128 and heads % (128 // local) == 0 else 1
    groups, chunk = heads // join, join * local
    lanes = n_ten * chunk
    channels = groups * lanes

    def shape(dims, kind=F32):
        return jax.ShapeDtypeStruct(dims, kind)

    def own_columns(array):
        n = array.shape[0]
        split = array.reshape(n, groups, n_ten, chunk)
        return lax.dynamic_index_in_dim(split, place, 2, False).reshape(n, heads, local)

    gate_rows = jnp.stack([gate_a, gate_i], 0).swapaxes(2, 3).reshape(2 * heads, local, n_ten * local)
    params = jnp.concatenate([conv_w, decay_param[None]], 0).reshape(CONV + 1, heads * local)
    params = jnp.pad(params, ((0, 7 - CONV), (0, 0)))
    (all_gates, full_x, full_y, full_out), params, cots, halo = gather_all(
        [
            gate_rows,
            jnp.transpose(w_x, (1, 2, 0)).reshape(groups, chunk, width),
            jnp.transpose(w_y, (1, 2, 0)).reshape(groups, chunk, width),
            w_out.reshape(groups, chunk, width),
        ],
        params, cotangent, tokens_in, HALO,
    )
    halo = jnp.where(linear == 0, jnp.zeros_like(halo), halo)
    full_x, full_y, full_out = (w.reshape(channels, width) for w in (full_x, full_y, full_out))
    gates = all_gates.reshape(2, groups, join, n_ten, local, n_ten * local)
    gates = jnp.transpose(gates, (1, 0, 3, 2, 4, 5)).reshape(groups, 2 * lanes, n_ten * local)
    key = jnp.arange(n_ten * local)[None, :, None]
    lane = jnp.arange(lanes)[None, None, :]
    member = jnp.arange(join)[:, None, None]
    select = (
        (lane // chunk == key // local) & (lane % local == key % local) & (lane // local % join == member)
    ).astype(BF16)
    params = jnp.transpose(params.reshape(n_ten, 8, groups, chunk), (1, 2, 0, 3)).reshape(8, channels)
    conv_rows, decay_full = params, params[CONV : CONV + 1]
    rate_gain = -8.0 * jax.nn.softplus(decay_full)

    own_in = tokens_in.astype(F32)
    in_scale, in_unit = rms_parts(own_in)
    normed = (in_unit * gain_pre).astype(BF16)
    normed_halo = (rms_parts(halo.astype(F32))[1] * gain_pre).astype(BF16)
    x_long = dot_nt(jnp.concatenate([normed_halo, normed], 0), full_x).astype(BF16)
    y_branch = dot_nt(normed, full_y)
    scratch = [pltpu.VMEM((lanes // 128, rows, 128), F32)] * 2
    conv_out, rate_pre, input_pre, products, partial, carry, wide_gates = lane_call(
        functools.partial(forward_kernel, length, local), groups, lanes, base,
        (x_long, conv_rows, rate_gain, gates, select),
        [
            shape((rows, channels), BF16),
            shape((rows, channels)),
            shape((rows, channels)),
            shape((rows, channels)),
            shape((rows, channels)),
            shape((2, channels)),
            shape((groups, 2 * lanes, lanes), BF16),
        ],
        scratch, 4 * rows * lanes * channels,
    )
    reach = min(-(-length // rows), devices - 1)
    enter = entering(carry, reach, linear, devices, False)
    states = partial + products * enter
    mixed = (states * jax.nn.gelu(y_branch, approximate=True)).astype(BF16)
    middle = own_in + dot_nn(mixed, full_out)
    mid_scale, mid_unit = rms_parts(middle)
    normed_mlp = (mid_unit * gain_mlp).astype(BF16)

    if n_ten == 4 and n_seq == 8:
        *kept, mlp_input, downs = feed_forward(normed_mlp, cots, w_gate, w_up, w_down)
        cot_rows = cots.reshape(n_ten * rows, width)
        token_rows, hidden_rows, gate_rows, up_rows = (
            a.reshape(n_ten * rows, a.shape[2]) for a in kept
        )
    else:
        cots = [cotangent] + [
            lax.dynamic_index_in_dim(cots, label_index(k), 0, False) for k in range(1, n_ten)
        ]
        tokens = [normed_mlp] + others(normed_mlp)
        hiddens, gate_grads, up_grads, downs, pulls = [], [], [], [], []
        for n, c in zip(tokens, cots):
            gate_vals, up_vals = dot_nn(n, w_gate), dot_nn(n, w_up)
            value, slope = gelu_both(gate_vals)
            hidden = (value * up_vals).astype(BF16)
            hidden_grad = dot_nt(c, w_down)
            gate_grad = (hidden_grad * up_vals * slope).astype(BF16)
            up_grad = (hidden_grad * value).astype(BF16)
            hiddens.append(hidden)
            gate_grads.append(gate_grad)
            up_grads.append(up_grad)
            pulls.append(dot_nt(gate_grad, w_gate) + dot_nt(up_grad, w_up))
            downs.append(dot_nn(hidden, w_down).astype(BF16))
        mlp_input = line_sum(pulls[0], [p.astype(BF16) for p in pulls[1:]])
        cot_rows, token_rows, hidden_rows, gate_rows, up_rows = (
            jnp.concatenate(a, 0) for a in (cots, tokens, hiddens, gate_grads, up_grads)
        )
    grad_down = dot_tn(cot_rows, hidden_rows).astype(BF16)
    grad_gate = dot_tn(token_rows, gate_rows).astype(BF16)
    grad_up = dot_tn(token_rows, up_rows).astype(BF16)
    gain_mlp_part, mid_back = rms_back(mlp_input, gain_mlp, mid_scale, mid_unit)
    middle_grad = cotangent.astype(F32) + mid_back
    middle_low, grad_down, grad_gate, grad_up = lax.optimization_barrier(
        (middle_grad.astype(BF16), grad_down, grad_gate, grad_up)
    )
    grad_down, grad_gate, grad_up = (
        lax.psum_scatter(g, "seq", scatter_dimension=0, tiled=True)
        for g in (grad_down, grad_gate, grad_up)
    )
    mixed_grad = dot_nt(middle_low, full_out)
    y_low, back_products, back_partial, carry = lane_call(
        functools.partial(middle_kernel, length), groups, lanes, base,
        (mixed_grad, y_branch, products, partial, enter, rate_pre, rate_gain),
        [
            shape((rows, channels), BF16),
            shape((rows, channels)),
            shape((rows, channels)),
            shape((2, channels)),
        ],
        scratch, 60 * rows * channels,
    )
    leave = entering(carry, reach, linear, devices, True)
    gate_parts, x_back, edge, sums = lane_call(
        functools.partial(backward_kernel, length, local), groups, lanes, base,
        (
            back_products, back_partial, leave, products, partial, enter, rate_pre, input_pre,
            conv_out, rate_gain, wide_gates, conv_rows, x_long, select,
        ),
        [
            shape((groups, n_ten * local, 2 * lanes), BF16),
            shape((rows, channels)),
            shape((HALO, channels)),
            shape((8, channels)),
        ],
        [], 8 * rows * lanes * channels,
    )
    edge = lax.ppermute(edge, BOTH, [(i + 1, i) for i in range(devices - 1)])
    x_low = jnp.concatenate(
        [x_back[: rows - HALO], x_back[rows - HALO :] + edge], 0
    ).astype(BF16)

    normed_grad = dot_nn(x_low, full_x) + dot_nn(y_low, full_y)
    gain_pre_part, in_back = rms_back(normed_grad, gain_pre, in_scale, in_unit)
    input_grad = middle_grad + in_back

    part = n_ten * local // n_seq
    split = gate_parts.reshape(groups, n_seq, part, 2, n_ten, chunk)
    split = jnp.transpose(split, (1, 4, 0, 3, 2, 5)).reshape(devices, groups * 2 * part, chunk)
    packed = jnp.concatenate(
        [sums[: CONV + 1], gain_pre_part[None], gain_mlp_part[None], sums[CONV + 3 :]], 0
    )
    (grad_out, grad_y, grad_x), down, gate_sum, packed = weight_grads(
        (0, 1, 1), [middle_low, normed], [mixed, y_low, x_low], groups, downs, split, packed
    )
    block_out = (middle + down).astype(BF16)
    gate_sum = gate_sum.reshape(groups, 2, part, join, local)
    gate_sum = jnp.transpose(gate_sum, (1, 0, 3, 2, 4)).reshape(2, heads, part, local)
    conv_sum = own_columns(packed[:CONV])
    decay_sum = own_columns(packed[CONV : CONV + 1] * (-8.0 * jax.nn.sigmoid(decay_full)))[0]
    share = local // n_seq
    grad_conv = lax.dynamic_slice_in_dim(conv_sum, run * share, share, 2)
    grad_decay = lax.dynamic_slice_in_dim(decay_sum, run * share, share, 1)
    grad_gain_mlp = lax.dynamic_slice_in_dim(
        packed[CONV + 2], run * (width // n_seq), width // n_seq, 0
    )

    def weight(grad):
        return grad.T.reshape(heads, local, -1)

    return (
        block_out,
        input_grad,
        packed[CONV + 1],
        jnp.transpose(weight(grad_x), (2, 0, 1)),
        jnp.transpose(weight(grad_y), (2, 0, 1)),
        grad_conv,
        gate_sum[0],
        gate_sum[1],
        grad_decay,
        weight(grad_out),
        grad_gain_mlp,
        grad_gate.astype(F32),
        grad_up.astype(F32),
        grad_down.astype(F32).T,
    )


def solution(mesh):
    placed = (
        P(("seq", "tensor"), None),
        P(),
        P(None, None, "tensor"),
        P(None, None, "tensor"),
        P(None, None, "tensor"),
        P(None, None, "tensor"),
        P(None, None, "tensor"),
        P(None, "tensor"),
        P(None, "tensor", None),
        P(),
        P(None, "tensor"),
        P(None, "tensor"),
        P("tensor", None),
        P(("seq", "tensor"), None),
    )
    return jax.shard_map(
        shards,
        mesh=mesh,
        in_specs=placed,
        out_specs=(
            P(("seq", "tensor"), None),
            P(("seq", "tensor"), None),
            P(),
            P("seq", None, "tensor"),
            P("seq", None, "tensor"),
            P(None, None, ("tensor", "seq")),
            P(None, "seq", "tensor"),
            P(None, "seq", "tensor"),
            P(None, ("tensor", "seq")),
            P(None, "tensor", "seq"),
            P("seq"),
            P("seq", "tensor"),
            P("seq", "tensor"),
            P("tensor", "seq"),
        ),
        check_vma=False,
    )
```

```python
import functools
import math

import jax
import jax.numpy as jnp
from jax import lax
from jax.experimental import pallas as pl
from jax.experimental.pallas import tpu as pltpu
from jax.sharding import PartitionSpec as P

CONV = 4
SEQS = 3
HALO = 16
epsilon = 1e-06
F32 = jnp.float32
BF16 = jnp.bfloat16
ROOT = math.sqrt(2.0 / math.pi)
BOTH = ("seq", "tensor")


def dot_nn(a, b):
    return lax.dot_general(a, b, (((1,), (0,)), ((), ())), preferred_element_type=F32)


def dot_nt(a, b):
    return lax.dot_general(a, b, (((1,), (1,)), ((), ())), preferred_element_type=F32)


def dot_tn(a, b):
    return lax.dot_general(a, b, (((0,), (0,)), ((), ())), preferred_element_type=F32)


def rms_parts(values):
    scale = lax.rsqrt(jnp.mean(values * values, axis=-1, keepdims=True) + epsilon)
    return scale, values * scale


def rms_back(grad, gain, scale, unit):
    pulled = gain * grad
    inner = jnp.mean(pulled * unit, axis=-1, keepdims=True)
    return jnp.sum(grad * unit, axis=0), scale * (pulled - unit * inner)


def gelu_both(v):
    inner = v * v
    th = jnp.tanh(ROOT * (v + 0.044715 * v * inner))
    half = 0.5 * (1.0 + th)
    slope = half + 0.5 * v * (1.0 - th * th) * (ROOT * (1.0 + 3 * 0.044715 * inner))
    return v * half, slope


LABELS = ((1, 2, 3, 2), (2, 0, 1, 1), (3, 3, 0, 0))


def along(block, pairs):
    return lax.ppermute(block, "tensor", pairs)


def line_streams(own):
    right, left = [], []
    right.append(along(own, [(0, 1), (1, 2), (2, 3)]))
    left.append(along(own, [(1, 0), (2, 1), (3, 2)]))
    right.append(along(right[0], [(1, 2), (2, 3)]))
    left.append(along(left[0], [(1, 0), (2, 1)]))
    right.append(along(right[1], [(2, 3)]))
    left.append(along(left[1], [(1, 0)]))
    return right, left


def others(own):
    count = lax.axis_size("tensor")
    place = lax.axis_index("tensor")
    if count == 4:
        right, left = line_streams(own)
        first = jnp.where(place == 3, right[0], left[0])
        second = jnp.where(place == 0, left[1], jnp.where(place == 3, right[1], right[0]))
        third = jnp.where(
            place == 0, left[2], jnp.where(place == 1, left[1], jnp.where(place == 2, right[1], right[2]))
        )
        return [first, second, third]
    whole = lax.all_gather(own, "tensor", axis=0)
    return [lax.dynamic_index_in_dim(whole, (place + k) % count, 0, False) for k in range(1, count)]


def label_index(k):
    count = lax.axis_size("tensor")
    place = lax.axis_index("tensor")
    if count == 4:
        table = LABELS[k - 1]
        return jnp.where(
            place == 0, table[0], jnp.where(place == 1, table[1], jnp.where(place == 2, table[2], table[3]))
        )
    return (place + k) % count


def in_order(own):
    count = lax.axis_size("tensor")
    place = lax.axis_index("tensor")
    if count == 4:
        right, left = line_streams(own)
        rows = []
        for want in range(4):
            pick = own
            for at in range(4):
                if at < want:
                    pick = jnp.where(place == at, left[want - at - 1], pick)
                elif at > want:
                    pick = jnp.where(place == at, right[at - want - 1], pick)
            rows.append(pick)
        return jnp.stack(rows, 0)
    return lax.all_gather(own, "tensor", axis=0)


def line_sum(own, parts):
    count = lax.axis_size("tensor")
    place = lax.axis_index("tensor")
    if count == 4:
        first, second, third = parts
        end = (place == 0) | (place == 3)
        right = along(third, [(0, 1)])
        left = along(third, [(3, 2)])
        arrived = jnp.where(place == 1, right, left)
        send = jnp.where(
            end, second, (third.astype(F32) + arrived.astype(F32)).astype(BF16)
        )
        right = along(send, [(0, 1), (1, 2)])
        left = along(send, [(3, 2), (2, 1)])
        send_right = (first.astype(F32) + right.astype(F32)).astype(BF16)
        send_left = (
            jnp.where(place == 3, first, second).astype(F32) + left.astype(F32)
        ).astype(BF16)
        right = along(send_right, [(0, 1), (1, 2), (2, 3)])
        left = along(send_left, [(3, 2), (2, 1), (1, 0)])
        return own.astype(F32) + right.astype(F32) + left.astype(F32)
    stack = jnp.zeros((count,) + own.shape, BF16)
    stack = lax.dynamic_update_index_in_dim(stack, own.astype(BF16), place, 0)
    for k in range(1, count):
        stack = lax.dynamic_update_index_in_dim(stack, parts[k - 1], label_index(k), 0)
    return lax.psum_scatter(stack, "tensor", scatter_dimension=0, tiled=False).astype(F32)


MESH = pl.DeviceIdType.MESH


def ring_places():
    s, t = lax.axis_index("seq"), lax.axis_index("tensor")
    c, x, y = s % 2, (s // 2) % 2, s // 4
    return s, t, c, x, y


def greet(targets):
    barrier = pltpu.get_barrier_semaphore()
    for target in targets:
        pl.semaphore_signal(barrier, inc=1, device_id=target, device_id_type=MESH)
    pl.semaphore_wait(barrier, len(targets))


def gather_kernel(count, *refs):
    weights, (small, cot, tokens) = refs[:count], refs[count : count + 3]
    full = refs[count + 3 : 2 * count + 3]
    smalls, cots, halo = refs[2 * count + 3 : 2 * count + 6]
    rest = refs[2 * count + 6 :]
    stage, rest = rest[: count + 2], rest[count + 2 :]
    local_sem, send_sem, recv_sem, line_send, line_recv, halo_sem = rest
    s, t, c, x, y = ring_places()
    s_core, s_x, s_y = s + 1 - 2 * c, s + 2 - 4 * x, s + 4 - 8 * y
    s_far = s_x + 4 - 8 * y
    right, left = (s, t + 1), (s, t - 1)
    near_x, near_y, core = (s_x, t), (s_y, t), (s_core, t)
    linear = 4 * s + t
    after, before = (linear + 1) % 32, (linear + 31) % 32
    greet(
        [(s, (t + 1) % 4), (s, (t + 3) % 4), near_x, near_y, core, (before // 4, before % 4)]
    )
    sent = []
    tail_rows = halo.shape[0]
    onward = pltpu.make_async_remote_copy(
        src_ref=tokens.at[pl.ds(tokens.shape[0] - tail_rows, tail_rows)], dst_ref=halo,
        send_sem=halo_sem.at[0], recv_sem=halo_sem.at[1],
        device_id=(after // 4, after % 4), device_id_type=MESH,
    )
    pl.when(linear < 31)(onward.start)

    def slot(w, tt, ss):
        return full[w].at[:, tt, ss]

    def copy(w, src, tt, ss, kind, target):
        return pltpu.make_async_remote_copy(
            src_ref=src, dst_ref=slot(w, tt, ss), send_sem=send_sem.at[w, tt, kind],
            recv_sem=recv_sem.at[w, tt, ss], device_id=target, device_id_type=MESH,
        )

    def arrived(w, tt, ss):
        copy(w, slot(w, tt, ss), tt, ss, 0, core).wait_recv()

    def send(w, src, tt, ss, kind, target, when=None):
        def go():
            copy(w, src, tt, ss, kind, target).start()

        def done():
            copy(w, src, tt, ss, kind, target).wait_send()

        if when is None:
            go()
            sent.append(done)
        else:
            pl.when(when)(go)
            sent.append(lambda: pl.when(when)(done))

    def spread(w, src, tt):
        send(w, src, tt, s, 2, near_x)
        send(w, src, tt, s, 3, near_y)
        send(w, src, tt, s, 4, core)

    def open_line(w):
        own = weights[w].at[:, s]
        send(w, own, t, s, 0, right, t < 3)
        send(w, own, t, s, 1, left, t > 0)
        spread(w, own, t)

    def line_events(w):
        for k in (1, 2, 3):
            for way in (-1, 1):
                tt = t + way * k

                def event(tt=tt, way=way, tail=sent):
                    arrived(w, tt, s)
                    if way < 0:
                        pl.when(t < 3)(lambda: copy(w, slot(w, tt, s), tt, s, 0, right).start())
                    else:
                        pl.when(t > 0)(lambda: copy(w, slot(w, tt, s), tt, s, 1, left).start())
                    copy(w, slot(w, tt, s), tt, s, 2, near_x).start()
                    copy(w, slot(w, tt, s), tt, s, 3, near_y).start()
                    copy(w, slot(w, tt, s), tt, s, 4, core).start()

                def finish(tt=tt, way=way):
                    if way < 0:
                        pl.when(t < 3)(lambda: copy(w, slot(w, tt, s), tt, s, 0, right).wait_send())
                    else:
                        pl.when(t > 0)(lambda: copy(w, slot(w, tt, s), tt, s, 1, left).wait_send())
                    for kind, target in ((2, near_x), (3, near_y), (4, core)):
                        copy(w, slot(w, tt, s), tt, s, kind, target).wait_send()

                ok = tt >= 0 if way < 0 else tt <= 3
                pl.when(ok)(event)
                sent.append(lambda ok=ok, finish=finish: pl.when(ok)(finish))

    def plane_events(w):
        for tt in range(4):
            arrived(w, tt, s_x)
            send(w, slot(w, tt, s_x), tt, s_x, 6, core)
            if tt % 2 == 0:
                send(w, slot(w, tt, s_x), tt, s_x, 5, near_y)
            arrived(w, tt, s_y)
            send(w, slot(w, tt, s_y), tt, s_y, 8, core)
            if tt % 2 == 1:
                send(w, slot(w, tt, s_y), tt, s_y, 7, near_x)

    def far_events(w):
        for tt in range(4):
            arrived(w, tt, s_far)
            send(w, slot(w, tt, s_far), tt, s_far, 9, core)

    def core_events(w):
        for tt in range(4):
            for base in (s, s_x, s_y, s_far):
                arrived(w, tt, base + 1 - 2 * c)

    lines = ((small, smalls), (cot, cots))

    def line_copy(v, src, tt, kind, target):
        return pltpu.make_async_remote_copy(
            src_ref=src, dst_ref=lines[v][1].at[tt], send_sem=line_send.at[v, tt, kind],
            recv_sem=line_recv.at[v, tt], device_id=target, device_id_type=MESH,
        )

    def open_other(v):
        own = lines[v][0]
        pl.when(t < 3)(lambda: line_copy(v, own, t, 0, right).start())
        pl.when(t > 0)(lambda: line_copy(v, own, t, 1, left).start())
        sent.append(lambda: pl.when(t < 3)(lambda: line_copy(v, own, t, 0, right).wait_send()))
        sent.append(lambda: pl.when(t > 0)(lambda: line_copy(v, own, t, 1, left).wait_send()))

    def other_events(v, k):
        whole = lines[v][1]
        for way in (-1, 1):
            tt = t + way * k
            kind, target = (0, right) if way < 0 else (1, left)
            more = t < 3 if way < 0 else t > 0

            def event(tt=tt, kind=kind, target=target, more=more):
                line_copy(v, whole.at[tt], tt, kind, target).wait_recv()
                pl.when(more)(lambda: line_copy(v, whole.at[tt], tt, kind, target).start())

            def finish(tt=tt, kind=kind, target=target, more=more):
                pl.when(more)(lambda: line_copy(v, whole.at[tt], tt, kind, target).wait_send())

            ok = tt >= 0 if way < 0 else tt <= 3
            pl.when(ok)(event)
            sent.append(lambda ok=ok, finish=finish: pl.when(ok)(finish))

    into = [pltpu.make_async_copy(weights[w].at[:, s], stage[w], local_sem.at[w]) for w in range(count)]
    out = [pltpu.make_async_copy(stage[w], slot(w, t, s), local_sem.at[w]) for w in range(count)]
    for v, (own, whole) in enumerate(lines):
        into.append(pltpu.make_async_copy(own, stage[count + v], local_sem.at[count + v]))
        out.append(pltpu.make_async_copy(stage[count + v], whole.at[t], local_sem.at[count + v]))

    open_other(0)
    for w in range(count):
        open_line(w)
    for move in into:
        move.start()
    line_events(0)
    line_events(1)
    for a, b in zip(into, out):
        a.wait()
        b.start()
    open_other(1)
    plane_events(0)
    line_events(2)
    far_events(0)
    plane_events(1)
    line_events(3)
    far_events(1)
    other_events(1, 1)
    plane_events(2)
    far_events(2)
    other_events(1, 2)
    plane_events(3)
    for k in (1, 2, 3):
        other_events(0, k)
    other_events(1, 3)
    far_events(3)
    for w in range(count):
        core_events(w)
    for move in out:
        move.wait()
    for done in sent:
        done()
    pl.when(linear > 0)(onward.wait_recv)
    pl.when(linear < 31)(onward.wait_send)


def gather_all(weights, small, cotangent, tokens, tail_rows):
    n_ten, n_seq = lax.axis_size("tensor"), lax.axis_size("seq")
    if not (n_ten == 4 and n_seq == 8):
        full = [jnp.moveaxis(lax.all_gather(w, "tensor", axis=0), 0, 1) for w in weights]
        devices = n_ten * n_seq
        halo = lax.ppermute(
            tokens[tokens.shape[0] - tail_rows :], BOTH, [(i, i + 1) for i in range(devices - 1)]
        )
        whole = (lax.all_gather(a, "tensor", axis=0) for a in (small, cotangent))
        return full, *whole, halo
    count = len(weights)
    cut = [w.reshape(w.shape[0], 8, w.shape[1] // 8, w.shape[2]) for w in weights]
    anywhere = pl.BlockSpec(memory_space=pl.ANY)
    outs = [jax.ShapeDtypeStruct((w.shape[0], 4) + w.shape[1:], w.dtype) for w in cut]
    outs += [jax.ShapeDtypeStruct((4,) + a.shape, a.dtype) for a in (small, cotangent)]
    outs.append(jax.ShapeDtypeStruct((tail_rows, tokens.shape[1]), tokens.dtype))
    dma = pltpu.SemaphoreType.DMA
    got = pl.pallas_call(
        functools.partial(gather_kernel, count),
        out_shape=outs,
        in_specs=[anywhere] * (count + 3),
        out_specs=[anywhere] * (count + 3),
        scratch_shapes=[pltpu.VMEM((w.shape[0],) + w.shape[2:], w.dtype) for w in cut]
        + [pltpu.VMEM(a.shape, a.dtype) for a in (small, cotangent)]
        + [
            dma((count + 2,)), dma((count, 4, 10)), dma((count, 4, 8)),
            dma((2, 4, 2)), dma((2, 4)), dma((2,)),
        ],
        compiler_params=pltpu.CompilerParams(collective_id=1, has_side_effects=True),
        name="gather",
    )(*cut, small, cotangent, tokens)
    full = [g.reshape(w.shape[0], 4, w.shape[1], w.shape[2]) for g, w in zip(got, weights)]
    return full, *got[count:]


def carry_kernel(reach, reverse, carry_ref, out_ref, send_sem, recv_sem):
    n_ten = lax.axis_size("tensor")
    devices = n_ten * lax.axis_size("seq")
    me = lax.axis_index("seq") * n_ten + lax.axis_index("tensor")
    way = -1 if reverse else 1

    def place(linear):
        return linear // n_ten, linear % n_ten

    greet([place((me - way * k + devices) % devices) for k in range(1, reach + 1)])

    def copy(k):
        return pltpu.make_async_remote_copy(
            src_ref=carry_ref, dst_ref=out_ref.at[k - 1], send_sem=send_sem.at[k - 1],
            recv_sem=recv_sem.at[k - 1], device_id=place((me + way * k + devices) % devices),
            device_id_type=MESH,
        )

    def there(k, back):
        spot = me - way * k if back else me + way * k
        return (spot >= 0) & (spot < devices)

    for k in range(1, reach + 1):
        pl.when(there(k, False))(lambda k=k: copy(k).start())
    for k in range(1, reach + 1):
        pl.when(there(k, True))(lambda k=k: copy(k).wait_recv())
        pl.when(there(k, False))(lambda k=k: copy(k).wait_send())


def entering(carry, reach, linear, devices, reverse):
    channels = carry.shape[1]
    vmem = pl.BlockSpec(memory_space=pltpu.VMEM)
    got = pl.pallas_call(
        functools.partial(carry_kernel, reach, reverse),
        out_shape=jax.ShapeDtypeStruct((reach, 2, channels), F32),
        in_specs=[vmem],
        out_specs=vmem,
        scratch_shapes=[pltpu.SemaphoreType.DMA((reach,)), pltpu.SemaphoreType.DMA((reach,))],
        compiler_params=pltpu.CompilerParams(
            collective_id=3 if reverse else 2, has_side_effects=True
        ),
        name="carry_back" if reverse else "carry",
    )(carry)
    state = jnp.zeros((1, channels), F32)
    for k in range(reach, 0, -1):
        source = linear + k if reverse else linear - k
        there = (source >= 0) & (source < devices)
        state = jnp.where(there, got[k - 1, 0:1] * state + got[k - 1, 1:2], state)
    return state


def pick4(t, a, b, c, d):
    return jnp.where(t == 0, a, jnp.where(t == 1, b, jnp.where(t == 2, c, d)))


def tail_kernel(lefts, rows, groups, chunk, share, *refs):
    n_a, n_b = max(lefts) + 1, len(lefts)
    a_refs, b_refs = refs[:n_a], refs[n_a : n_a + n_b]
    down_ref, gates_ref, small_ref, out_ref, land_ref, gates_out, small_out = refs[
        n_a + n_b : n_a + n_b + 7
    ]
    (
        a_all, b_all, product, to_x, to_y, to_far, far_x, far_y, from_x, from_y, total,
        line_send, line_recv, fill_sem, out_sem, pair_send, pair_recv,
        send_sem, recv_sem, zs_sem, zr_sem,
        down_send, down_recv,
        g_core, g_own, g_far, g_from, g_line, g_total, g_load, g_send, g_recv,
        acc, got, line, small_total, s_load, s_send, s_recv,
    ) = refs[n_a + n_b + 7 :]
    cols = groups * chunk
    s, t = lax.axis_index("seq"), lax.axis_index("tensor")
    c, x, y = s % 2, (s // 2) % 2, s // 4
    p = s // 2
    p_x, p_y = p + 1 - 2 * x, p + 2 - 4 * y
    p_far = p_x + 2 - 4 * y
    near_x, near_y, core = (s + 2 - 4 * x, t), (s + 4 - 8 * y, t), (s + 1 - 2 * c, t)
    right, left = (s, t + 1), (s, t - 1)
    greet([(s, (t + k) % 4) for k in (1, 2, 3)] + [near_x, near_y, core])
    half = share // 2
    steps = 4 * n_b

    def pass_down(label):
        third, second, first = pick4(t, 3, 3, 0, 0), pick4(t, 2, 0, 1, 1), pick4(t, 1, 2, 3, 2)
        target = (first, second, third)[label]
        return pltpu.make_async_remote_copy(
            src_ref=down_ref.at[label + 1], dst_ref=land_ref.at[t], send_sem=down_send.at[label],
            recv_sem=down_recv.at[t], device_id=(s, target), device_id_type=MESH,
        )

    def down_here(tt):
        return pltpu.make_async_remote_copy(
            src_ref=down_ref.at[0], dst_ref=land_ref.at[tt], send_sem=down_send.at[0],
            recv_sem=down_recv.at[tt], device_id=core, device_id_type=MESH,
        )

    def g_copy(k, src, dst, target):
        return pltpu.make_async_remote_copy(
            src_ref=src, dst_ref=dst, send_sem=g_send.at[k], recv_sem=g_recv.at[k],
            device_id=target, device_id_type=MESH,
        )

    g_pair = g_copy(0, gates_ref.at[:, 1 - c], g_core, core)
    g_fill = pltpu.make_async_copy(gates_ref.at[:, c], g_own, g_load.at[0])
    g_fars = (
        g_copy(1, g_own.at[p_far, pl.ds(0, 2)], g_far.at[0], near_x),
        g_copy(2, g_own.at[p_far, pl.ds(2, 2)], g_far.at[1], near_y),
    )
    g_nears = (
        g_copy(3, g_own.at[p_x], g_from.at[0], near_x),
        g_copy(4, g_own.at[p_y], g_from.at[1], near_y),
    )

    def g_hop(k, back):
        other = (t - k + 4) % 4 if back else (t + k) % 4
        return pltpu.make_async_remote_copy(
            src_ref=g_own.at[p, other], dst_ref=g_line.at[other if back else t],
            send_sem=g_send.at[4 + k], recv_sem=g_recv.at[4 + k],
            device_id=(s, other), device_id_type=MESH,
        )

    g_store = pltpu.make_async_copy(g_total, gates_out, g_load.at[1])

    def s_copy(k, target):
        return pltpu.make_async_remote_copy(
            src_ref=acc.at[k], dst_ref=got.at[k], send_sem=s_send.at[k], recv_sem=s_recv.at[k],
            device_id=target, device_id_type=MESH,
        )

    s_turns = (s_copy(0, core), s_copy(1, near_x), s_copy(2, near_y))

    def s_hop(k, back):
        other = (t - k + 4) % 4 if back else (t + k) % 4
        return pltpu.make_async_remote_copy(
            src_ref=acc.at[3], dst_ref=line.at[other if back else t],
            send_sem=s_send.at[2 + k], recv_sem=s_recv.at[2 + k],
            device_id=(s, other), device_id_type=MESH,
        )

    s_fill = pltpu.make_async_copy(small_ref, acc.at[0], s_load.at[0])
    s_store = pltpu.make_async_copy(small_total, small_out, s_load.at[1])

    def small_steps(n):
        @pl.when(n == 0)
        def _():
            s_fill.wait()
            s_turns[0].start()

        @pl.when(n == 1)
        def _():
            s_turns[0].wait_recv()
            acc[1] = acc[0] + got[0]
            s_turns[1].start()
            g_fill.wait()
            g_pair.wait_recv()
            for q in range(4):
                g_own[q] = (g_own[q].astype(F32) + g_core[q].astype(F32)).astype(BF16)
            for move in g_fars:
                move.start()

        @pl.when(n == 2)
        def _():
            s_turns[1].wait_recv()
            acc[2] = acc[1] + got[1]
            s_turns[2].start()
            for move in g_fars:
                move.wait_recv()
            g_own[p_y, pl.ds(0, 2)] = (
                g_own[p_y, pl.ds(0, 2)].astype(F32) + g_far[0].astype(F32)
            ).astype(BF16)
            g_own[p_x, pl.ds(2, 2)] = (
                g_own[p_x, pl.ds(2, 2)].astype(F32) + g_far[1].astype(F32)
            ).astype(BF16)
            for move in g_nears:
                move.start()

        @pl.when(n == 3)
        def _():
            s_turns[2].wait_recv()
            acc[3] = acc[2] + got[2]
            line[t] = acc[3]
            for move in g_nears:
                move.wait_recv()
            g_own[p] = (
                g_own[p].astype(F32) + g_from[0].astype(F32) + g_from[1].astype(F32)
            ).astype(BF16)
            g_line[t] = g_own[p, t]
            for k in (1, 2, 3):
                s_hop(k, False).start()
                g_hop(k, False).start()

        @pl.when(n == 6)
        def _():
            for k in (1, 2, 3):
                s_hop(k, True).wait_recv()
                g_hop(k, True).wait_recv()
            small_total[...] = line[0] + line[1] + line[2] + line[3]
            g_total[...] = (
                g_line[0].astype(F32) + g_line[1].astype(F32)
                + g_line[2].astype(F32) + g_line[3].astype(F32)
            )
            s_store.start()
            g_store.start()

    s_fill.start()
    g_fill.start()
    g_pair.start()
    for label in (2, 1, 0):
        pass_down(label).start()

    def fill_b(w, k):
        tt, j = k // groups, k % groups
        return pltpu.make_async_copy(
            b_refs[w].at[:, pl.ds(pl.multiple_of((j * 4 + tt) * chunk, 128), chunk)],
            b_all.at[w, tt, pl.ds(0, rows), pl.ds(pl.multiple_of(j * chunk, 128), chunk)],
            fill_sem.at[n_a + w, k],
        )

    def fill_a(v):
        return pltpu.make_async_copy(a_refs[v], a_all.at[v, pl.ds(0, rows)], fill_sem.at[v, 0])

    def pair_a(v):
        return pltpu.make_async_remote_copy(
            src_ref=a_refs[v], dst_ref=a_all.at[v, pl.ds(rows, rows)],
            send_sem=pair_send.at[v, 0], recv_sem=pair_recv.at[v, 0],
            device_id=core, device_id_type=MESH,
        )

    def pair_b(w, k):
        return pltpu.make_async_remote_copy(
            src_ref=b_all.at[w, k, pl.ds(0, rows)], dst_ref=b_all.at[w, k, pl.ds(rows, rows)],
            send_sem=pair_send.at[n_a + w, k], recv_sem=pair_recv.at[n_a + w, k],
            device_id=core, device_id_type=MESH,
        )

    for w in range(n_b):
        if w == 0 or lefts[w] != lefts[w - 1]:
            pair_a(lefts[w]).start()
            fill_a(lefts[w]).start()

        @pl.loop(0, 4 * groups)
        def _(k, w=w):
            fill_b(w, k).start()

    for w in range(n_b):

        @pl.loop(0, 4 * groups)
        def _(k, w=w):
            fill_b(w, k).wait()

        @pl.loop(0, 4)
        def _(k, w=w):
            pair_b(w, k).start()

    for v in range(n_a):
        fill_a(v).wait()
        pair_a(v).wait_recv()

    def dest(n):
        i = n % 4
        third, second, first = pick4(t, 3, 3, 0, 0), pick4(t, 2, 0, 1, 1), pick4(t, 1, 2, 3, 2)
        return pick4(i, third, second, first, t)

    def make(n, q):
        w = n // 4
        start = pl.multiple_of(2 * share * q + (share - 64) * c, 128)
        v = sum(jnp.where(w >= k, lefts[k] - (lefts[k - 1] if k else 0), 0) for k in range(n_b))
        lhs = a_all[v, :, pl.ds(start, share + 64)]
        rhs = b_all[w, dest(n)]
        product[...] = lax.dot_general(lhs, rhs, (((0,), (0,)), ((), ())), preferred_element_type=F32)
        return product[pl.ds(pl.multiple_of(64 * c, 64), share), :]

    def remote(n, src, dst, k, target):
        return pltpu.make_async_remote_copy(
            src_ref=src, dst_ref=dst, send_sem=send_sem.at[n, k], recv_sem=recv_sem.at[n, k],
            device_id=target, device_id_type=MESH,
        )

    def directs(n):
        return (
            remote(n, to_far.at[n, pl.ds(0, half)], far_x.at[n], 0, near_x),
            remote(n, to_far.at[n, pl.ds(half, half)], far_y.at[n], 1, near_y),
            remote(n, to_x.at[n, pl.ds(0, half)], from_x.at[n, pl.ds(0, half)], 2, near_x),
            remote(n, to_y.at[n, pl.ds(half, half)], from_y.at[n, pl.ds(half, half)], 3, near_y),
        )

    def seconds(n):
        return (
            remote(n, to_x.at[n, pl.ds(half, half)], from_x.at[n, pl.ds(half, half)], 4, near_x),
            remote(n, to_y.at[n, pl.ds(0, half)], from_y.at[n, pl.ds(0, half)], 5, near_y),
        )

    def begin(n):
        pair_b(n // 4, dest(n)).wait_recv()
        to_far[n] = make(n, p_far).astype(BF16)
        directs(n)[0].start()
        directs(n)[1].start()
        to_x[n] = make(n, p_x).astype(BF16)
        directs(n)[2].start()
        to_y[n] = make(n, p_y).astype(BF16)
        directs(n)[3].start()

    def forward(n):
        first, second = directs(n)[:2]
        first.wait_recv()
        to_y[n, pl.ds(0, half)] = (
            to_y[n, pl.ds(0, half)].astype(F32) + far_x[n].astype(F32)
        ).astype(BF16)
        seconds(n)[1].start()
        second.wait_recv()
        to_x[n, pl.ds(half, half)] = (
            to_x[n, pl.ds(half, half)].astype(F32) + far_y[n].astype(F32)
        ).astype(BF16)
        seconds(n)[0].start()

    def hop(w, out, into, target):
        return pltpu.make_async_remote_copy(
            src_ref=line_send.at[w, out], dst_ref=line_recv.at[w, into],
            send_sem=zs_sem.at[w, out], recv_sem=zr_sem.at[w, into],
            device_id=target, device_id_type=MESH,
        )

    end = (t == 0) | (t == 3)

    def finish(n):
        w, i = n // 4, n % 4
        mine = make(n, p)
        for move in directs(n)[2:] + seconds(n):
            move.wait_recv()
        total[w] = mine + from_x[n].astype(F32) + from_y[n].astype(F32)

        @pl.when((i < 3) & end)
        def _():
            line_send[w, i] = total[w].astype(BF16)

        @pl.when((i == 0) & (t == 0))
        def _():
            hop(w, 0, 0, right).start()

        @pl.when((i == 0) & (t == 3))
        def _():
            hop(w, 0, 0, left).start()

        @pl.when((i == 1) & (t == 0))
        def _():
            hop(w, 1, 1, right).start()

        @pl.when((i == 1) & (t == 3))
        def _():
            hop(w, 1, 2, left).start()

        @pl.when((i == 2) & (t == 0))
        def _():
            hop(w, 2, 3, right).start()

        @pl.when((i == 2) & (t == 3))
        def _():
            hop(w, 2, 4, left).start()

        @pl.when((i == 0) & (t == 1))
        def _():
            hop(w, 0, 0, right).wait_recv()
            line_send[w, 0] = (total[w] + line_recv[w, 0].astype(F32)).astype(BF16)
            hop(w, 0, 1, right).start()

        @pl.when((i == 0) & (t == 2))
        def _():
            hop(w, 0, 0, left).wait_recv()
            line_send[w, 0] = (total[w] + line_recv[w, 0].astype(F32)).astype(BF16)
            hop(w, 0, 2, left).start()

        @pl.when((i == 1) & ~end)
        def _():
            hop(w, 1, 2, left).wait_recv()
            line_send[w, 1] = (total[w] + line_recv[w, 2].astype(F32)).astype(BF16)
            hop(w, 1, 4, left).start()

        @pl.when((i == 2) & ~end)
        def _():
            hop(w, 1, 1, right).wait_recv()
            line_send[w, 2] = (total[w] + line_recv[w, 1].astype(F32)).astype(BF16)
            hop(w, 2, 3, right).start()

    @pl.loop(0, steps + 3)
    def _(n):
        @pl.when(n < steps)
        def _():
            begin(n)

        @pl.when((n >= 1) & (n <= steps))
        def _():
            forward(n - 1)

        small_steps(n)

        @pl.when(n >= 3)
        def _():
            finish(n - 3)

    def result(w):
        return pltpu.make_async_copy(total.at[w], out_ref.at[w], out_sem.at[w])

    for w in range(n_b):

        @pl.when(t > 0)
        def _(w=w):
            hop(w, 2, 3, right).wait_recv()
            total[w] = total[w] + line_recv[w, 3].astype(F32)

        @pl.when(t < 3)
        def _(w=w):
            hop(w, 2, 4, left).wait_recv()
            total[w] = total[w] + line_recv[w, 4].astype(F32)

        result(w).start()

    @pl.loop(0, steps)
    def _(n):
        for move in directs(n) + seconds(n):
            move.wait_send()

    for w in range(n_b):
        for k in range(3):
            hop(w, k, 0, right).wait_send()
        result(w).wait()

        @pl.loop(0, 4)
        def _(k, w=w):
            pair_b(w, k).wait_send()

    for v in range(n_a):
        pair_a(v).wait_send()

    for label in range(3):
        pass_down(label).wait_send()
    for tt in range(4):
        pl.when(t != tt)(lambda tt=tt: down_here(tt).wait_recv())
    for move in (g_pair,) + g_fars + g_nears + s_turns:
        move.wait_send()
    for k in (1, 2, 3):
        s_hop(k, False).wait_send()
        g_hop(k, False).wait_send()
    s_store.wait()
    g_store.wait()


def weight_grads(lefts, a_list, b_list, groups, downs, blocks, small):
    n_ten, n_seq = lax.axis_size("tensor"), lax.axis_size("seq")
    rows, width = a_list[0].shape
    channels = b_list[0].shape[1]
    chunk = channels // groups // n_ten
    share = width // n_seq
    if not (n_ten == 4 and n_seq == 8):
        out = []
        for v, b in zip(lefts, b_list):
            b = jnp.swapaxes(b.reshape(rows, groups, n_ten, chunk), 1, 2).reshape(rows, channels)
            grad = dot_tn(a_list[v], b).astype(BF16)
            grad = lax.psum_scatter(grad, "seq", scatter_dimension=0, tiled=True)
            out.append(lax.psum_scatter(grad, "tensor", scatter_dimension=1, tiled=True).astype(F32))
        sums = lax.psum_scatter(blocks, BOTH, scatter_dimension=0, tiled=True)[0].astype(F32)
        return out, line_sum(downs[0], downs[1:]), sums, lax.psum(small, BOTH)
    count, cols = len(b_list), groups * chunk
    half, steps = share // 2, 4 * count
    anywhere = pl.BlockSpec(memory_space=pl.ANY)
    dma = pltpu.SemaphoreType.DMA

    def room(*dims):
        return pltpu.VMEM(dims, BF16)

    both = len(a_list) + count
    blocks = blocks.reshape((4, 2, 4) + blocks.shape[1:])
    piece = blocks.shape[3:]
    grads, land, block_sum, small_sum = pl.pallas_call(
        functools.partial(tail_kernel, lefts, rows, groups, chunk, share),
        out_shape=[
            jax.ShapeDtypeStruct((count, share, cols), F32),
            jax.ShapeDtypeStruct((4, rows, width), BF16),
            jax.ShapeDtypeStruct(piece, F32),
            jax.ShapeDtypeStruct(small.shape, F32),
        ],
        in_specs=[anywhere] * (both + 3),
        out_specs=[anywhere] * 4,
        scratch_shapes=[
            room(len(a_list), 2 * rows, width), room(count, 4, 2 * rows, cols),
            pltpu.VMEM((share + 64, cols), F32),
            room(steps, share, cols), room(steps, share, cols), room(steps, share, cols),
            room(steps, half, cols), room(steps, half, cols),
            room(steps, share, cols), room(steps, share, cols),
            pltpu.VMEM((count, share, cols), F32),
            room(count, 3, share, cols), room(count, 5, share, cols),
            dma((both, 4 * groups)), dma((count,)), dma((both, 4)), dma((both, 4)),
            dma((steps, 6)), dma((steps, 6)), dma((count, 3)), dma((count, 5)),
            dma((3,)), dma((4,)),
            room(4, 4, *piece), room(4, 4, *piece), room(2, 2, *piece), room(2, 4, *piece),
            room(4, *piece), pltpu.VMEM(piece, F32), dma((2,)), dma((8,)), dma((8,)),
            pltpu.VMEM((4,) + small.shape, F32), pltpu.VMEM((3,) + small.shape, F32),
            pltpu.VMEM((4,) + small.shape, F32), pltpu.VMEM(small.shape, F32),
            dma((2,)), dma((6,)), dma((6,)),
        ],
        compiler_params=pltpu.CompilerParams(
            collective_id=4, has_side_effects=True, vmem_limit_bytes=67043328
        ),
        cost_estimate=pl.CostEstimate(
            flops=2 * count * rows * width * channels, bytes_accessed=1 << 29, transcendentals=0
        ),
        name="tail",
    )(*a_list, *b_list, downs, blocks, small)
    place = lax.axis_index("tensor")
    down = downs[0].astype(F32)
    for k in range(4):
        down = down + jnp.where(place == k, 0.0, land[k].astype(F32))
    return grads, down, block_sum, small_sum


def feed_kernel(tiles, parts, own_ref, cots_ref, wg_ref, wu_ref, wd_ref, *refs):
    tokens_ref, hid_ref, gg_ref, ug_ref, sum_ref, down_ref = refs[:6]
    (
        wg, wu, wd, tok, cot, hid, gg, ug, part, land, total, down,
        load_sem, store_sem, sum_sem, ag_send, ag_recv, rs_send, rs_recv,
    ) = refs[6:]
    s, t = lax.axis_index("seq"), lax.axis_index("tensor")
    right, left = (s, t + 1), (s, t - 1)
    width, units = wg.shape
    span, cut = width // tiles, units // parts
    greet([(s, (t + 1) % 4), (s, (t + 3) % 4)])

    def pass_on(src, tt, kind):
        return pltpu.make_async_remote_copy(
            src_ref=src, dst_ref=tokens_ref.at[tt], send_sem=ag_send.at[tt, kind],
            recv_sem=ag_recv.at[tt], device_id=left if kind else right, device_id_type=MESH,
        )

    pl.when(t < 3)(lambda: pass_on(own_ref, t, 0).start())
    pl.when(t > 0)(lambda: pass_on(own_ref, t, 1).start())
    weights = [
        pltpu.make_async_copy(src, dst, load_sem.at[2 + k])
        for k, (src, dst) in enumerate(((wg_ref, wg), (wu_ref, wu), (wd_ref, wd)))
    ]
    for move in weights:
        move.start()

    def whose(i):
        third, second, first = pick4(t, 3, 3, 0, 0), pick4(t, 2, 0, 1, 1), pick4(t, 1, 2, 3, 2)
        return pick4(i, t, first, second, third)

    def stores(i):
        ch = whose(i)
        return [
            pltpu.make_async_copy(src, dst.at[ch], store_sem.at[k])
            for k, (src, dst) in enumerate(((hid, hid_ref), (gg, gg_ref), (ug, ug_ref)))
        ]

    def hop(label, k, way):
        return pltpu.make_async_remote_copy(
            src_ref=part.at[label, k], dst_ref=land.at[way, label, k],
            send_sem=rs_send.at[label, k], recv_sem=rs_recv.at[way, label, k],
            device_id=left if way else right, device_id_type=MESH,
        )

    def landed(label, k, way):
        hop(label, k, way).wait_recv()
        return land[way, label, k].astype(F32)

    def put_down(i):
        return pltpu.make_async_copy(down, down_ref.at[i], store_sem.at[4])

    def column(k, size):
        return pl.ds(pl.multiple_of(k * size, 128), size)

    def give(i, k, value):
        label = i - 1

        @pl.when(i == 0)
        def _():
            total[k] = value

        @pl.when((i > 0) & ((i < 3) | (t == 0) | (t == 3)))
        def _():
            part[label, k] = value.astype(BF16)

        @pl.when((i > 0) & (t == 0))
        def _():
            hop(label, k, 0).start()

        @pl.when((i > 0) & (t == 3))
        def _():
            hop(label, k, 1).start()

        @pl.when((i == 3) & (t == 1))
        def _():
            part[2, k] = (value + landed(2, k, 0)).astype(BF16)
            hop(2, k, 0).start()

        @pl.when((i == 3) & (t == 2))
        def _():
            part[2, k] = (value + landed(2, k, 1)).astype(BF16)
            hop(2, k, 1).start()

    @pl.loop(0, 4)
    def _(i):
        ch = whose(i)
        for way in (-1, 1):
            tt = t + way * i
            ok = (i > 0) & (tt >= 0) & (tt <= 3)

            @pl.when(ok)
            def _(tt=tt, way=way):
                pass_on(tokens_ref.at[tt], tt, 0).wait_recv()
                if way < 0:
                    pl.when(t < 3)(lambda: pass_on(tokens_ref.at[tt], tt, 0).start())
                else:
                    pl.when(t > 0)(lambda: pass_on(tokens_ref.at[tt], tt, 1).start())

        get_cot = pltpu.make_async_copy(cots_ref.at[ch], cot, load_sem.at[1])
        get_cot.start()

        @pl.when(i == 0)
        def _():
            move = pltpu.make_async_copy(own_ref, tok, load_sem.at[0])
            move.start()
            move.wait()
            pltpu.make_async_copy(tok, tokens_ref.at[t], store_sem.at[3]).start()
            for move in weights:
                move.wait()

        @pl.when(i == 1)
        def _():
            pltpu.make_async_copy(tok, tokens_ref.at[t], store_sem.at[3]).wait()

        @pl.when(i > 0)
        def _():
            move = pltpu.make_async_copy(tokens_ref.at[ch], tok, load_sem.at[0])
            move.start()
            move.wait()
            for store in stores(i - 1):
                store.wait()
            put_down(i - 1).wait()

        get_cot.wait()

        @pl.loop(0, parts)
        def _(f):
            here = column(f, cut)
            gate_vals = jnp.dot(tok[...], wg[:, here], preferred_element_type=F32)
            up_vals = jnp.dot(tok[...], wu[:, here], preferred_element_type=F32)
            back = lax.dot_general(
                cot[...], wd[here, :], (((1,), (1,)), ((), ())), preferred_element_type=F32
            )
            value, slope = gelu_both(gate_vals)
            hid[:, here] = (value * up_vals).astype(BF16)
            gg[:, here] = (back * up_vals * slope).astype(BF16)
            ug[:, here] = (back * value).astype(BF16)

        for store in stores(i):
            store.start()

        @pl.loop(0, tiles)
        def _(k):
            here = column(k, span)
            value = lax.dot_general(
                gg[...], wg[here, :], (((1,), (1,)), ((), ())), preferred_element_type=F32
            ) + lax.dot_general(
                ug[...], wu[here, :], (((1,), (1,)), ((), ())), preferred_element_type=F32
            )
            give(i, k, value)

        @pl.loop(0, tiles)
        def _(k):
            here = column(k, span)
            down[:, here] = jnp.dot(hid[...], wd[:, here], preferred_element_type=F32).astype(BF16)

        put_down(i).start()

    def add_and_send(k, label, arrived, way):
        part[label, k] = (part[label, k].astype(F32) + landed(arrived, k, way)).astype(BF16)
        hop(label, k, way).start()

    def add_total(k, label, way):
        total[k] = total[k] + landed(label, k, way)

    def put_sum(k):
        return pltpu.make_async_copy(total.at[k], sum_ref.at[:, column(k, span)], sum_sem.at[k])

    @pl.loop(0, tiles)
    def _(k):
        pl.when(t == 1)(lambda: add_and_send(k, 0, 1, 0))
        pl.when(t == 2)(lambda: add_and_send(k, 1, 1, 1))
        pl.when(t == 1)(lambda: add_and_send(k, 1, 2, 1))
        pl.when(t == 2)(lambda: add_and_send(k, 0, 2, 0))

    @pl.loop(0, tiles)
    def _(k):
        pl.when(t == 0)(lambda: add_total(k, 1, 1))
        pl.when(t > 0)(lambda: add_total(k, 0, 0))
        pl.when(t == 1)(lambda: add_total(k, 1, 1))
        pl.when(t == 2)(lambda: add_total(k, 0, 1))
        put_sum(k).start()

    @pl.loop(0, tiles)
    def _(k):
        put_sum(k).wait()
        for label in range(3):
            hop(label, k, 0).wait_send()

    put_down(3).wait()
    for store in stores(3):
        store.wait()
    pl.when(t < 3)(lambda: pass_on(own_ref, t, 0).wait_send())
    pl.when(t > 0)(lambda: pass_on(own_ref, t, 1).wait_send())
    for i in (1, 2, 3):
        pl.when((t - i >= 0) & (t < 3))(
            lambda i=i: pass_on(tokens_ref.at[t - i], t - i, 0).wait_send()
        )
        pl.when((t + i <= 3) & (t > 0))(
            lambda i=i: pass_on(tokens_ref.at[t + i], t + i, 1).wait_send()
        )


def feed_forward(own, cots, w_gate, w_up, w_down):
    rows, width = own.shape
    units = w_gate.shape[1]
    tiles, parts = 4, 5
    anywhere = pl.BlockSpec(memory_space=pl.ANY)
    dma = pltpu.SemaphoreType.DMA

    def room(*dims):
        return pltpu.VMEM(dims, BF16)

    def out(*dims, kind=BF16):
        return jax.ShapeDtypeStruct(dims, kind)

    flops = 2 * 4 * rows * width * units * 6
    got = pl.pallas_call(
        functools.partial(feed_kernel, tiles, parts),
        out_shape=[
            out(4, rows, width), out(4, rows, units), out(4, rows, units), out(4, rows, units),
            out(rows, width, kind=F32), out(4, rows, width),
        ],
        in_specs=[anywhere] * 5,
        out_specs=[anywhere] * 6,
        scratch_shapes=[
            room(width, units), room(width, units), room(units, width),
            room(rows, width), room(rows, width),
            room(rows, units), room(rows, units), room(rows, units),
            room(3, tiles, rows, width // tiles), room(2, 3, tiles, rows, width // tiles),
            pltpu.VMEM((tiles, rows, width // tiles), F32), room(rows, width),
            dma((5,)), dma((5,)), dma((tiles,)), dma((4, 2)), dma((4,)),
            dma((3, tiles)), dma((2, 3, tiles)),
        ],
        compiler_params=pltpu.CompilerParams(
            collective_id=5, has_side_effects=True, vmem_limit_bytes=67043328
        ),
        cost_estimate=pl.CostEstimate(flops=flops, bytes_accessed=3 << 27, transcendentals=0),
        name="feed",
    )(own, cots, w_gate, w_up, w_down)
    return got


def chunk_scan(a_ref, d_ref, p_ref, s_ref, reverse):
    tiles, rows, wide = a_ref.shape
    run = rows // 8

    def first(i, carry):
        r = run - 1 - i if reverse else i
        here = pl.ds(r, 8, stride=run)
        after = []
        for b in range(tiles):
            prod, state = carry[b]
            a = a_ref[b, here, :]
            prod = prod * a
            state = a * state + d_ref[b, here, :]
            a_ref[b, here, :] = prod
            d_ref[b, here, :] = state
            after.append((prod, state))
        return tuple(after)

    start = (jnp.ones((8, wide), F32), jnp.zeros((8, wide), F32))
    ends = lax.fori_loop(0, run, first, (start,) * tiles, unroll=4)
    leads, totals = [], []
    for b in range(tiles):
        prod, state = ends[b]
        enter_p, enter_s = [None] * 8, [None] * 8
        now_p, now_s = jnp.ones((1, wide), F32), jnp.zeros((1, wide), F32)
        for c in range(7, -1, -1) if reverse else range(8):
            enter_p[c], enter_s[c] = now_p, now_s
            now_p, now_s = now_p * prod[c : c + 1], prod[c : c + 1] * now_s + state[c : c + 1]
        leads.append((jnp.concatenate(enter_p, 0), jnp.concatenate(enter_s, 0)))
        totals.append((now_p, now_s))

    def second(r, _):
        here = pl.ds(r, 8, stride=run)
        for b in range(tiles):
            p = a_ref[b, here, :]
            a_ref[b, here, :] = p * leads[b][0]
            d_ref[b, here, :] = d_ref[b, here, :] + p * leads[b][1]
        return 0

    lax.fori_loop(0, run, second, 0, unroll=4)
    for b in range(tiles):
        p_ref[:, b * wide : (b + 1) * wide] = a_ref[b]
        s_ref[:, b * wide : (b + 1) * wide] = d_ref[b]
    return jnp.concatenate([p for p, _ in totals], 1), jnp.concatenate([v for _, v in totals], 1)


def tiled_store(ref, value):
    tiles, _, wide = ref.shape
    for b in range(tiles):
        ref[b] = value[:, b * wide : (b + 1) * wide]


def positions(base_ref, rows, lanes, length):
    place = lax.broadcasted_iota(jnp.int32, (rows, lanes), 0) + base_ref[0]
    return jnp.where(place >= length, place - length, place)


def forward_kernel(
    length, local, base_ref, x_ref, cw_ref, rate_gain_ref, g_ref, sel_ref,
    conv_ref, rate_ref, in_ref, p_ref, s_ref, carry_ref, w_ref, a_ref, d_ref,
):
    rows, lanes = conv_ref.shape
    spot = positions(base_ref, rows, lanes, length)
    x = x_ref[...].astype(F32)
    total = cw_ref[0:1, :] * x[HALO:]
    for k in range(1, CONV):
        moved = pltpu.roll(x, k, 0)[HALO:]
        total = total + jnp.where(spot >= k, cw_ref[k : k + 1, :] * moved, 0.0)
    conv = total.astype(BF16)
    conv_ref[...] = conv
    join = sel_ref.shape[0]
    wide = jnp.dot(g_ref[0], sel_ref[0], preferred_element_type=F32)
    for q in range(1, join):
        other = jnp.dot(g_ref[0], sel_ref[q], preferred_element_type=F32)
        which = lax.broadcasted_iota(jnp.int32, wide.shape, 0) // local % join
        wide = jnp.where(which == q, other, wide)
    gates = wide.astype(BF16)
    w_ref[0] = gates
    pre = lax.dot_general(conv, gates, (((1,), (1,)), ((), ())), preferred_element_type=F32)
    rate, inp = pre[:, :lanes], pre[:, lanes:]
    rate_ref[...] = rate
    in_ref[...] = inp
    decay = jnp.where(spot == 0, 0.0, jnp.exp(rate_gain_ref[...] * jax.nn.sigmoid(rate)))
    tiled_store(a_ref, decay)
    tiled_store(
        d_ref,
        jnp.sqrt(jnp.maximum(1.0 - decay * decay, 0.01)) * jax.nn.sigmoid(inp) * conv.astype(F32),
    )
    prod, state = chunk_scan(a_ref, d_ref, p_ref, s_ref, False)
    carry_ref[0:1, :] = prod
    carry_ref[1:2, :] = state


def middle_kernel(
    length, base_ref, mg_ref, y_ref, p_ref, s_ref, enter_ref, rate_ref, rate_gain_ref,
    ylow_ref, bp_ref, bs_ref, carry_ref, a_ref, d_ref,
):
    rows, lanes = mg_ref.shape
    spot = positions(base_ref, rows, lanes, length)
    states = s_ref[...] + p_ref[...] * enter_ref[...]
    value, slope = gelu_both(y_ref[...])
    grad = mg_ref[...]
    ylow_ref[...] = (grad * states * slope).astype(BF16)
    tiled_store(d_ref, grad * value)
    decay = jnp.where(spot == 0, 0.0, jnp.exp(rate_gain_ref[...] * jax.nn.sigmoid(rate_ref[...])))
    row = lax.broadcasted_iota(jnp.int32, (rows, lanes), 0)
    tiled_store(a_ref, jnp.where(row == rows - 1, 1.0, pltpu.roll(decay, rows - 1, 0)))
    prod, state = chunk_scan(a_ref, d_ref, bp_ref, bs_ref, True)
    carry_ref[0:1, :] = decay[0:1] * prod
    carry_ref[1:2, :] = decay[0:1] * state


def backward_kernel(
    length, local, base_ref, bp_ref, bs_ref, leave_ref, p_ref, s_ref, enter_ref, rate_ref, in_ref,
    conv_ref, rate_gain_ref, w_ref, cw_ref, x_ref, sel_ref,
    gates_ref, xback_ref, edge_ref, small_ref,
):
    rows, lanes = bp_ref.shape
    spot = positions(base_ref, rows, lanes, length)
    row = lax.broadcasted_iota(jnp.int32, (rows, lanes), 0)
    adjoint = bs_ref[...] + bp_ref[...] * leave_ref[...]
    states = s_ref[...] + p_ref[...] * enter_ref[...]
    before = jnp.where(row == 0, enter_ref[...], pltpu.roll(states, 1, 0))
    gain = rate_gain_ref[...]
    sig_r = jax.nn.sigmoid(rate_ref[...])
    sig_i = jax.nn.sigmoid(in_ref[...])
    conv = conv_ref[...]
    conv_f = conv.astype(F32)
    decay = jnp.where(spot == 0, 0.0, jnp.exp(gain * sig_r))
    room = 1.0 - decay * decay
    scale = jnp.sqrt(jnp.maximum(room, 0.01))
    pulled = adjoint * sig_i
    slope = jnp.where(room > 0.01, -decay / scale, 0.0)
    decay_grad = adjoint * before + pulled * conv_f * slope
    log_grad = decay_grad * decay
    pull_r = log_grad * sig_r
    rate_back = (pull_r * gain * (1.0 - sig_r)).astype(BF16)
    conv_direct = pulled * scale
    in_back = (conv_direct * conv_f * (1.0 - sig_i)).astype(BF16)
    both = jnp.concatenate([rate_back, in_back], 1)
    join = sel_ref.shape[0]
    for q in range(join):
        some = lax.dot_general(
            conv, sel_ref[q], (((1,), (1,)), ((), ())), preferred_element_type=F32
        ).astype(BF16)
        part = lax.dot_general(some, both, (((0,), (0,)), ((), ())), preferred_element_type=F32)
        if q == 0:
            gate_sum = part
        else:
            which = lax.broadcasted_iota(jnp.int32, part.shape, 1) // local % join
            gate_sum = jnp.where(which == q, part, gate_sum)
    runs, places, _, kinds, part, wide = gates_ref.shape
    gate_low = gate_sum.astype(BF16)
    for r in range(runs):
        for q in range(places):
            for kind in range(kinds):
                at = (kind * places + q) * wide
                gates_ref[r, q, 0, kind] = gate_low[r * part : (r + 1) * part, at : at + wide]
    grad = conv_direct + lax.dot_general(
        both, w_ref[0], (((1,), (0,)), ((), ())), preferred_element_type=F32
    )
    x = x_ref[...].astype(F32)
    zeros = jnp.zeros((HALO, lanes), F32)
    out = jnp.concatenate([zeros, grad * cw_ref[0:1, :]], 0)
    small_ref[0:1, :] = jnp.sum(grad * x[HALO:], axis=0, keepdims=True)
    for k in range(1, CONV):
        masked = jnp.where(spot >= k, grad, 0.0)
        small_ref[k : k + 1, :] = jnp.sum(
            masked * pltpu.roll(x, k, 0)[HALO:], axis=0, keepdims=True
        )
        tall = jnp.concatenate([zeros, masked * cw_ref[k : k + 1, :]], 0)
        out = out + pltpu.roll(tall, rows + HALO - k, 0)
    small_ref[CONV : CONV + 1, :] = jnp.sum(pull_r, axis=0, keepdims=True)
    small_ref[CONV + 1 : 8, :] = jnp.zeros((7 - CONV, lanes), F32)
    edge_ref[...] = out[:HALO]
    xback_ref[...] = out[HALO:]


def lane_call(kernel, grid, lanes, base, operands, outputs, scratch, flops):
    def spec(shape):
        if len(shape) == 6:
            return pl.BlockSpec(
                shape[:2] + (1,) + shape[3:], lambda j, *_: (0, 0, j, 0, 0, 0)
            )
        if len(shape) == 3 and shape[0] != grid:
            return pl.BlockSpec(shape, lambda j, *_: (0, 0, 0))
        if len(shape) == 3:
            return pl.BlockSpec((1,) + shape[1:], lambda j, *_: (j, 0, 0))
        return pl.BlockSpec((shape[0], lanes), lambda j, *_: (0, j))

    moved = sum(math.prod(a.shape) * a.dtype.itemsize for a in list(operands) + list(outputs))
    return pl.pallas_call(
        kernel,
        grid_spec=pltpu.PrefetchScalarGridSpec(
            num_scalar_prefetch=1,
            grid=(grid,),
            in_specs=[spec(a.shape) for a in operands],
            out_specs=[spec(a.shape) for a in outputs],
            scratch_shapes=scratch,
        ),
        out_shape=outputs,
        compiler_params=pltpu.CompilerParams(
            dimension_semantics=("arbitrary",), vmem_limit_bytes=56 << 20
        ),
        cost_estimate=pl.CostEstimate(flops=flops, bytes_accessed=moved, transcendentals=0),
    )(base, *operands)


def shards(
    tokens_in, gain_pre, w_x, w_y, conv_w, gate_a, gate_i, decay_param, w_out,
    gain_mlp, w_gate, w_up, w_down, cotangent,
):
    rows, width = tokens_in.shape
    heads, local = w_x.shape[1:]
    n_ten, n_seq = lax.axis_size("tensor"), lax.axis_size("seq")
    devices = n_ten * n_seq
    place, run = lax.axis_index("tensor"), lax.axis_index("seq")
    linear = run * n_ten + place
    length = devices * rows // SEQS
    base = jnp.reshape((linear * rows) % length, (1,)).astype(jnp.int32)
    join = 128 // local if local < 128 and heads % (128 // local) == 0 else 1
    groups, chunk = heads // join, join * local
    lanes = n_ten * chunk
    channels = groups * lanes

    def shape(dims, kind=F32):
        return jax.ShapeDtypeStruct(dims, kind)

    def own_columns(array):
        n = array.shape[0]
        split = array.reshape(n, groups, n_ten, chunk)
        return lax.dynamic_index_in_dim(split, place, 2, False).reshape(n, heads, local)

    gate_rows = jnp.stack([gate_a, gate_i], 0).swapaxes(2, 3).reshape(2 * heads, local, n_ten * local)
    params = jnp.concatenate([conv_w, decay_param[None]], 0).reshape(CONV + 1, heads * local)
    params = jnp.pad(params, ((0, 7 - CONV), (0, 0)))
    (all_gates, full_x, full_y, full_out), params, cots, halo = gather_all(
        [
            gate_rows,
            jnp.transpose(w_x, (1, 2, 0)).reshape(groups, chunk, width),
            jnp.transpose(w_y, (1, 2, 0)).reshape(groups, chunk, width),
            w_out.reshape(groups, chunk, width),
        ],
        params, cotangent, tokens_in, HALO,
    )
    halo = jnp.where(linear == 0, jnp.zeros_like(halo), halo)
    full_x, full_y, full_out = (w.reshape(channels, width) for w in (full_x, full_y, full_out))
    gates = all_gates.reshape(2, groups, join, n_ten, local, n_ten * local)
    gates = jnp.transpose(gates, (1, 0, 3, 2, 4, 5)).reshape(groups, 2 * lanes, n_ten * local)
    key = jnp.arange(n_ten * local)[None, :, None]
    lane = jnp.arange(lanes)[None, None, :]
    member = jnp.arange(join)[:, None, None]
    select = (
        (lane // chunk == key // local) & (lane % local == key % local) & (lane // local % join == member)
    ).astype(BF16)
    params = jnp.transpose(params.reshape(n_ten, 8, groups, chunk), (1, 2, 0, 3)).reshape(8, channels)
    conv_rows, decay_full = params, params[CONV : CONV + 1]
    rate_gain = -8.0 * jax.nn.softplus(decay_full)

    own_in = tokens_in.astype(F32)
    in_scale, in_unit = rms_parts(own_in)
    normed = (in_unit * gain_pre).astype(BF16)
    normed_halo = (rms_parts(halo.astype(F32))[1] * gain_pre).astype(BF16)
    x_long = dot_nt(jnp.concatenate([normed_halo, normed], 0), full_x).astype(BF16)
    y_branch = dot_nt(normed, full_y)
    scratch = [pltpu.VMEM((lanes // 128, rows, 128), F32)] * 2
    conv_out, rate_pre, input_pre, products, partial, carry, wide_gates = lane_call(
        functools.partial(forward_kernel, length, local), groups, lanes, base,
        (x_long, conv_rows, rate_gain, gates, select),
        [
            shape((rows, channels), BF16),
            shape((rows, channels)),
            shape((rows, channels)),
            shape((rows, channels)),
            shape((rows, channels)),
            shape((2, channels)),
            shape((groups, 2 * lanes, lanes), BF16),
        ],
        scratch, 4 * rows * lanes * channels,
    )
    reach = min(-(-length // rows), devices - 1)
    enter = entering(carry, reach, linear, devices, False)
    states = partial + products * enter
    mixed = (states * jax.nn.gelu(y_branch, approximate=True)).astype(BF16)
    middle = own_in + dot_nn(mixed, full_out)
    mid_scale, mid_unit = rms_parts(middle)
    normed_mlp = (mid_unit * gain_mlp).astype(BF16)

    if n_ten == 4 and n_seq == 8:
        *kept, mlp_input, downs = feed_forward(normed_mlp, cots, w_gate, w_up, w_down)
        cot_rows = cots.reshape(n_ten * rows, width)
        token_rows, hidden_rows, gate_rows, up_rows = (
            a.reshape(n_ten * rows, a.shape[2]) for a in kept
        )
    else:
        cots = [cotangent] + [
            lax.dynamic_index_in_dim(cots, label_index(k), 0, False) for k in range(1, n_ten)
        ]
        tokens = [normed_mlp] + others(normed_mlp)
        hiddens, gate_grads, up_grads, downs, pulls = [], [], [], [], []
        for n, c in zip(tokens, cots):
            gate_vals, up_vals = dot_nn(n, w_gate), dot_nn(n, w_up)
            value, slope = gelu_both(gate_vals)
            hidden = (value * up_vals).astype(BF16)
            hidden_grad = dot_nt(c, w_down)
            gate_grad = (hidden_grad * up_vals * slope).astype(BF16)
            up_grad = (hidden_grad * value).astype(BF16)
            hiddens.append(hidden)
            gate_grads.append(gate_grad)
            up_grads.append(up_grad)
            pulls.append(dot_nt(gate_grad, w_gate) + dot_nt(up_grad, w_up))
            downs.append(dot_nn(hidden, w_down).astype(BF16))
        mlp_input = line_sum(pulls[0], [p.astype(BF16) for p in pulls[1:]])
        cot_rows, token_rows, hidden_rows, gate_rows, up_rows = (
            jnp.concatenate(a, 0) for a in (cots, tokens, hiddens, gate_grads, up_grads)
        )
    grad_down = dot_tn(cot_rows, hidden_rows).astype(BF16)
    grad_gate = dot_tn(token_rows, gate_rows).astype(BF16)
    grad_up = dot_tn(token_rows, up_rows).astype(BF16)
    gain_mlp_part, mid_back = rms_back(mlp_input, gain_mlp, mid_scale, mid_unit)
    middle_grad = cotangent.astype(F32) + mid_back
    middle_low, *_ = lax.optimization_barrier(
        (middle_grad.astype(BF16), grad_down, grad_gate, grad_up)
    )
    grad_down, grad_gate, grad_up = (
        lax.psum_scatter(g, "seq", scatter_dimension=0, tiled=True)
        for g in (grad_down, grad_gate, grad_up)
    )
    mixed_grad = dot_nt(middle_low, full_out)
    y_low, back_products, back_partial, carry = lane_call(
        functools.partial(middle_kernel, length), groups, lanes, base,
        (mixed_grad, y_branch, products, partial, enter, rate_pre, rate_gain),
        [
            shape((rows, channels), BF16),
            shape((rows, channels)),
            shape((rows, channels)),
            shape((2, channels)),
        ],
        scratch, 60 * rows * channels,
    )
    leave = entering(carry, reach, linear, devices, True)
    part = n_ten * local // n_seq
    gate_parts, x_back, edge, sums = lane_call(
        functools.partial(backward_kernel, length, local), groups, lanes, base,
        (
            back_products, back_partial, leave, products, partial, enter, rate_pre, input_pre,
            conv_out, rate_gain, wide_gates, conv_rows, x_long, select,
        ),
        [
            shape((n_seq, n_ten, groups, 2, part, chunk), BF16),
            shape((rows, channels)),
            shape((HALO, channels)),
            shape((8, channels)),
        ],
        [], 8 * rows * lanes * channels,
    )
    edge = lax.ppermute(edge, BOTH, [(i + 1, i) for i in range(devices - 1)])
    x_low = jnp.concatenate(
        [x_back[: rows - HALO], x_back[rows - HALO :] + edge], 0
    ).astype(BF16)

    normed_grad = dot_nn(x_low, full_x) + dot_nn(y_low, full_y)
    gain_pre_part, in_back = rms_back(normed_grad, gain_pre, in_scale, in_unit)
    input_grad = middle_grad + in_back

    split = gate_parts.reshape(devices, groups * 2 * part, chunk)
    packed = jnp.concatenate(
        [sums[: CONV + 1], gain_pre_part[None], gain_mlp_part[None], sums[CONV + 3 :]], 0
    )
    (grad_out, grad_y, grad_x), down, gate_sum, packed = weight_grads(
        (0, 1, 1), [middle_low, normed], [mixed, y_low, x_low], groups, downs, split, packed
    )
    block_out = (middle + down).astype(BF16)
    gate_sum = gate_sum.reshape(groups, 2, part, join, local)
    gate_sum = jnp.transpose(gate_sum, (1, 0, 3, 2, 4)).reshape(2, heads, part, local)
    conv_sum = own_columns(packed[:CONV])
    decay_sum = own_columns(packed[CONV : CONV + 1] * (-8.0 * jax.nn.sigmoid(decay_full)))[0]
    share = local // n_seq
    grad_conv = lax.dynamic_slice_in_dim(conv_sum, run * share, share, 2)
    grad_decay = lax.dynamic_slice_in_dim(decay_sum, run * share, share, 1)
    grad_gain_mlp = lax.dynamic_slice_in_dim(
        packed[CONV + 2], run * (width // n_seq), width // n_seq, 0
    )

    def weight(grad):
        return grad.T.reshape(heads, local, -1)

    return (
        block_out,
        input_grad,
        packed[CONV + 1],
        jnp.transpose(weight(grad_x), (2, 0, 1)),
        jnp.transpose(weight(grad_y), (2, 0, 1)),
        grad_conv,
        gate_sum[0],
        gate_sum[1],
        grad_decay,
        weight(grad_out),
        grad_gain_mlp,
        grad_gate.astype(F32),
        grad_up.astype(F32),
        grad_down.astype(F32).T,
    )


def solution(mesh):
    placed = (
        P(("seq", "tensor"), None),
        P(),
        P(None, None, "tensor"),
        P(None, None, "tensor"),
        P(None, None, "tensor"),
        P(None, None, "tensor"),
        P(None, None, "tensor"),
        P(None, "tensor"),
        P(None, "tensor", None),
        P(),
        P(None, "tensor"),
        P(None, "tensor"),
        P("tensor", None),
        P(("seq", "tensor"), None),
    )
    return jax.shard_map(
        shards,
        mesh=mesh,
        in_specs=placed,
        out_specs=(
            P(("seq", "tensor"), None),
            P(("seq", "tensor"), None),
            P(),
            P("seq", None, "tensor"),
            P("seq", None, "tensor"),
            P(None, None, ("tensor", "seq")),
            P(None, "seq", "tensor"),
            P(None, "seq", "tensor"),
            P(None, ("tensor", "seq")),
            P(None, "tensor", "seq"),
            P("seq"),
            P("seq", "tensor"),
            P("seq", "tensor"),
            P("tensor", "seq"),
        ),
        check_vma=False,
    )
```

```python
import functools
import math

import jax
import jax.numpy as jnp
from jax import lax
from jax.experimental import pallas as pl
from jax.experimental.pallas import tpu as pltpu
from jax.sharding import PartitionSpec as P

CONV = 4
SEQS = 3
HALO = 16
epsilon = 1e-06
F32 = jnp.float32
BF16 = jnp.bfloat16
ROOT = math.sqrt(2.0 / math.pi)
BOTH = ("seq", "tensor")


def dot_nn(a, b):
    return lax.dot_general(a, b, (((1,), (0,)), ((), ())), preferred_element_type=F32)


def dot_nt(a, b):
    return lax.dot_general(a, b, (((1,), (1,)), ((), ())), preferred_element_type=F32)


def dot_tn(a, b):
    return lax.dot_general(a, b, (((0,), (0,)), ((), ())), preferred_element_type=F32)


def rms_parts(values):
    scale = lax.rsqrt(jnp.mean(values * values, axis=-1, keepdims=True) + epsilon)
    return scale, values * scale


def rms_back(grad, gain, scale, unit):
    pulled = gain * grad
    inner = jnp.mean(pulled * unit, axis=-1, keepdims=True)
    return jnp.sum(grad * unit, axis=0), scale * (pulled - unit * inner)


def gelu_both(v):
    inner = v * v
    th = jnp.tanh(ROOT * (v + 0.044715 * v * inner))
    half = 0.5 * (1.0 + th)
    slope = half + 0.5 * v * (1.0 - th * th) * (ROOT * (1.0 + 3 * 0.044715 * inner))
    return v * half, slope


LABELS = ((1, 2, 3, 2), (2, 0, 1, 1), (3, 3, 0, 0))


def along(block, pairs):
    return lax.ppermute(block, "tensor", pairs)


def line_streams(own):
    right, left = [], []
    right.append(along(own, [(0, 1), (1, 2), (2, 3)]))
    left.append(along(own, [(1, 0), (2, 1), (3, 2)]))
    right.append(along(right[0], [(1, 2), (2, 3)]))
    left.append(along(left[0], [(1, 0), (2, 1)]))
    right.append(along(right[1], [(2, 3)]))
    left.append(along(left[1], [(1, 0)]))
    return right, left


def others(own):
    count = lax.axis_size("tensor")
    place = lax.axis_index("tensor")
    if count == 4:
        right, left = line_streams(own)
        first = jnp.where(place == 3, right[0], left[0])
        second = jnp.where(place == 0, left[1], jnp.where(place == 3, right[1], right[0]))
        third = jnp.where(
            place == 0, left[2], jnp.where(place == 1, left[1], jnp.where(place == 2, right[1], right[2]))
        )
        return [first, second, third]
    whole = lax.all_gather(own, "tensor", axis=0)
    return [lax.dynamic_index_in_dim(whole, (place + k) % count, 0, False) for k in range(1, count)]


def label_index(k):
    count = lax.axis_size("tensor")
    place = lax.axis_index("tensor")
    if count == 4:
        table = LABELS[k - 1]
        return jnp.where(
            place == 0, table[0], jnp.where(place == 1, table[1], jnp.where(place == 2, table[2], table[3]))
        )
    return (place + k) % count


def in_order(own):
    count = lax.axis_size("tensor")
    place = lax.axis_index("tensor")
    if count == 4:
        right, left = line_streams(own)
        rows = []
        for want in range(4):
            pick = own
            for at in range(4):
                if at < want:
                    pick = jnp.where(place == at, left[want - at - 1], pick)
                elif at > want:
                    pick = jnp.where(place == at, right[at - want - 1], pick)
            rows.append(pick)
        return jnp.stack(rows, 0)
    return lax.all_gather(own, "tensor", axis=0)


def line_sum(own, parts):
    count = lax.axis_size("tensor")
    place = lax.axis_index("tensor")
    if count == 4:
        first, second, third = parts
        end = (place == 0) | (place == 3)
        right = along(third, [(0, 1)])
        left = along(third, [(3, 2)])
        arrived = jnp.where(place == 1, right, left)
        send = jnp.where(
            end, second, (third.astype(F32) + arrived.astype(F32)).astype(BF16)
        )
        right = along(send, [(0, 1), (1, 2)])
        left = along(send, [(3, 2), (2, 1)])
        send_right = (first.astype(F32) + right.astype(F32)).astype(BF16)
        send_left = (
            jnp.where(place == 3, first, second).astype(F32) + left.astype(F32)
        ).astype(BF16)
        right = along(send_right, [(0, 1), (1, 2), (2, 3)])
        left = along(send_left, [(3, 2), (2, 1), (1, 0)])
        return own.astype(F32) + right.astype(F32) + left.astype(F32)
    stack = jnp.zeros((count,) + own.shape, BF16)
    stack = lax.dynamic_update_index_in_dim(stack, own.astype(BF16), place, 0)
    for k in range(1, count):
        stack = lax.dynamic_update_index_in_dim(stack, parts[k - 1], label_index(k), 0)
    return lax.psum_scatter(stack, "tensor", scatter_dimension=0, tiled=False).astype(F32)


MESH = pl.DeviceIdType.MESH


def ring_places():
    s, t = lax.axis_index("seq"), lax.axis_index("tensor")
    c, x, y = s % 2, (s // 2) % 2, s // 4
    return s, t, c, x, y


def greet(targets):
    barrier = pltpu.get_barrier_semaphore()
    for target in targets:
        pl.semaphore_signal(barrier, inc=1, device_id=target, device_id_type=MESH)
    pl.semaphore_wait(barrier, len(targets))


def gather_kernel(count, *refs):
    weights, (small, cot, tokens) = refs[:count], refs[count : count + 3]
    full = refs[count + 3 : 2 * count + 3]
    smalls, cots, halo = refs[2 * count + 3 : 2 * count + 6]
    rest = refs[2 * count + 6 :]
    stage, rest = rest[: count + 2], rest[count + 2 :]
    local_sem, send_sem, recv_sem, line_send, line_recv, halo_sem = rest
    s, t, c, x, y = ring_places()
    s_core, s_x, s_y = s + 1 - 2 * c, s + 2 - 4 * x, s + 4 - 8 * y
    s_far = s_x + 4 - 8 * y
    right, left = (s, t + 1), (s, t - 1)
    near_x, near_y, core = (s_x, t), (s_y, t), (s_core, t)
    linear = 4 * s + t
    after, before = (linear + 1) % 32, (linear + 31) % 32
    greet(
        [(s, (t + 1) % 4), (s, (t + 3) % 4), near_x, near_y, core, (before // 4, before % 4)]
    )
    sent = []
    tail_rows = halo.shape[0]
    onward = pltpu.make_async_remote_copy(
        src_ref=tokens.at[pl.ds(tokens.shape[0] - tail_rows, tail_rows)], dst_ref=halo,
        send_sem=halo_sem.at[0], recv_sem=halo_sem.at[1],
        device_id=(after // 4, after % 4), device_id_type=MESH,
    )
    pl.when(linear < 31)(onward.start)

    def slot(w, tt, ss):
        return full[w].at[:, tt, ss]

    def copy(w, src, tt, ss, kind, target):
        return pltpu.make_async_remote_copy(
            src_ref=src, dst_ref=slot(w, tt, ss), send_sem=send_sem.at[w, tt, kind],
            recv_sem=recv_sem.at[w, tt, ss], device_id=target, device_id_type=MESH,
        )

    def arrived(w, tt, ss):
        copy(w, slot(w, tt, ss), tt, ss, 0, core).wait_recv()

    def send(w, src, tt, ss, kind, target, when=None):
        def go():
            copy(w, src, tt, ss, kind, target).start()

        def done():
            copy(w, src, tt, ss, kind, target).wait_send()

        if when is None:
            go()
            sent.append(done)
        else:
            pl.when(when)(go)
            sent.append(lambda: pl.when(when)(done))

    def spread(w, src, tt):
        send(w, src, tt, s, 2, near_x)
        send(w, src, tt, s, 3, near_y)
        send(w, src, tt, s, 4, core)

    def open_line(w):
        own = weights[w].at[:, s]
        send(w, own, t, s, 0, right, t < 3)
        send(w, own, t, s, 1, left, t > 0)
        spread(w, own, t)

    def line_events(w):
        for k in (1, 2, 3):
            for way in (-1, 1):
                tt = t + way * k

                def event(tt=tt, way=way, tail=sent):
                    arrived(w, tt, s)
                    if way < 0:
                        pl.when(t < 3)(lambda: copy(w, slot(w, tt, s), tt, s, 0, right).start())
                    else:
                        pl.when(t > 0)(lambda: copy(w, slot(w, tt, s), tt, s, 1, left).start())
                    copy(w, slot(w, tt, s), tt, s, 2, near_x).start()
                    copy(w, slot(w, tt, s), tt, s, 3, near_y).start()
                    copy(w, slot(w, tt, s), tt, s, 4, core).start()

                def finish(tt=tt, way=way):
                    if way < 0:
                        pl.when(t < 3)(lambda: copy(w, slot(w, tt, s), tt, s, 0, right).wait_send())
                    else:
                        pl.when(t > 0)(lambda: copy(w, slot(w, tt, s), tt, s, 1, left).wait_send())
                    for kind, target in ((2, near_x), (3, near_y), (4, core)):
                        copy(w, slot(w, tt, s), tt, s, kind, target).wait_send()

                ok = tt >= 0 if way < 0 else tt <= 3
                pl.when(ok)(event)
                sent.append(lambda ok=ok, finish=finish: pl.when(ok)(finish))

    def plane_events(w):
        for tt in range(4):
            arrived(w, tt, s_x)
            send(w, slot(w, tt, s_x), tt, s_x, 6, core)
            if tt % 2 == 0:
                send(w, slot(w, tt, s_x), tt, s_x, 5, near_y)
            arrived(w, tt, s_y)
            send(w, slot(w, tt, s_y), tt, s_y, 8, core)
            if tt % 2 == 1:
                send(w, slot(w, tt, s_y), tt, s_y, 7, near_x)

    def far_events(w):
        for tt in range(4):
            arrived(w, tt, s_far)
            send(w, slot(w, tt, s_far), tt, s_far, 9, core)

    def core_events(w):
        for tt in range(4):
            for base in (s, s_x, s_y, s_far):
                arrived(w, tt, base + 1 - 2 * c)

    lines = ((small, smalls), (cot, cots))

    def line_copy(v, src, tt, kind, target):
        return pltpu.make_async_remote_copy(
            src_ref=src, dst_ref=lines[v][1].at[tt], send_sem=line_send.at[v, tt, kind],
            recv_sem=line_recv.at[v, tt], device_id=target, device_id_type=MESH,
        )

    def open_other(v):
        own = lines[v][0]
        pl.when(t < 3)(lambda: line_copy(v, own, t, 0, right).start())
        pl.when(t > 0)(lambda: line_copy(v, own, t, 1, left).start())
        sent.append(lambda: pl.when(t < 3)(lambda: line_copy(v, own, t, 0, right).wait_send()))
        sent.append(lambda: pl.when(t > 0)(lambda: line_copy(v, own, t, 1, left).wait_send()))

    def other_events(v, k):
        whole = lines[v][1]
        for way in (-1, 1):
            tt = t + way * k
            kind, target = (0, right) if way < 0 else (1, left)
            more = t < 3 if way < 0 else t > 0

            def event(tt=tt, kind=kind, target=target, more=more):
                line_copy(v, whole.at[tt], tt, kind, target).wait_recv()
                pl.when(more)(lambda: line_copy(v, whole.at[tt], tt, kind, target).start())

            def finish(tt=tt, kind=kind, target=target, more=more):
                pl.when(more)(lambda: line_copy(v, whole.at[tt], tt, kind, target).wait_send())

            ok = tt >= 0 if way < 0 else tt <= 3
            pl.when(ok)(event)
            sent.append(lambda ok=ok, finish=finish: pl.when(ok)(finish))

    into = [pltpu.make_async_copy(weights[w].at[:, s], stage[w], local_sem.at[w]) for w in range(count)]
    out = [pltpu.make_async_copy(stage[w], slot(w, t, s), local_sem.at[w]) for w in range(count)]
    for v, (own, whole) in enumerate(lines):
        into.append(pltpu.make_async_copy(own, stage[count + v], local_sem.at[count + v]))
        out.append(pltpu.make_async_copy(stage[count + v], whole.at[t], local_sem.at[count + v]))

    open_other(0)
    for w in range(count):
        open_line(w)
    for move in into:
        move.start()
    line_events(0)
    line_events(1)
    for a, b in zip(into, out):
        a.wait()
        b.start()
    open_other(1)
    plane_events(0)
    line_events(2)
    far_events(0)
    plane_events(1)
    line_events(3)
    far_events(1)
    other_events(1, 1)
    plane_events(2)
    far_events(2)
    other_events(1, 2)
    plane_events(3)
    for k in (1, 2, 3):
        other_events(0, k)
    other_events(1, 3)
    far_events(3)
    for w in range(count):
        core_events(w)
    for move in out:
        move.wait()
    for done in sent:
        done()
    pl.when(linear > 0)(onward.wait_recv)
    pl.when(linear < 31)(onward.wait_send)


def gather_all(weights, small, cotangent, tokens, tail_rows):
    n_ten, n_seq = lax.axis_size("tensor"), lax.axis_size("seq")
    if not (n_ten == 4 and n_seq == 8):
        full = [jnp.moveaxis(lax.all_gather(w, "tensor", axis=0), 0, 1) for w in weights]
        devices = n_ten * n_seq
        halo = lax.ppermute(
            tokens[tokens.shape[0] - tail_rows :], BOTH, [(i, i + 1) for i in range(devices - 1)]
        )
        whole = (lax.all_gather(a, "tensor", axis=0) for a in (small, cotangent))
        return full, *whole, halo
    count = len(weights)
    cut = [w.reshape(w.shape[0], 8, w.shape[1] // 8, w.shape[2]) for w in weights]
    anywhere = pl.BlockSpec(memory_space=pl.ANY)
    outs = [jax.ShapeDtypeStruct((w.shape[0], 4) + w.shape[1:], w.dtype) for w in cut]
    outs += [jax.ShapeDtypeStruct((4,) + a.shape, a.dtype) for a in (small, cotangent)]
    outs.append(jax.ShapeDtypeStruct((tail_rows, tokens.shape[1]), tokens.dtype))
    dma = pltpu.SemaphoreType.DMA
    got = pl.pallas_call(
        functools.partial(gather_kernel, count),
        out_shape=outs,
        in_specs=[anywhere] * (count + 3),
        out_specs=[anywhere] * (count + 3),
        scratch_shapes=[pltpu.VMEM((w.shape[0],) + w.shape[2:], w.dtype) for w in cut]
        + [pltpu.VMEM(a.shape, a.dtype) for a in (small, cotangent)]
        + [
            dma((count + 2,)), dma((count, 4, 10)), dma((count, 4, 8)),
            dma((2, 4, 2)), dma((2, 4)), dma((2,)),
        ],
        compiler_params=pltpu.CompilerParams(collective_id=1, has_side_effects=True),
        name="gather",
    )(*cut, small, cotangent, tokens)
    full = [g.reshape(w.shape[0], 4, w.shape[1], w.shape[2]) for g, w in zip(got, weights)]
    return full, *got[count:]


def carry_kernel(reach, reverse, carry_ref, out_ref, send_sem, recv_sem):
    n_ten = lax.axis_size("tensor")
    devices = n_ten * lax.axis_size("seq")
    me = lax.axis_index("seq") * n_ten + lax.axis_index("tensor")
    way = -1 if reverse else 1

    def place(linear):
        return linear // n_ten, linear % n_ten

    greet([place((me - way * k + devices) % devices) for k in range(1, reach + 1)])

    def copy(k):
        return pltpu.make_async_remote_copy(
            src_ref=carry_ref, dst_ref=out_ref.at[k - 1], send_sem=send_sem.at[k - 1],
            recv_sem=recv_sem.at[k - 1], device_id=place((me + way * k + devices) % devices),
            device_id_type=MESH,
        )

    def there(k, back):
        spot = me - way * k if back else me + way * k
        return (spot >= 0) & (spot < devices)

    for k in range(1, reach + 1):
        pl.when(there(k, False))(lambda k=k: copy(k).start())
    for k in range(1, reach + 1):
        pl.when(there(k, True))(lambda k=k: copy(k).wait_recv())
        pl.when(there(k, False))(lambda k=k: copy(k).wait_send())


def entering(carry, reach, linear, devices, reverse):
    channels = carry.shape[1]
    vmem = pl.BlockSpec(memory_space=pltpu.VMEM)
    got = pl.pallas_call(
        functools.partial(carry_kernel, reach, reverse),
        out_shape=jax.ShapeDtypeStruct((reach, 2, channels), F32),
        in_specs=[vmem],
        out_specs=vmem,
        scratch_shapes=[pltpu.SemaphoreType.DMA((reach,)), pltpu.SemaphoreType.DMA((reach,))],
        compiler_params=pltpu.CompilerParams(
            collective_id=3 if reverse else 2, has_side_effects=True
        ),
        name="carry_back" if reverse else "carry",
    )(carry)
    state = jnp.zeros((1, channels), F32)
    for k in range(reach, 0, -1):
        source = linear + k if reverse else linear - k
        there = (source >= 0) & (source < devices)
        state = jnp.where(there, got[k - 1, 0:1] * state + got[k - 1, 1:2], state)
    return state


def pick4(t, a, b, c, d):
    return jnp.where(t == 0, a, jnp.where(t == 1, b, jnp.where(t == 2, c, d)))


def tail_kernel(lefts, rows, groups, chunk, share, *refs):
    n_a, n_b = max(lefts) + 1, len(lefts)
    a_refs, b_refs = refs[:n_a], refs[n_a : n_a + n_b]
    down_ref, gates_ref, small_ref, out_ref, land_ref, gates_out, small_out = refs[
        n_a + n_b : n_a + n_b + 7
    ]
    (
        a_all, b_all, product, to_x, to_y, to_far, far_x, far_y, from_x, from_y, total, turned,
        line_send, line_recv, fill_sem, out_sem, pair_send, pair_recv,
        send_sem, recv_sem, zs_sem, zr_sem,
        down_send, down_recv,
        g_core, g_own, g_far, g_from, g_line, g_total, g_load, g_send, g_recv,
        acc, got, line, small_total, s_load, s_send, s_recv,
    ) = refs[n_a + n_b + 7 :]
    cols = groups * chunk
    s, t = lax.axis_index("seq"), lax.axis_index("tensor")
    c, x, y = s % 2, (s // 2) % 2, s // 4
    p = s // 2
    p_x, p_y = p + 1 - 2 * x, p + 2 - 4 * y
    p_far = p_x + 2 - 4 * y
    near_x, near_y, core = (s + 2 - 4 * x, t), (s + 4 - 8 * y, t), (s + 1 - 2 * c, t)
    right, left = (s, t + 1), (s, t - 1)
    greet([(s, (t + k) % 4) for k in (1, 2, 3)] + [near_x, near_y, core])
    half = share // 2
    steps = 4 * n_b

    def pass_down(label):
        third, second, first = pick4(t, 3, 3, 0, 0), pick4(t, 2, 0, 1, 1), pick4(t, 1, 2, 3, 2)
        target = (first, second, third)[label]
        return pltpu.make_async_remote_copy(
            src_ref=down_ref.at[label + 1], dst_ref=land_ref.at[t], send_sem=down_send.at[label],
            recv_sem=down_recv.at[t], device_id=(s, target), device_id_type=MESH,
        )

    def down_here(tt):
        return pltpu.make_async_remote_copy(
            src_ref=down_ref.at[0], dst_ref=land_ref.at[tt], send_sem=down_send.at[0],
            recv_sem=down_recv.at[tt], device_id=core, device_id_type=MESH,
        )

    def g_copy(k, src, dst, target):
        return pltpu.make_async_remote_copy(
            src_ref=src, dst_ref=dst, send_sem=g_send.at[k], recv_sem=g_recv.at[k],
            device_id=target, device_id_type=MESH,
        )

    g_pair = g_copy(0, gates_ref.at[:, 1 - c], g_core, core)
    g_fill = pltpu.make_async_copy(gates_ref.at[:, c], g_own, g_load.at[0])
    g_fars = (
        g_copy(1, g_own.at[p_far, pl.ds(0, 2)], g_far.at[0], near_x),
        g_copy(2, g_own.at[p_far, pl.ds(2, 2)], g_far.at[1], near_y),
    )
    g_nears = (
        g_copy(3, g_own.at[p_x], g_from.at[0], near_x),
        g_copy(4, g_own.at[p_y], g_from.at[1], near_y),
    )

    def g_hop(k, back):
        other = (t - k + 4) % 4 if back else (t + k) % 4
        return pltpu.make_async_remote_copy(
            src_ref=g_own.at[p, other], dst_ref=g_line.at[other if back else t],
            send_sem=g_send.at[4 + k], recv_sem=g_recv.at[4 + k],
            device_id=(s, other), device_id_type=MESH,
        )

    g_store = pltpu.make_async_copy(g_total, gates_out, g_load.at[1])

    def s_copy(k, target):
        return pltpu.make_async_remote_copy(
            src_ref=acc.at[k], dst_ref=got.at[k], send_sem=s_send.at[k], recv_sem=s_recv.at[k],
            device_id=target, device_id_type=MESH,
        )

    s_turns = (s_copy(0, core), s_copy(1, near_x), s_copy(2, near_y))

    def s_hop(k, back):
        other = (t - k + 4) % 4 if back else (t + k) % 4
        return pltpu.make_async_remote_copy(
            src_ref=acc.at[3], dst_ref=line.at[other if back else t],
            send_sem=s_send.at[2 + k], recv_sem=s_recv.at[2 + k],
            device_id=(s, other), device_id_type=MESH,
        )

    s_fill = pltpu.make_async_copy(small_ref, acc.at[0], s_load.at[0])
    s_store = pltpu.make_async_copy(small_total, small_out, s_load.at[1])

    def small_steps(n):
        @pl.when(n == 0)
        def _():
            s_fill.wait()
            s_turns[0].start()

        @pl.when(n == 1)
        def _():
            s_turns[0].wait_recv()
            acc[1] = acc[0] + got[0]
            s_turns[1].start()
            g_fill.wait()
            g_pair.wait_recv()
            for q in range(4):
                g_own[q] = (g_own[q].astype(F32) + g_core[q].astype(F32)).astype(BF16)
            for move in g_fars:
                move.start()

        @pl.when(n == 2)
        def _():
            s_turns[1].wait_recv()
            acc[2] = acc[1] + got[1]
            s_turns[2].start()
            for move in g_fars:
                move.wait_recv()
            g_own[p_y, pl.ds(0, 2)] = (
                g_own[p_y, pl.ds(0, 2)].astype(F32) + g_far[0].astype(F32)
            ).astype(BF16)
            g_own[p_x, pl.ds(2, 2)] = (
                g_own[p_x, pl.ds(2, 2)].astype(F32) + g_far[1].astype(F32)
            ).astype(BF16)
            for move in g_nears:
                move.start()

        @pl.when(n == 3)
        def _():
            s_turns[2].wait_recv()
            acc[3] = acc[2] + got[2]
            line[t] = acc[3]
            for move in g_nears:
                move.wait_recv()
            g_own[p] = (
                g_own[p].astype(F32) + g_from[0].astype(F32) + g_from[1].astype(F32)
            ).astype(BF16)
            g_line[t] = g_own[p, t]
            for k in (1, 2, 3):
                s_hop(k, False).start()
                g_hop(k, False).start()

        @pl.when(n == 6)
        def _():
            for k in (1, 2, 3):
                s_hop(k, True).wait_recv()
                g_hop(k, True).wait_recv()
            small_total[...] = line[0] + line[1] + line[2] + line[3]
            g_total[...] = (
                g_line[0].astype(F32) + g_line[1].astype(F32)
                + g_line[2].astype(F32) + g_line[3].astype(F32)
            )
            s_store.start()
            g_store.start()

    s_fill.start()
    g_fill.start()
    g_pair.start()
    for label in (2, 1, 0):
        pass_down(label).start()

    def fill_b(w, k):
        tt, j = k // groups, k % groups
        return pltpu.make_async_copy(
            b_refs[w].at[:, pl.ds(pl.multiple_of((j * 4 + tt) * chunk, 128), chunk)],
            b_all.at[w, tt, pl.ds(0, rows), pl.ds(pl.multiple_of(j * chunk, 128), chunk)],
            fill_sem.at[n_a + w, k],
        )

    def fill_a(v):
        return pltpu.make_async_copy(a_refs[v], a_all.at[v, pl.ds(0, rows)], fill_sem.at[v, 0])

    def pair_a(v):
        return pltpu.make_async_remote_copy(
            src_ref=a_refs[v], dst_ref=a_all.at[v, pl.ds(rows, rows)],
            send_sem=pair_send.at[v, 0], recv_sem=pair_recv.at[v, 0],
            device_id=core, device_id_type=MESH,
        )

    def pair_b(w, k):
        return pltpu.make_async_remote_copy(
            src_ref=b_all.at[w, k, pl.ds(0, rows)], dst_ref=b_all.at[w, k, pl.ds(rows, rows)],
            send_sem=pair_send.at[n_a + w, k], recv_sem=pair_recv.at[n_a + w, k],
            device_id=core, device_id_type=MESH,
        )

    for w in range(n_b):
        if w == 0 or lefts[w] != lefts[w - 1]:
            pair_a(lefts[w]).start()
            fill_a(lefts[w]).start()

        @pl.loop(0, 4 * groups)
        def _(k, w=w):
            fill_b(w, k).start()

    for w in range(n_b):

        @pl.loop(0, 4 * groups)
        def _(k, w=w):
            fill_b(w, k).wait()

        @pl.loop(0, 4)
        def _(k, w=w):
            pair_b(w, k).start()

    for v in range(n_a):
        fill_a(v).wait()
        pair_a(v).wait_recv()

    def dest(n):
        i = n % 4
        third, second, first = pick4(t, 3, 3, 0, 0), pick4(t, 2, 0, 1, 1), pick4(t, 1, 2, 3, 2)
        return pick4(i, third, second, first, t)

    def make(n, q):
        w = n // 4
        start = pl.multiple_of(2 * share * q + (share - 64) * c, 128)
        v = sum(jnp.where(w >= k, lefts[k] - (lefts[k - 1] if k else 0), 0) for k in range(n_b))
        lhs = a_all[v, :, pl.ds(start, share + 64)]
        rhs = b_all[w, dest(n)]
        product[...] = lax.dot_general(lhs, rhs, (((0,), (0,)), ((), ())), preferred_element_type=F32)
        return product[pl.ds(pl.multiple_of(64 * c, 64), share), :]

    def remote(n, src, dst, k, target):
        return pltpu.make_async_remote_copy(
            src_ref=src, dst_ref=dst, send_sem=send_sem.at[n, k], recv_sem=recv_sem.at[n, k],
            device_id=target, device_id_type=MESH,
        )

    def directs(n):
        return (
            remote(n, to_far.at[n, pl.ds(0, half)], far_x.at[n], 0, near_x),
            remote(n, to_far.at[n, pl.ds(half, half)], far_y.at[n], 1, near_y),
            remote(n, to_x.at[n, pl.ds(0, half)], from_x.at[n, pl.ds(0, half)], 2, near_x),
            remote(n, to_y.at[n, pl.ds(half, half)], from_y.at[n, pl.ds(half, half)], 3, near_y),
        )

    def seconds(n):
        return (
            remote(n, to_x.at[n, pl.ds(half, half)], from_x.at[n, pl.ds(half, half)], 4, near_x),
            remote(n, to_y.at[n, pl.ds(0, half)], from_y.at[n, pl.ds(0, half)], 5, near_y),
        )

    def begin(n):
        pair_b(n // 4, dest(n)).wait_recv()
        to_far[n] = make(n, p_far).astype(BF16)
        directs(n)[0].start()
        directs(n)[1].start()
        to_x[n] = make(n, p_x).astype(BF16)
        directs(n)[2].start()
        to_y[n] = make(n, p_y).astype(BF16)
        directs(n)[3].start()

    def forward(n):
        first, second = directs(n)[:2]
        first.wait_recv()
        to_y[n, pl.ds(0, half)] = (
            to_y[n, pl.ds(0, half)].astype(F32) + far_x[n].astype(F32)
        ).astype(BF16)
        seconds(n)[1].start()
        second.wait_recv()
        to_x[n, pl.ds(half, half)] = (
            to_x[n, pl.ds(half, half)].astype(F32) + far_y[n].astype(F32)
        ).astype(BF16)
        seconds(n)[0].start()

    def hop(w, out, into, target):
        return pltpu.make_async_remote_copy(
            src_ref=line_send.at[w, out], dst_ref=line_recv.at[w, into],
            send_sem=zs_sem.at[w, out], recv_sem=zr_sem.at[w, into],
            device_id=target, device_id_type=MESH,
        )

    end = (t == 0) | (t == 3)

    def finish(n):
        w, i = n // 4, n % 4
        mine = make(n, p)
        for move in directs(n)[2:] + seconds(n):
            move.wait_recv()
        total[w] = mine + from_x[n].astype(F32) + from_y[n].astype(F32)

        @pl.when((i < 3) & end)
        def _():
            line_send[w, i] = total[w].astype(BF16)

        @pl.when((i == 0) & (t == 0))
        def _():
            hop(w, 0, 0, right).start()

        @pl.when((i == 0) & (t == 3))
        def _():
            hop(w, 0, 0, left).start()

        @pl.when((i == 1) & (t == 0))
        def _():
            hop(w, 1, 1, right).start()

        @pl.when((i == 1) & (t == 3))
        def _():
            hop(w, 1, 2, left).start()

        @pl.when((i == 2) & (t == 0))
        def _():
            hop(w, 2, 3, right).start()

        @pl.when((i == 2) & (t == 3))
        def _():
            hop(w, 2, 4, left).start()

        @pl.when((i == 0) & (t == 1))
        def _():
            hop(w, 0, 0, right).wait_recv()
            line_send[w, 0] = (total[w] + line_recv[w, 0].astype(F32)).astype(BF16)
            hop(w, 0, 1, right).start()

        @pl.when((i == 0) & (t == 2))
        def _():
            hop(w, 0, 0, left).wait_recv()
            line_send[w, 0] = (total[w] + line_recv[w, 0].astype(F32)).astype(BF16)
            hop(w, 0, 2, left).start()

        @pl.when((i == 1) & ~end)
        def _():
            hop(w, 1, 2, left).wait_recv()
            line_send[w, 1] = (total[w] + line_recv[w, 2].astype(F32)).astype(BF16)
            hop(w, 1, 4, left).start()

        @pl.when((i == 2) & ~end)
        def _():
            hop(w, 1, 1, right).wait_recv()
            line_send[w, 2] = (total[w] + line_recv[w, 1].astype(F32)).astype(BF16)
            hop(w, 2, 3, right).start()

    @pl.loop(0, steps + 3)
    def _(n):
        @pl.when(n < steps)
        def _():
            begin(n)

        @pl.when((n >= 1) & (n <= steps))
        def _():
            forward(n - 1)

        small_steps(n)

        @pl.when(n >= 3)
        def _():
            finish(n - 3)

    def result(w):
        return pltpu.make_async_copy(turned.at[w % 2], out_ref.at[w], out_sem.at[w])

    for w in range(n_b):

        @pl.when(t > 0)
        def _(w=w):
            hop(w, 2, 3, right).wait_recv()
            total[w] = total[w] + line_recv[w, 3].astype(F32)

        @pl.when(t < 3)
        def _(w=w):
            hop(w, 2, 4, left).wait_recv()
            total[w] = total[w] + line_recv[w, 4].astype(F32)

        if w >= 2:
            result(w - 2).wait()
        turned[w % 2] = total[w].T
        result(w).start()

    @pl.loop(0, steps)
    def _(n):
        for move in directs(n) + seconds(n):
            move.wait_send()

    for w in range(n_b):
        for k in range(3):
            hop(w, k, 0, right).wait_send()
        if w >= n_b - 2:
            result(w).wait()

        @pl.loop(0, 4)
        def _(k, w=w):
            pair_b(w, k).wait_send()

    for v in range(n_a):
        pair_a(v).wait_send()

    for label in range(3):
        pass_down(label).wait_send()
    for tt in range(4):
        pl.when(t != tt)(lambda tt=tt: down_here(tt).wait_recv())
    for move in (g_pair,) + g_fars + g_nears + s_turns:
        move.wait_send()
    for k in (1, 2, 3):
        s_hop(k, False).wait_send()
        g_hop(k, False).wait_send()
    s_store.wait()
    g_store.wait()


def weight_grads(lefts, a_list, b_list, groups, downs, blocks, small):
    n_ten, n_seq = lax.axis_size("tensor"), lax.axis_size("seq")
    rows, width = a_list[0].shape
    channels = b_list[0].shape[1]
    chunk = channels // groups // n_ten
    share = width // n_seq
    if not (n_ten == 4 and n_seq == 8):
        out = []
        for v, b in zip(lefts, b_list):
            b = jnp.swapaxes(b.reshape(rows, groups, n_ten, chunk), 1, 2).reshape(rows, channels)
            grad = dot_tn(a_list[v], b).astype(BF16)
            grad = lax.psum_scatter(grad, "seq", scatter_dimension=0, tiled=True)
            out.append(lax.psum_scatter(grad, "tensor", scatter_dimension=1, tiled=True).astype(F32).T)
        sums = lax.psum_scatter(blocks, BOTH, scatter_dimension=0, tiled=True)[0].astype(F32)
        return out, line_sum(downs[0], downs[1:]), sums, lax.psum(small, BOTH)
    count, cols = len(b_list), groups * chunk
    half, steps = share // 2, 4 * count
    anywhere = pl.BlockSpec(memory_space=pl.ANY)
    dma = pltpu.SemaphoreType.DMA

    def room(*dims):
        return pltpu.VMEM(dims, BF16)

    both = len(a_list) + count
    blocks = blocks.reshape((4, 2, 4) + blocks.shape[1:])
    piece = blocks.shape[3:]
    grads, land, block_sum, small_sum = pl.pallas_call(
        functools.partial(tail_kernel, lefts, rows, groups, chunk, share),
        out_shape=[
            jax.ShapeDtypeStruct((count, cols, share), F32),
            jax.ShapeDtypeStruct((4, rows, width), BF16),
            jax.ShapeDtypeStruct(piece, F32),
            jax.ShapeDtypeStruct(small.shape, F32),
        ],
        in_specs=[anywhere] * (both + 3),
        out_specs=[anywhere] * 4,
        scratch_shapes=[
            room(len(a_list), 2 * rows, width), room(count, 4, 2 * rows, cols),
            pltpu.VMEM((share + 64, cols), F32),
            room(steps, share, cols), room(steps, share, cols), room(steps, share, cols),
            room(steps, half, cols), room(steps, half, cols),
            room(steps, share, cols), room(steps, share, cols),
            pltpu.VMEM((count, share, cols), F32), pltpu.VMEM((2, cols, share), F32),
            room(count, 3, share, cols), room(count, 5, share, cols),
            dma((both, 4 * groups)), dma((count,)), dma((both, 4)), dma((both, 4)),
            dma((steps, 6)), dma((steps, 6)), dma((count, 3)), dma((count, 5)),
            dma((3,)), dma((4,)),
            room(4, 4, *piece), room(4, 4, *piece), room(2, 2, *piece), room(2, 4, *piece),
            room(4, *piece), pltpu.VMEM(piece, F32), dma((2,)), dma((8,)), dma((8,)),
            pltpu.VMEM((4,) + small.shape, F32), pltpu.VMEM((3,) + small.shape, F32),
            pltpu.VMEM((4,) + small.shape, F32), pltpu.VMEM(small.shape, F32),
            dma((2,)), dma((6,)), dma((6,)),
        ],
        compiler_params=pltpu.CompilerParams(
            collective_id=4, has_side_effects=True, vmem_limit_bytes=67043328
        ),
        cost_estimate=pl.CostEstimate(
            flops=2 * count * rows * width * channels, bytes_accessed=1 << 29, transcendentals=0
        ),
        name="tail",
    )(*a_list, *b_list, downs, blocks, small)
    place = lax.axis_index("tensor")
    down = downs[0].astype(F32)
    for k in range(4):
        down = down + jnp.where(place == k, 0.0, land[k].astype(F32))
    return grads, down, block_sum, small_sum


def feed_kernel(tiles, parts, own_ref, cots_ref, wg_ref, wu_ref, wd_ref, *refs):
    tokens_ref, hid_ref, gg_ref, ug_ref, sum_ref, down_ref = refs[:6]
    (
        wg, wu, wd, tok, cot, hid, gg, ug, part, land, total, down,
        load_sem, store_sem, sum_sem, ag_send, ag_recv, rs_send, rs_recv,
    ) = refs[6:]
    s, t = lax.axis_index("seq"), lax.axis_index("tensor")
    right, left = (s, t + 1), (s, t - 1)
    width, units = wg.shape
    span, cut = width // tiles, units // parts
    greet([(s, (t + 1) % 4), (s, (t + 3) % 4)])

    def pass_on(src, tt, kind):
        return pltpu.make_async_remote_copy(
            src_ref=src, dst_ref=tokens_ref.at[tt], send_sem=ag_send.at[tt, kind],
            recv_sem=ag_recv.at[tt], device_id=left if kind else right, device_id_type=MESH,
        )

    pl.when(t < 3)(lambda: pass_on(own_ref, t, 0).start())
    pl.when(t > 0)(lambda: pass_on(own_ref, t, 1).start())
    weights = [
        pltpu.make_async_copy(src, dst, load_sem.at[2 + k])
        for k, (src, dst) in enumerate(((wg_ref, wg), (wu_ref, wu), (wd_ref, wd)))
    ]
    for move in weights:
        move.start()

    def whose(i):
        third, second, first = pick4(t, 3, 3, 0, 0), pick4(t, 2, 0, 1, 1), pick4(t, 1, 2, 3, 2)
        return pick4(i, t, first, second, third)

    def stores(i):
        ch = whose(i)
        return [
            pltpu.make_async_copy(src, dst.at[ch], store_sem.at[k])
            for k, (src, dst) in enumerate(((hid, hid_ref), (gg, gg_ref), (ug, ug_ref)))
        ]

    def hop(label, k, way):
        return pltpu.make_async_remote_copy(
            src_ref=part.at[label, k], dst_ref=land.at[way, label, k],
            send_sem=rs_send.at[label, k], recv_sem=rs_recv.at[way, label, k],
            device_id=left if way else right, device_id_type=MESH,
        )

    def landed(label, k, way):
        hop(label, k, way).wait_recv()
        return land[way, label, k].astype(F32)

    def put_down(i):
        return pltpu.make_async_copy(down, down_ref.at[i], store_sem.at[4])

    def column(k, size):
        return pl.ds(pl.multiple_of(k * size, 128), size)

    def give(i, k, value):
        label = i - 1

        @pl.when(i == 0)
        def _():
            total[k] = value

        @pl.when((i > 0) & ((i < 3) | (t == 0) | (t == 3)))
        def _():
            part[label, k] = value.astype(BF16)

        @pl.when((i > 0) & (t == 0))
        def _():
            hop(label, k, 0).start()

        @pl.when((i > 0) & (t == 3))
        def _():
            hop(label, k, 1).start()

        @pl.when((i == 3) & (t == 1))
        def _():
            part[2, k] = (value + landed(2, k, 0)).astype(BF16)
            hop(2, k, 0).start()

        @pl.when((i == 3) & (t == 2))
        def _():
            part[2, k] = (value + landed(2, k, 1)).astype(BF16)
            hop(2, k, 1).start()

    @pl.loop(0, 4)
    def _(i):
        ch = whose(i)
        for way in (-1, 1):
            tt = t + way * i
            ok = (i > 0) & (tt >= 0) & (tt <= 3)

            @pl.when(ok)
            def _(tt=tt, way=way):
                pass_on(tokens_ref.at[tt], tt, 0).wait_recv()
                if way < 0:
                    pl.when(t < 3)(lambda: pass_on(tokens_ref.at[tt], tt, 0).start())
                else:
                    pl.when(t > 0)(lambda: pass_on(tokens_ref.at[tt], tt, 1).start())

        get_cot = pltpu.make_async_copy(cots_ref.at[ch], cot, load_sem.at[1])
        get_cot.start()

        @pl.when(i == 0)
        def _():
            move = pltpu.make_async_copy(own_ref, tok, load_sem.at[0])
            move.start()
            move.wait()
            pltpu.make_async_copy(tok, tokens_ref.at[t], store_sem.at[3]).start()
            for move in weights:
                move.wait()

        @pl.when(i == 1)
        def _():
            pltpu.make_async_copy(tok, tokens_ref.at[t], store_sem.at[3]).wait()

        @pl.when(i > 0)
        def _():
            move = pltpu.make_async_copy(tokens_ref.at[ch], tok, load_sem.at[0])
            move.start()
            move.wait()
            for store in stores(i - 1):
                store.wait()
            put_down(i - 1).wait()

        get_cot.wait()

        @pl.loop(0, parts)
        def _(f):
            here = column(f, cut)
            gate_vals = jnp.dot(tok[...], wg[:, here], preferred_element_type=F32)
            up_vals = jnp.dot(tok[...], wu[:, here], preferred_element_type=F32)
            back = lax.dot_general(
                cot[...], wd[here, :], (((1,), (1,)), ((), ())), preferred_element_type=F32
            )
            value, slope = gelu_both(gate_vals)
            hid[:, here] = (value * up_vals).astype(BF16)
            gg[:, here] = (back * up_vals * slope).astype(BF16)
            ug[:, here] = (back * value).astype(BF16)

        for store in stores(i):
            store.start()

        @pl.loop(0, tiles)
        def _(k):
            here = column(k, span)
            value = lax.dot_general(
                gg[...], wg[here, :], (((1,), (1,)), ((), ())), preferred_element_type=F32
            ) + lax.dot_general(
                ug[...], wu[here, :], (((1,), (1,)), ((), ())), preferred_element_type=F32
            )
            give(i, k, value)

        @pl.loop(0, tiles)
        def _(k):
            here = column(k, span)
            down[:, here] = jnp.dot(hid[...], wd[:, here], preferred_element_type=F32).astype(BF16)

        put_down(i).start()

    def add_and_send(k, label, arrived, way):
        part[label, k] = (part[label, k].astype(F32) + landed(arrived, k, way)).astype(BF16)
        hop(label, k, way).start()

    def add_total(k, label, way):
        total[k] = total[k] + landed(label, k, way)

    def put_sum(k):
        return pltpu.make_async_copy(total.at[k], sum_ref.at[:, column(k, span)], sum_sem.at[k])

    @pl.loop(0, tiles)
    def _(k):
        pl.when(t == 1)(lambda: add_and_send(k, 0, 1, 0))
        pl.when(t == 2)(lambda: add_and_send(k, 1, 1, 1))
        pl.when(t == 1)(lambda: add_and_send(k, 1, 2, 1))
        pl.when(t == 2)(lambda: add_and_send(k, 0, 2, 0))

    @pl.loop(0, tiles)
    def _(k):
        pl.when(t == 0)(lambda: add_total(k, 1, 1))
        pl.when(t > 0)(lambda: add_total(k, 0, 0))
        pl.when(t == 1)(lambda: add_total(k, 1, 1))
        pl.when(t == 2)(lambda: add_total(k, 0, 1))
        put_sum(k).start()

    @pl.loop(0, tiles)
    def _(k):
        put_sum(k).wait()
        for label in range(3):
            hop(label, k, 0).wait_send()

    put_down(3).wait()
    for store in stores(3):
        store.wait()
    pl.when(t < 3)(lambda: pass_on(own_ref, t, 0).wait_send())
    pl.when(t > 0)(lambda: pass_on(own_ref, t, 1).wait_send())
    for i in (1, 2, 3):
        pl.when((t - i >= 0) & (t < 3))(
            lambda i=i: pass_on(tokens_ref.at[t - i], t - i, 0).wait_send()
        )
        pl.when((t + i <= 3) & (t > 0))(
            lambda i=i: pass_on(tokens_ref.at[t + i], t + i, 1).wait_send()
        )


def feed_forward(own, cots, w_gate, w_up, w_down):
    rows, width = own.shape
    units = w_gate.shape[1]
    tiles, parts = width // 256, 5
    anywhere = pl.BlockSpec(memory_space=pl.ANY)
    dma = pltpu.SemaphoreType.DMA

    def room(*dims):
        return pltpu.VMEM(dims, BF16)

    def out(*dims, kind=BF16):
        return jax.ShapeDtypeStruct(dims, kind)

    flops = 2 * 4 * rows * width * units * 6
    got = pl.pallas_call(
        functools.partial(feed_kernel, tiles, parts),
        out_shape=[
            out(4, rows, width), out(4, rows, units), out(4, rows, units), out(4, rows, units),
            out(rows, width, kind=F32), out(4, rows, width),
        ],
        in_specs=[anywhere] * 5,
        out_specs=[anywhere] * 6,
        scratch_shapes=[
            room(width, units), room(width, units), room(units, width),
            room(rows, width), room(rows, width),
            room(rows, units), room(rows, units), room(rows, units),
            room(3, tiles, rows, width // tiles), room(2, 3, tiles, rows, width // tiles),
            pltpu.VMEM((tiles, rows, width // tiles), F32), room(rows, width),
            dma((5,)), dma((5,)), dma((tiles,)), dma((4, 2)), dma((4,)),
            dma((3, tiles)), dma((2, 3, tiles)),
        ],
        compiler_params=pltpu.CompilerParams(
            collective_id=5, has_side_effects=True, vmem_limit_bytes=67043328
        ),
        cost_estimate=pl.CostEstimate(flops=flops, bytes_accessed=3 << 27, transcendentals=0),
        name="feed",
    )(own, cots, w_gate, w_up, w_down)
    return got


def chunk_scan(a_ref, d_ref, p_ref, s_ref, reverse):
    tiles, rows, wide = a_ref.shape
    run = rows // 8

    def first(i, carry):
        r = run - 1 - i if reverse else i
        here = pl.ds(r, 8, stride=run)
        after = []
        for b in range(tiles):
            prod, state = carry[b]
            a = a_ref[b, here, :]
            prod = prod * a
            state = a * state + d_ref[b, here, :]
            a_ref[b, here, :] = prod
            d_ref[b, here, :] = state
            after.append((prod, state))
        return tuple(after)

    start = (jnp.ones((8, wide), F32), jnp.zeros((8, wide), F32))
    ends = lax.fori_loop(0, run, first, (start,) * tiles, unroll=4)
    leads, totals = [], []
    for b in range(tiles):
        prod, state = ends[b]
        enter_p, enter_s = [None] * 8, [None] * 8
        now_p, now_s = jnp.ones((1, wide), F32), jnp.zeros((1, wide), F32)
        for c in range(7, -1, -1) if reverse else range(8):
            enter_p[c], enter_s[c] = now_p, now_s
            now_p, now_s = now_p * prod[c : c + 1], prod[c : c + 1] * now_s + state[c : c + 1]
        leads.append((jnp.concatenate(enter_p, 0), jnp.concatenate(enter_s, 0)))
        totals.append((now_p, now_s))

    def second(r, _):
        here = pl.ds(r, 8, stride=run)
        for b in range(tiles):
            p = a_ref[b, here, :]
            a_ref[b, here, :] = p * leads[b][0]
            d_ref[b, here, :] = d_ref[b, here, :] + p * leads[b][1]
        return 0

    lax.fori_loop(0, run, second, 0, unroll=4)
    for b in range(tiles):
        p_ref[:, b * wide : (b + 1) * wide] = a_ref[b]
        s_ref[:, b * wide : (b + 1) * wide] = d_ref[b]
    return jnp.concatenate([p for p, _ in totals], 1), jnp.concatenate([v for _, v in totals], 1)


def tiled_store(ref, value):
    tiles, _, wide = ref.shape
    for b in range(tiles):
        ref[b] = value[:, b * wide : (b + 1) * wide]


def positions(base_ref, rows, lanes, length):
    place = lax.broadcasted_iota(jnp.int32, (rows, lanes), 0) + base_ref[0]
    return jnp.where(place >= length, place - length, place)


def forward_kernel(
    length, local, base_ref, x_ref, cw_ref, rate_gain_ref, g_ref, sel_ref,
    conv_ref, rate_ref, in_ref, p_ref, s_ref, carry_ref, w_ref, a_ref, d_ref,
):
    rows, lanes = conv_ref.shape
    spot = positions(base_ref, rows, lanes, length)
    x = x_ref[...].astype(F32)
    total = cw_ref[0:1, :] * x[HALO:]
    for k in range(1, CONV):
        moved = pltpu.roll(x, k, 0)[HALO:]
        total = total + jnp.where(spot >= k, cw_ref[k : k + 1, :] * moved, 0.0)
    conv = total.astype(BF16)
    conv_ref[...] = conv
    join = sel_ref.shape[0]
    wide = jnp.dot(g_ref[0], sel_ref[0], preferred_element_type=F32)
    for q in range(1, join):
        other = jnp.dot(g_ref[0], sel_ref[q], preferred_element_type=F32)
        which = lax.broadcasted_iota(jnp.int32, wide.shape, 0) // local % join
        wide = jnp.where(which == q, other, wide)
    gates = wide.astype(BF16)
    w_ref[0] = gates
    pre = lax.dot_general(conv, gates, (((1,), (1,)), ((), ())), preferred_element_type=F32)
    rate, inp = pre[:, :lanes], pre[:, lanes:]
    rate_ref[...] = rate
    in_ref[...] = inp
    decay = jnp.where(spot == 0, 0.0, jnp.exp(rate_gain_ref[...] * jax.nn.sigmoid(rate)))
    tiled_store(a_ref, decay)
    tiled_store(
        d_ref,
        jnp.sqrt(jnp.maximum(1.0 - decay * decay, 0.01)) * jax.nn.sigmoid(inp) * conv.astype(F32),
    )
    prod, state = chunk_scan(a_ref, d_ref, p_ref, s_ref, False)
    carry_ref[0:1, :] = prod
    carry_ref[1:2, :] = state


def middle_kernel(
    length, base_ref, mg_ref, y_ref, p_ref, s_ref, enter_ref, rate_ref, rate_gain_ref,
    ylow_ref, bp_ref, bs_ref, carry_ref, a_ref, d_ref,
):
    rows, lanes = mg_ref.shape
    spot = positions(base_ref, rows, lanes, length)
    states = s_ref[...] + p_ref[...] * enter_ref[...]
    value, slope = gelu_both(y_ref[...])
    grad = mg_ref[...]
    ylow_ref[...] = (grad * states * slope).astype(BF16)
    tiled_store(d_ref, grad * value)
    decay = jnp.where(spot == 0, 0.0, jnp.exp(rate_gain_ref[...] * jax.nn.sigmoid(rate_ref[...])))
    row = lax.broadcasted_iota(jnp.int32, (rows, lanes), 0)
    tiled_store(a_ref, jnp.where(row == rows - 1, 1.0, pltpu.roll(decay, rows - 1, 0)))
    prod, state = chunk_scan(a_ref, d_ref, bp_ref, bs_ref, True)
    carry_ref[0:1, :] = decay[0:1] * prod
    carry_ref[1:2, :] = decay[0:1] * state


def backward_kernel(
    length, local, base_ref, bp_ref, bs_ref, leave_ref, p_ref, s_ref, enter_ref, rate_ref, in_ref,
    conv_ref, rate_gain_ref, w_ref, cw_ref, x_ref, sel_ref,
    gates_ref, xback_ref, edge_ref, small_ref,
):
    rows, lanes = bp_ref.shape
    spot = positions(base_ref, rows, lanes, length)
    row = lax.broadcasted_iota(jnp.int32, (rows, lanes), 0)
    adjoint = bs_ref[...] + bp_ref[...] * leave_ref[...]
    states = s_ref[...] + p_ref[...] * enter_ref[...]
    before = jnp.where(row == 0, enter_ref[...], pltpu.roll(states, 1, 0))
    gain = rate_gain_ref[...]
    sig_r = jax.nn.sigmoid(rate_ref[...])
    sig_i = jax.nn.sigmoid(in_ref[...])
    conv = conv_ref[...]
    conv_f = conv.astype(F32)
    decay = jnp.where(spot == 0, 0.0, jnp.exp(gain * sig_r))
    room = 1.0 - decay * decay
    scale = jnp.sqrt(jnp.maximum(room, 0.01))
    pulled = adjoint * sig_i
    slope = jnp.where(room > 0.01, -decay / scale, 0.0)
    decay_grad = adjoint * before + pulled * conv_f * slope
    log_grad = decay_grad * decay
    pull_r = log_grad * sig_r
    rate_back = (pull_r * gain * (1.0 - sig_r)).astype(BF16)
    conv_direct = pulled * scale
    in_back = (conv_direct * conv_f * (1.0 - sig_i)).astype(BF16)
    both = jnp.concatenate([rate_back, in_back], 1)
    join = sel_ref.shape[0]
    for q in range(join):
        some = lax.dot_general(
            conv, sel_ref[q], (((1,), (1,)), ((), ())), preferred_element_type=F32
        ).astype(BF16)
        part = lax.dot_general(some, both, (((0,), (0,)), ((), ())), preferred_element_type=F32)
        if q == 0:
            gate_sum = part
        else:
            which = lax.broadcasted_iota(jnp.int32, part.shape, 1) // local % join
            gate_sum = jnp.where(which == q, part, gate_sum)
    runs, places, _, kinds, part, wide = gates_ref.shape
    gate_low = gate_sum.astype(BF16)
    for r in range(runs):
        for q in range(places):
            for kind in range(kinds):
                at = (kind * places + q) * wide
                gates_ref[r, q, 0, kind] = gate_low[r * part : (r + 1) * part, at : at + wide]
    grad = conv_direct + lax.dot_general(
        both, w_ref[0], (((1,), (0,)), ((), ())), preferred_element_type=F32
    )
    x = x_ref[...].astype(F32)
    zeros = jnp.zeros((HALO, lanes), F32)
    out = jnp.concatenate([zeros, grad * cw_ref[0:1, :]], 0)
    small_ref[0:1, :] = jnp.sum(grad * x[HALO:], axis=0, keepdims=True)
    for k in range(1, CONV):
        masked = jnp.where(spot >= k, grad, 0.0)
        small_ref[k : k + 1, :] = jnp.sum(
            masked * pltpu.roll(x, k, 0)[HALO:], axis=0, keepdims=True
        )
        tall = jnp.concatenate([zeros, masked * cw_ref[k : k + 1, :]], 0)
        out = out + pltpu.roll(tall, rows + HALO - k, 0)
    small_ref[CONV : CONV + 1, :] = jnp.sum(pull_r, axis=0, keepdims=True)
    small_ref[CONV + 1 : 8, :] = jnp.zeros((7 - CONV, lanes), F32)
    edge_ref[...] = out[:HALO]
    xback_ref[...] = out[HALO:]


def lane_call(kernel, grid, lanes, base, operands, outputs, scratch, flops):
    def spec(shape):
        if len(shape) == 6:
            return pl.BlockSpec(
                shape[:2] + (1,) + shape[3:], lambda j, *_: (0, 0, j, 0, 0, 0)
            )
        if len(shape) == 3 and shape[0] != grid:
            return pl.BlockSpec(shape, lambda j, *_: (0, 0, 0))
        if len(shape) == 3:
            return pl.BlockSpec((1,) + shape[1:], lambda j, *_: (j, 0, 0))
        return pl.BlockSpec((shape[0], lanes), lambda j, *_: (0, j))

    moved = sum(math.prod(a.shape) * a.dtype.itemsize for a in list(operands) + list(outputs))
    return pl.pallas_call(
        kernel,
        grid_spec=pltpu.PrefetchScalarGridSpec(
            num_scalar_prefetch=1,
            grid=(grid,),
            in_specs=[spec(a.shape) for a in operands],
            out_specs=[spec(a.shape) for a in outputs],
            scratch_shapes=scratch,
        ),
        out_shape=outputs,
        compiler_params=pltpu.CompilerParams(
            dimension_semantics=("arbitrary",), vmem_limit_bytes=56 << 20
        ),
        cost_estimate=pl.CostEstimate(flops=flops, bytes_accessed=moved, transcendentals=0),
    )(base, *operands)


def shards(
    tokens_in, gain_pre, w_x, w_y, conv_w, gate_a, gate_i, decay_param, w_out,
    gain_mlp, w_gate, w_up, w_down, cotangent,
):
    rows, width = tokens_in.shape
    heads, local = w_x.shape[1:]
    n_ten, n_seq = lax.axis_size("tensor"), lax.axis_size("seq")
    devices = n_ten * n_seq
    place, run = lax.axis_index("tensor"), lax.axis_index("seq")
    linear = run * n_ten + place
    length = devices * rows // SEQS
    base = jnp.reshape((linear * rows) % length, (1,)).astype(jnp.int32)
    join = 128 // local if local < 128 and heads % (128 // local) == 0 else 1
    groups, chunk = heads // join, join * local
    lanes = n_ten * chunk
    channels = groups * lanes

    def shape(dims, kind=F32):
        return jax.ShapeDtypeStruct(dims, kind)

    def own_columns(array):
        n = array.shape[0]
        split = array.reshape(n, groups, n_ten, chunk)
        return lax.dynamic_index_in_dim(split, place, 2, False).reshape(n, heads, local)

    gate_rows = jnp.stack([gate_a, gate_i], 0).swapaxes(2, 3).reshape(2 * heads, local, n_ten * local)
    params = jnp.concatenate([conv_w, decay_param[None]], 0).reshape(CONV + 1, heads * local)
    params = jnp.pad(params, ((0, 7 - CONV), (0, 0)))
    (all_gates, full_x, full_y, full_out), params, cots, halo = gather_all(
        [
            gate_rows,
            jnp.transpose(w_x, (1, 2, 0)).reshape(groups, chunk, width),
            jnp.transpose(w_y, (1, 2, 0)).reshape(groups, chunk, width),
            w_out.reshape(groups, chunk, width),
        ],
        params, cotangent, tokens_in, HALO,
    )
    halo = jnp.where(linear == 0, jnp.zeros_like(halo), halo)
    full_x, full_y, full_out = (w.reshape(channels, width) for w in (full_x, full_y, full_out))
    gates = all_gates.reshape(2, groups, join, n_ten, local, n_ten * local)
    gates = jnp.transpose(gates, (1, 0, 3, 2, 4, 5)).reshape(groups, 2 * lanes, n_ten * local)
    key = jnp.arange(n_ten * local)[None, :, None]
    lane = jnp.arange(lanes)[None, None, :]
    member = jnp.arange(join)[:, None, None]
    select = (
        (lane // chunk == key // local) & (lane % local == key % local) & (lane // local % join == member)
    ).astype(BF16)
    params = jnp.transpose(params.reshape(n_ten, 8, groups, chunk), (1, 2, 0, 3)).reshape(8, channels)
    conv_rows, decay_full = params, params[CONV : CONV + 1]
    rate_gain = -8.0 * jax.nn.softplus(decay_full)

    own_in = tokens_in.astype(F32)
    in_scale, in_unit = rms_parts(own_in)
    normed = (in_unit * gain_pre).astype(BF16)
    normed_halo = (rms_parts(halo.astype(F32))[1] * gain_pre).astype(BF16)
    x_long = dot_nt(jnp.concatenate([normed_halo, normed], 0), full_x).astype(BF16)
    y_branch = dot_nt(normed, full_y)
    scratch = [pltpu.VMEM((lanes // 128, rows, 128), F32)] * 2
    conv_out, rate_pre, input_pre, products, partial, carry, wide_gates = lane_call(
        functools.partial(forward_kernel, length, local), groups, lanes, base,
        (x_long, conv_rows, rate_gain, gates, select),
        [
            shape((rows, channels), BF16),
            shape((rows, channels)),
            shape((rows, channels)),
            shape((rows, channels)),
            shape((rows, channels)),
            shape((2, channels)),
            shape((groups, 2 * lanes, lanes), BF16),
        ],
        scratch, 4 * rows * lanes * channels,
    )
    reach = min(-(-length // rows), devices - 1)
    enter = entering(carry, reach, linear, devices, False)
    states = partial + products * enter
    mixed = (states * jax.nn.gelu(y_branch, approximate=True)).astype(BF16)
    middle = own_in + dot_nn(mixed, full_out)
    mid_scale, mid_unit = rms_parts(middle)
    normed_mlp = (mid_unit * gain_mlp).astype(BF16)

    if n_ten == 4 and n_seq == 8:
        *kept, mlp_input, downs = feed_forward(normed_mlp, cots, w_gate, w_up, w_down)
        cot_rows = cots.reshape(n_ten * rows, width)
        token_rows, hidden_rows, gate_rows, up_rows = (
            a.reshape(n_ten * rows, a.shape[2]) for a in kept
        )
    else:
        cots = [cotangent] + [
            lax.dynamic_index_in_dim(cots, label_index(k), 0, False) for k in range(1, n_ten)
        ]
        tokens = [normed_mlp] + others(normed_mlp)
        hiddens, gate_grads, up_grads, downs, pulls = [], [], [], [], []
        for n, c in zip(tokens, cots):
            gate_vals, up_vals = dot_nn(n, w_gate), dot_nn(n, w_up)
            value, slope = gelu_both(gate_vals)
            hidden = (value * up_vals).astype(BF16)
            hidden_grad = dot_nt(c, w_down)
            gate_grad = (hidden_grad * up_vals * slope).astype(BF16)
            up_grad = (hidden_grad * value).astype(BF16)
            hiddens.append(hidden)
            gate_grads.append(gate_grad)
            up_grads.append(up_grad)
            pulls.append(dot_nt(gate_grad, w_gate) + dot_nt(up_grad, w_up))
            downs.append(dot_nn(hidden, w_down).astype(BF16))
        mlp_input = line_sum(pulls[0], [p.astype(BF16) for p in pulls[1:]])
        cot_rows, token_rows, hidden_rows, gate_rows, up_rows = (
            jnp.concatenate(a, 0) for a in (cots, tokens, hiddens, gate_grads, up_grads)
        )
    grad_down = dot_tn(cot_rows, hidden_rows).astype(BF16)
    grad_gate = dot_tn(token_rows, gate_rows).astype(BF16)
    grad_up = dot_tn(token_rows, up_rows).astype(BF16)
    gain_mlp_part, mid_back = rms_back(mlp_input, gain_mlp, mid_scale, mid_unit)
    middle_grad = cotangent.astype(F32) + mid_back
    middle_low, *_ = lax.optimization_barrier(
        (middle_grad.astype(BF16), grad_down, grad_gate, grad_up)
    )
    grad_down, grad_gate, grad_up = (
        lax.psum_scatter(g, "seq", scatter_dimension=0, tiled=True)
        for g in (grad_down, grad_gate, grad_up)
    )
    mixed_grad = dot_nt(middle_low, full_out)
    y_low, back_products, back_partial, carry = lane_call(
        functools.partial(middle_kernel, length), groups, lanes, base,
        (mixed_grad, y_branch, products, partial, enter, rate_pre, rate_gain),
        [
            shape((rows, channels), BF16),
            shape((rows, channels)),
            shape((rows, channels)),
            shape((2, channels)),
        ],
        scratch, 60 * rows * channels,
    )
    leave = entering(carry, reach, linear, devices, True)
    part = n_ten * local // n_seq
    gate_parts, x_back, edge, sums = lane_call(
        functools.partial(backward_kernel, length, local), groups, lanes, base,
        (
            back_products, back_partial, leave, products, partial, enter, rate_pre, input_pre,
            conv_out, rate_gain, wide_gates, conv_rows, x_long, select,
        ),
        [
            shape((n_seq, n_ten, groups, 2, part, chunk), BF16),
            shape((rows, channels)),
            shape((HALO, channels)),
            shape((8, channels)),
        ],
        [], 8 * rows * lanes * channels,
    )
    edge = lax.ppermute(edge, BOTH, [(i + 1, i) for i in range(devices - 1)])
    x_low = jnp.concatenate(
        [x_back[: rows - HALO], x_back[rows - HALO :] + edge], 0
    ).astype(BF16)

    normed_grad = dot_nn(x_low, full_x) + dot_nn(y_low, full_y)
    gain_pre_part, in_back = rms_back(normed_grad, gain_pre, in_scale, in_unit)
    input_grad = middle_grad + in_back

    split = gate_parts.reshape(devices, groups * 2 * part, chunk)
    packed = jnp.concatenate(
        [sums[: CONV + 1], gain_pre_part[None], gain_mlp_part[None], sums[CONV + 3 :]], 0
    )
    (grad_out, grad_y, grad_x), down, gate_sum, packed = weight_grads(
        (0, 1, 1), [middle_low, normed], [mixed, y_low, x_low], groups, downs, split, packed
    )
    block_out = (middle + down).astype(BF16)
    gate_sum = gate_sum.reshape(groups, 2, part, join, local)
    gate_sum = jnp.transpose(gate_sum, (1, 0, 3, 2, 4)).reshape(2, heads, part, local)
    conv_sum = own_columns(packed[:CONV])
    decay_sum = own_columns(packed[CONV : CONV + 1] * (-8.0 * jax.nn.sigmoid(decay_full)))[0]
    share = local // n_seq
    grad_conv = lax.dynamic_slice_in_dim(conv_sum, run * share, share, 2)
    grad_decay = lax.dynamic_slice_in_dim(decay_sum, run * share, share, 1)
    grad_gain_mlp = lax.dynamic_slice_in_dim(
        packed[CONV + 2], run * (width // n_seq), width // n_seq, 0
    )

    def weight(grad):
        return grad.reshape(heads, local, -1)

    return (
        block_out,
        input_grad,
        packed[CONV + 1],
        jnp.transpose(weight(grad_x), (2, 0, 1)),
        jnp.transpose(weight(grad_y), (2, 0, 1)),
        grad_conv,
        gate_sum[0],
        gate_sum[1],
        grad_decay,
        weight(grad_out),
        grad_gain_mlp,
        grad_gate.astype(F32),
        grad_up.astype(F32),
        grad_down.astype(F32).T,
    )


def solution(mesh):
    placed = (
        P(("seq", "tensor"), None),
        P(),
        P(None, None, "tensor"),
        P(None, None, "tensor"),
        P(None, None, "tensor"),
        P(None, None, "tensor"),
        P(None, None, "tensor"),
        P(None, "tensor"),
        P(None, "tensor", None),
        P(),
        P(None, "tensor"),
        P(None, "tensor"),
        P("tensor", None),
        P(("seq", "tensor"), None),
    )
    return jax.shard_map(
        shards,
        mesh=mesh,
        in_specs=placed,
        out_specs=(
            P(("seq", "tensor"), None),
            P(("seq", "tensor"), None),
            P(),
            P("seq", None, "tensor"),
            P("seq", None, "tensor"),
            P(None, None, ("tensor", "seq")),
            P(None, "seq", "tensor"),
            P(None, "seq", "tensor"),
            P(None, ("tensor", "seq")),
            P(None, "tensor", "seq"),
            P("seq"),
            P("seq", "tensor"),
            P("seq", "tensor"),
            P("tensor", "seq"),
        ),
        check_vma=False,
    )
```
